8 devices in a mesh: dp: 1 (over z), tp: 2 (over y), sq: 4 (over x, core).
Axes of the slice: x: 2, y: 2, z: 1, core: 2. Of those that a mesh axis runs over, the one named last changes fastest.
Arguments:
- x_steps: bfloat16 [4, 128, 3072], P(None, 'dp')
- positions: int32 [128], P('dp')
- k_cache: bfloat16 [128, 4096, 2, 128], P('dp', 'sq', 'tp')
- v_cache: bfloat16 [128, 4096, 2, 128], P('dp', 'sq', 'tp')
- w_q: bfloat16 [3072, 3072], P(None, 'tp')
- b_q: bfloat16 [3072], P('tp')
- w_k: bfloat16 [3072, 256], P(None, 'tp')
- b_k: bfloat16 [256], P('tp')
- w_v: bfloat16 [3072, 256], P(None, 'tp')
- b_v: bfloat16 [256], P('tp')
- w_o: bfloat16 [3072, 3072], P('tp')
- b_o: bfloat16 [3072], replicated
- ln1_gain: bfloat16 [3072], replicated
- ln1_bias: bfloat16 [3072], replicated
- ln2_gain: bfloat16 [3072], replicated
- ln2_bias: bfloat16 [3072], replicated
- w_fc: bfloat16 [3072, 12288], P(None, 'tp')
- b_fc: bfloat16 [12288], P('tp')
- w_proj: bfloat16 [12288, 3072], P('tp')
- b_proj: bfloat16 [3072], replicated
Outputs:
- output 1: bfloat16 [4, 128, 3072], P(None, 'dp')
- output 2: bfloat16 [128, 4096, 2, 128], P('dp', 'sq', 'tp')
- output 3: bfloat16 [128, 4096, 2, 128], P('dp', 'sq', 'tp')
All inputs are finite; a program needn't handle non-finite values.
Results may differ from the reference program's by a relative error of at most 0.0151432.
Values sent between devices are 32-bit elements.
A program may use at most 1 GiB of HBM per device.

```python
import jax
import jax.numpy as jnp
from jax import lax

D = 3072
HEADS = 24
KV_HEADS = 2
HEAD = 128
FF = 12288
WINDOW = 4096
BATCH = 128
STEPS = 4
ROPE_BASE = 1000000
POS_LOW = 100
POS_HIGH = 15000
HOT_ODDS = 512
HOT_RUN = 8


def rope_tables(positions, head_dim):
    half_dim = head_dim // 2
    inv_freq = jnp.power(jnp.float32(ROPE_BASE), -2.0 * jnp.arange(half_dim, dtype=jnp.float32) / head_dim)
    angle = positions.astype(jnp.float32)[..., None] * inv_freq
    return jnp.cos(angle), jnp.sin(angle)


def apply_rope(vectors, cos_t, sin_t):
    half_dim = vectors.shape[-1] // 2
    first = vectors[..., :half_dim]
    second = vectors[..., half_dim:]
    return jnp.concatenate([first * cos_t - second * sin_t, second * cos_t + first * sin_t], axis=-1)


def layer_norm(vectors, gain, shift):
    row_mean = jnp.mean(vectors, axis=-1, keepdims=True)
    centered = vectors - row_mean
    row_var = jnp.mean(centered * centered, axis=-1, keepdims=True)
    return centered * lax.rsqrt(row_var + 1e-5) * gain.astype(jnp.float32) + shift.astype(jnp.float32)


def linear(rows_in, weight, bias):
    return jnp.dot(rows_in, weight, preferred_element_type=jnp.float32) + bias.astype(jnp.float32)


def hot_direction():
    dim_ids = jnp.arange(HEAD)
    marked = (dim_ids % (HEAD // 2)) >= HEAD // 2 - 4
    return jnp.where(marked, 8.0 ** -0.5, 0.0).astype(jnp.float32)


def draw_positions(key):
    key_low, key_high, key_pick, key_perm = jax.random.split(key, 4)
    short = jax.random.randint(key_low, (BATCH,), POS_LOW, WINDOW)
    longer = jax.random.randint(key_high, (BATCH,), WINDOW, POS_HIGH + 1)
    chooser = jax.random.randint(key_pick, (BATCH,), 0, 4)
    mixed = jnp.where(chooser == 0, short, longer)
    mixed = mixed.at[0].set(POS_LOW).at[1].set(POS_HIGH)
    return jax.random.permutation(key_perm, mixed).astype(jnp.int32)


def setup_inputs(seed: int = 0, part: int = 0) -> dict:
    shared = jax.random.split(jax.random.key(seed), 16)
    own = jax.random.split(jax.random.fold_in(jax.random.key(seed + 1), part), 5)
    hot_amp = (8.0 * HEAD ** 0.5) ** 0.5
    hot_vec = hot_direction() * hot_amp
    positions = draw_positions(own[0])
    slot_ids = jnp.arange(WINDOW, dtype=jnp.int32)
    last_pos = positions[:, None] - 1
    held_pos = last_pos - (last_pos - slot_ids[None, :]) % WINDOW
    hot_slot = (jax.random.randint(own[1], (BATCH, WINDOW), 0, HOT_ODDS) == 0) | ((slot_ids[None, :] - positions[:, None]) % WINDOW < HOT_RUN)
    cos_t, sin_t = rope_tables(held_pos, HEAD)
    hot_keys = apply_rope(jnp.broadcast_to(hot_vec, (BATCH, WINDOW, HEAD)), cos_t, sin_t)
    hot_keys = jnp.where(hot_slot[:, :, None], hot_keys, 0.0)
    k_cache = (jax.random.normal(own[2], (BATCH, WINDOW, KV_HEADS, HEAD), jnp.float32) + hot_keys[:, :, None, :]).astype(jnp.bfloat16)
    v_cache = jax.random.normal(own[3], (BATCH, WINDOW, KV_HEADS, HEAD), jnp.float32).astype(jnp.bfloat16)
    x_steps = jax.random.normal(own[4], (STEPS, BATCH, D), jnp.float32).astype(jnp.bfloat16)

    def scaled(key, shape, scale):
        return (jax.random.normal(key, shape, jnp.float32) * scale).astype(jnp.bfloat16)

    b_q = (0.5 * jax.random.normal(shared[1], (HEADS * HEAD,), jnp.float32) + jnp.tile(hot_vec, HEADS)).astype(jnp.bfloat16)
    b_k = (0.5 * jax.random.normal(shared[3], (KV_HEADS * HEAD,), jnp.float32) + jnp.tile(hot_vec, KV_HEADS)).astype(jnp.bfloat16)
    return {
        "x_steps": x_steps,
        "positions": positions,
        "k_cache": k_cache,
        "v_cache": v_cache,
        "w_q": scaled(shared[0], (D, HEADS * HEAD), D ** -0.5),
        "b_q": b_q,
        "w_k": scaled(shared[2], (D, KV_HEADS * HEAD), D ** -0.5),
        "b_k": b_k,
        "w_v": scaled(shared[4], (D, KV_HEADS * HEAD), D ** -0.5),
        "b_v": scaled(shared[5], (KV_HEADS * HEAD,), 0.5),
        "w_o": scaled(shared[6], (HEADS * HEAD, D), 3.0 * (HEADS * HEAD) ** -0.5),
        "b_o": scaled(shared[7], (D,), 0.2),
        "ln1_gain": (1.0 + 0.2 * jax.random.normal(shared[8], (D,), jnp.float32)).astype(jnp.bfloat16),
        "ln1_bias": scaled(shared[9], (D,), 0.2),
        "ln2_gain": (1.0 + 0.2 * jax.random.normal(shared[10], (D,), jnp.float32)).astype(jnp.bfloat16),
        "ln2_bias": scaled(shared[11], (D,), 0.2),
        "w_fc": scaled(shared[12], (D, FF), D ** -0.5),
        "b_fc": scaled(shared[13], (FF,), 0.5),
        "w_proj": scaled(shared[14], (FF, D), 1.5 * FF ** -0.5),
        "b_proj": scaled(shared[15], (D,), 0.2),
    }


def reference(x_steps, positions, k_cache, v_cache, w_q, b_q, w_k, b_k, w_v, b_v, w_o, b_o,
              ln1_gain, ln1_bias, ln2_gain, ln2_bias, w_fc, b_fc, w_proj, b_proj):
    group = HEADS // KV_HEADS
    slot_ids = jnp.arange(WINDOW, dtype=jnp.int32)
    batch_ids = jnp.arange(BATCH, dtype=jnp.int32)
    score_scale = HEAD ** -0.5

    def attend_one(packed):
        q_one, k_one, v_one, slot_ok = packed
        scores = jnp.einsum("grd,wgd->grw", q_one.reshape(KV_HEADS, group, HEAD).astype(jnp.float32), k_one.astype(jnp.float32)) * score_scale
        scores = jnp.where(slot_ok[None, None, :], scores, -1e30)
        weights = jax.nn.softmax(scores, axis=-1)
        return jnp.einsum("grw,wgd->grd", weights, v_one.astype(jnp.float32))

    def one_step(carry, step_in):
        key_buf, val_buf = carry
        x_in, step_idx = step_in
        cur_pos = positions + step_idx
        hidden = layer_norm(x_in.astype(jnp.float32), ln1_gain, ln1_bias).astype(jnp.bfloat16)
        query = linear(hidden, w_q, b_q).astype(jnp.bfloat16)
        key_new = linear(hidden, w_k, b_k).astype(jnp.bfloat16)
        val_new = linear(hidden, w_v, b_v).astype(jnp.bfloat16)
        cos_t, sin_t = rope_tables(cur_pos, HEAD)
        q_rot = apply_rope(query.reshape(BATCH, HEADS, HEAD).astype(jnp.float32), cos_t[:, None, :], sin_t[:, None, :]).astype(jnp.bfloat16)
        k_rot = apply_rope(key_new.reshape(BATCH, KV_HEADS, HEAD).astype(jnp.float32), cos_t[:, None, :], sin_t[:, None, :]).astype(jnp.bfloat16)
        write_slot = cur_pos % WINDOW
        key_buf = key_buf.at[batch_ids, write_slot].set(k_rot)
        val_buf = val_buf.at[batch_ids, write_slot].set(val_new.reshape(BATCH, KV_HEADS, HEAD))
        held_pos = cur_pos[:, None] - (cur_pos[:, None] - slot_ids[None, :]) % WINDOW
        attn = lax.map(attend_one, (q_rot, key_buf, val_buf, held_pos >= 0))
        attn_out = attn.astype(jnp.bfloat16).reshape(BATCH, HEADS * HEAD)
        x_mid = (x_in.astype(jnp.float32) + jnp.dot(attn_out, w_o, preferred_element_type=jnp.float32) + b_o.astype(jnp.float32)).astype(jnp.bfloat16)
        hidden_two = layer_norm(x_mid.astype(jnp.float32), ln2_gain, ln2_bias).astype(jnp.bfloat16)
        gelu_out = jax.nn.gelu(linear(hidden_two, w_fc, b_fc), approximate=True).astype(jnp.bfloat16)
        y_out = (x_mid.astype(jnp.float32) + jnp.dot(gelu_out, w_proj, preferred_element_type=jnp.float32) + b_proj.astype(jnp.float32)).astype(jnp.bfloat16)
        return (key_buf, val_buf), y_out

    (k_final, v_final), y_steps = lax.scan(one_step, (k_cache, v_cache), (x_steps, jnp.arange(STEPS, dtype=jnp.int32)))
    return y_steps, k_final, v_final
```

```python
import functools
import math

import jax
import jax.numpy as jnp
from jax import lax
from jax.experimental import pallas as pl
from jax.experimental.pallas import tpu as pltpu
from jax.sharding import PartitionSpec as P

ROPE_BASE = 1000000.0
LN_EPS = 1e-5
NEG_BIG = -1e30
F32 = jnp.float32
BF16 = jnp.bfloat16
SQ = 4
QB = 8
NB = 4
CHUNK = SQ * QB
HEAD = 128
VMEM_LIMIT = 60 * 1024 * 1024


def dot(a, b):
    return lax.dot_general(a, b, (((1,), (0,)), ((), ())), preferred_element_type=F32)


def dot_nt(a, b):
    return lax.dot_general(a, b, (((1,), (1,)), ((), ())), preferred_element_type=F32)


def layer_norm(vectors, gain, shift):
    row_mean = jnp.mean(vectors, axis=-1, keepdims=True)
    centered = vectors - row_mean
    row_var = jnp.mean(centered * centered, axis=-1, keepdims=True)
    return centered * lax.rsqrt(row_var + LN_EPS) * gain + shift


def params(n_grid, **kw):
    return pltpu.CompilerParams(dimension_semantics=("arbitrary",) * n_grid, vmem_limit_bytes=VMEM_LIMIT, **kw)


def qkv_kernel(n_q, x_ref, gain_ref, shift_ref, wq_ref, bq_ref, wk_ref, bk_ref, wv_ref, bv_ref, cos_ref, sin_ref,
               q_ref, k_ref, v_ref, h_ref):
    step = pl.program_id(0)
    steps, batch = x_ref.shape[0], x_ref.shape[1]
    chunks = batch // CHUNK

    @pl.when(step == 0)
    def _():
        gain, shift = gain_ref[...].astype(F32), shift_ref[...].astype(F32)
        for s in range(steps):
            for r in range(0, batch, 32):
                h_ref[s * batch + r:s * batch + r + 32, :] = layer_norm(x_ref[s, r:r + 32, :].astype(F32), gain, shift).astype(BF16)

    def rope(vec, rows):
        vec = vec.astype(BF16).astype(F32)
        out = vec * cos_ref[rows, :] + pltpu.roll(vec, HEAD // 2, 1) * sin_ref[rows, :]
        return out.astype(BF16).astype(F32)

    @pl.when(step < n_q)
    def _():
        for s in range(steps):
            rows = slice(s * batch, (s + 1) * batch)
            acc = dot(h_ref[rows, :], wq_ref[...]) + bq_ref[0].astype(F32)
            for h in range(2):
                rot = rope(acc[:, h * HEAD:(h + 1) * HEAD], rows)
                for c in range(chunks):
                    q_ref[c, s, h] = rot[c * CHUNK:(c + 1) * CHUNK, :]

    @pl.when(step == n_q)
    def _():
        for s in range(steps):
            rows = slice(s * batch, (s + 1) * batch)
            hid = h_ref[rows, :]
            rot = rope(dot(hid, wk_ref[...]) + bk_ref[...].astype(F32), rows)
            val = (dot(hid, wv_ref[...]) + bv_ref[...].astype(F32)).astype(BF16).astype(F32)
            for c in range(chunks):
                k_ref[c, s] = rot[c * CHUNK:(c + 1) * CHUNK, :]
                v_ref[c, s] = val[c * CHUNK:(c + 1) * CHUNK, :]
        for s in range(steps, 8):
            for c in range(chunks):
                k_ref[c, s] = jnp.zeros((CHUNK, HEAD), F32)
                v_ref[c, s] = jnp.zeros((CHUNK, HEAD), F32)


def qkv(x_steps, gain, shift, w_q, b_q, w_k, b_k, w_v, b_v, cos_t, sin_t):
    steps, batch, dim = x_steps.shape
    chunks = batch // CHUNK
    heads = w_q.shape[1] // HEAD
    n_q = heads // 2
    whole = lambda *shape: pl.BlockSpec(shape, lambda j: (0,) * len(shape))
    last = n_q - 1
    return pl.pallas_call(
        functools.partial(qkv_kernel, n_q),
        grid=(n_q + 1,),
        in_specs=[
            whole(steps, batch, dim), whole(1, dim), whole(1, dim),
            pl.BlockSpec((dim, 2 * HEAD), lambda j: (0, jnp.minimum(j, last))),
            pl.BlockSpec((1, 1, 2 * HEAD), lambda j: (jnp.minimum(j, last), 0, 0)),
            whole(dim, HEAD), whole(1, HEAD), whole(dim, HEAD), whole(1, HEAD),
            whole(steps * batch, HEAD), whole(steps * batch, HEAD),
        ],
        out_specs=[
            pl.BlockSpec((chunks, steps, 2, CHUNK, HEAD), lambda j: (0, 0, jnp.minimum(j, last), 0, 0)),
            whole(chunks, 8, CHUNK, HEAD), whole(chunks, 8, CHUNK, HEAD),
        ],
        out_shape=[
            jax.ShapeDtypeStruct((chunks, steps, heads, CHUNK, HEAD), F32),
            jax.ShapeDtypeStruct((chunks, 8, CHUNK, HEAD), F32),
            jax.ShapeDtypeStruct((chunks, 8, CHUNK, HEAD), F32),
        ],
        scratch_shapes=[pltpu.VMEM((steps * batch, dim), BF16)],
        compiler_params=params(1),
        cost_estimate=pl.CostEstimate(flops=2 * steps * batch * dim * (w_q.shape[1] + 2 * HEAD), bytes_accessed=20_000_000, transcendentals=0),
        name="qkv",
    )(x_steps, gain[None], shift[None], w_q, b_q.reshape(n_q, 1, 2 * HEAD), w_k, b_k[None], w_v, b_v[None], cos_t, sin_t)


def attn_kernel(chunk, group, slots, n_alias, info_ref, q_ref, kn_ref, vn_ref, k_ref, v_ref, *rest):
    ko_ref, vo_ref, o0_ref, o1_ref, o2_ref, o3_ref, o_scr = rest[n_alias:]
    jj = pl.program_id(0)
    me = info_ref[0]
    rel = 3 - jj // 2
    part = jj % 2
    grp = jnp.bitwise_xor(me, rel) * 2 + part
    local = k_ref.shape[1]
    rows = 4 * group
    first_slot = me * local
    exp_scale = math.log2(math.e) * HEAD ** -0.5
    step_col = lax.broadcasted_iota(jnp.int32, (rows, 1), 0) // group
    lane = lax.broadcasted_iota(jnp.int32, (1, local), 1) + first_slot
    new_lane = lax.broadcasted_iota(jnp.int32, (1, 8), 1)
    diag = lax.broadcasted_iota(jnp.int32, (rows, HEAD), 0) == lax.broadcasted_iota(jnp.int32, (rows, HEAD), 1)
    order = [jnp.bitwise_and(jb + me, NB - 1) for jb in range(NB)]

    for jb in range(NB):
        bl = order[jb]
        seq = grp * NB + bl
        pos = info_ref[1 + chunk * CHUNK + seq]
        query = q_ref[0, pl.ds(seq, rows, stride=CHUNK), :].astype(BF16)
        keys = k_ref[bl]
        vals = v_ref[bl]
        ko_ref[bl] = keys
        vo_ref[bl] = vals
        age = jnp.where(lane < pos, jnp.bitwise_and(lane - pos, slots - 1), 0)
        scores = jnp.where(age > step_col, dot_nt(query, keys), NEG_BIG)
        part_max = jnp.max(scores, axis=1, keepdims=True)
        if jb == 0:
            new_keys = kn_ref[0, pl.ds(seq, 8, stride=CHUNK), :].astype(BF16)
            new_vals = vn_ref[0, pl.ds(seq, 8, stride=CHUNK), :].astype(BF16)
            new_scores = jnp.where(new_lane <= step_col, dot_nt(query, new_keys), NEG_BIG)
            part_max = jnp.maximum(part_max, jnp.max(new_scores, axis=1, keepdims=True))
        weights = jnp.exp2((scores - part_max) * exp_scale)
        part_sum = jnp.sum(weights, axis=1, keepdims=True)
        out = dot(weights.astype(BF16), vals)
        if jb == 0:
            new_weights = jnp.exp2((new_scores - part_max) * exp_scale)
            part_sum = part_sum + jnp.sum(new_weights, axis=1, keepdims=True)
            out = out + dot(new_weights.astype(BF16), new_vals)
        o_scr[pl.ds(pl.multiple_of(bl * rows, 8), rows), :] = out
        o_scr[pl.ds(NB * rows + bl, 1), :] = jnp.sum(jnp.where(diag, part_max, 0.0), axis=0, keepdims=True)
        o_scr[pl.ds(NB * rows + NB + bl, 1), :] = jnp.sum(jnp.where(diag, part_sum, 0.0), axis=0, keepdims=True)

    for r, o_ref in enumerate((o0_ref, o1_ref, o2_ref, o3_ref)):
        @pl.when(rel == r)
        def _(o_ref=o_ref):
            o_ref[part] = o_scr[...]

    row16 = lax.broadcasted_iota(jnp.int32, (16, HEAD), 0)
    for bl in range(NB):
        seq = grp * NB + bl
        pos = info_ref[1 + chunk * CHUNK + seq]
        begin = jnp.bitwise_and(pos, slots - 1) - first_slot
        near = jnp.bitwise_and(begin, slots - 1)

        @pl.when((near < local) | (near > slots - 4))
        def _(bl=bl, seq=seq, begin=begin):
            for t in range(4):
                slot = jnp.bitwise_and(begin + t, slots - 1)

                @pl.when(slot < local)
                def _(t=t, slot=slot):
                    base = pl.multiple_of(slot // 16 * 16, 16)
                    hit = row16 == slot % 16
                    for out_ref, new_ref in ((ko_ref, kn_ref), (vo_ref, vn_ref)):
                        new = new_ref[0, pl.ds(t * CHUNK + seq, 1), :]
                        old = out_ref[bl, pl.ds(base, 16), :].astype(F32)
                        out_ref[bl, pl.ds(base, 16), :] = jnp.where(hit, new, old).astype(BF16)


def attention(chunk, slots, info, q, kn, vn, k_cache, v_cache, outs):
    batch, local, _ = k_cache.shape
    chunks = batch // CHUNK
    group = q.shape[2]
    rows = 4 * group
    width = NB * rows + 2 * NB
    n_alias = 0 if outs is None else 2

    def cache_map(jj, info_ref):
        rel = 3 - jj // 2
        return (chunk * (CHUNK // NB) + jnp.bitwise_xor(info_ref[0], rel) * 2 + jj % 2, 0, 0)

    cache_spec = pl.BlockSpec((NB, local, HEAD), cache_map)
    pick = lambda n: pl.BlockSpec((1, n, HEAD), lambda jj, info_ref: (chunk, 0, 0))
    part_spec = pl.BlockSpec((2, width, HEAD), lambda jj, info_ref: (0, 0, 0))
    part_shape = jax.ShapeDtypeStruct((2, width, HEAD), F32)
    cache_shape = jax.ShapeDtypeStruct(k_cache.shape, BF16)
    grid_spec = pltpu.PrefetchScalarGridSpec(
        num_scalar_prefetch=1,
        grid=(CHUNK // NB,),
        in_specs=[pick(rows * CHUNK), pick(8 * CHUNK), pick(8 * CHUNK), cache_spec, cache_spec] + [pl.BlockSpec(memory_space=pl.ANY)] * n_alias,
        out_specs=[cache_spec, cache_spec] + [part_spec] * 4,
        scratch_shapes=[pltpu.VMEM((width, HEAD), F32)],
    )
    return pl.pallas_call(
        functools.partial(attn_kernel, chunk, group, slots, n_alias),
        grid_spec=grid_spec,
        out_shape=[cache_shape, cache_shape] + [part_shape] * 4,
        input_output_aliases={6: 0, 7: 1} if n_alias else {},
        compiler_params=params(1),
        cost_estimate=pl.CostEstimate(flops=10_000_000_000, bytes_accessed=CHUNK * local * HEAD * 8, transcendentals=CHUNK * rows * local),
        name="attn",
    )(info, q.reshape(chunks, rows * CHUNK, HEAD), kn.reshape(chunks, 8 * CHUNK, HEAD), vn.reshape(chunks, 8 * CHUNK, HEAD), k_cache, v_cache, *(outs or ()))


def combine_kernel(group, p0_ref, p1_ref, p2_ref, p3_ref, wo_ref, out_ref, a_scr, a32_scr, abf_scr):
    rows = 4 * group
    exp_scale = math.log2(math.e) * HEAD ** -0.5

    @pl.when(pl.program_id(0) == 0)
    def _():
        parts = (p0_ref, p1_ref, p2_ref, p3_ref)
        for g in range(2):
            stats = [p[g, NB * rows:NB * rows + 2 * NB, :] for p in parts]
            top = functools.reduce(jnp.maximum, stats)
            scale = [jnp.exp2((st - top) * exp_scale) for st in stats]
            total = sum(sc * pltpu.roll(st, NB, 0) for sc, st in zip(scale, stats))
            scale = [(sc / total).T for sc in scale]
            for b in range(NB):
                acc = sum(p[g, b * rows:(b + 1) * rows, :] * sc[:rows, b:b + 1] for p, sc in zip(parts, scale))
                a_scr[pl.ds((g * NB + b) * rows, rows), :] = acc
        for s in range(4):
            for h in range(group):
                a32_scr[s * QB:(s + 1) * QB, h * HEAD:(h + 1) * HEAD] = a_scr[pl.ds(s * group + h, QB, stride=rows), :]
        abf_scr[...] = a32_scr[...].astype(BF16)

    out_ref[...] = dot(abf_scr[...], wo_ref[...])


def combine(parts, w_o):
    depth, dim = w_o.shape
    group = depth // HEAD
    n, block = 4, dim // 4
    part_spec = pl.BlockSpec(parts[0].shape, lambda j: (0, 0, 0))
    return pl.pallas_call(
        functools.partial(combine_kernel, group),
        grid=(n,),
        in_specs=[part_spec] * 4 + [pl.BlockSpec((depth, block), lambda j: (0, j))],
        out_specs=pl.BlockSpec((4 * QB, block), lambda j: (0, j)),
        out_shape=jax.ShapeDtypeStruct((4 * QB, dim), F32),
        scratch_shapes=[pltpu.VMEM((4 * group * QB, HEAD), F32), pltpu.VMEM((4 * QB, depth), F32), pltpu.VMEM((4 * QB, depth), BF16)],
        compiler_params=params(1),
        cost_estimate=pl.CostEstimate(flops=2_500_000_000, bytes_accessed=depth * dim * 2, transcendentals=0),
        name="combine_wo",
    )(*parts, w_o)


def fc_kernel(n, info_ref, *refs):
    own, got = refs[:n], refs[n:2 * n]
    xs = refs[2 * n:3 * n]
    bo_ref, gain_ref, shift_ref, wfc_ref, bfc_ref, g_ref, x1_ref, h_ref = refs[3 * n:]

    @pl.when(pl.program_id(0) == 0)
    def _():
        gain, shift, bias = gain_ref[...].astype(F32), shift_ref[...].astype(F32), bo_ref[...].astype(F32)
        for c in range(n):
            for s in range(4):
                rows = slice(s * QB, (s + 1) * QB)
                mid = (xs[c][s, 0, 0].astype(F32) + (own[c][rows, :] + got[c][rows, :]) + bias).astype(BF16).astype(F32)
                out = slice(c * 4 * QB + s * QB, c * 4 * QB + (s + 1) * QB)
                x1_ref[out, :] = mid
                h_ref[out, :] = layer_norm(mid, gain, shift)

    g_ref[...] = jax.nn.gelu(dot(h_ref[...].astype(BF16), wfc_ref[...]) + bfc_ref[0].astype(F32), approximate=True).astype(BF16)


def first_mlp(info, group_ids, own, got, x_view, b_o, gain, shift, w_fc, b_fc):
    dim, width = w_fc.shape
    n = len(group_ids)
    rows = n * 4 * QB
    block = 512
    full = lambda r, c: pl.BlockSpec((r, c), lambda j, info_ref: (0, 0))
    x_specs = [pl.BlockSpec((4, 1, 1, QB, dim), lambda j, info_ref, c=c: (0, c, info_ref[0], 0, 0)) for c in group_ids]
    grid_spec = pltpu.PrefetchScalarGridSpec(
        num_scalar_prefetch=1,
        grid=(width // block,),
        in_specs=[full(4 * QB, dim)] * (2 * n) + x_specs + [full(1, dim)] * 3
        + [pl.BlockSpec((dim, block), lambda j, info_ref: (0, j)), pl.BlockSpec((1, 1, block), lambda j, info_ref: (j, 0, 0))],
        out_specs=[pl.BlockSpec((rows, block), lambda j, info_ref: (0, j)), full(rows, dim)],
        scratch_shapes=[pltpu.VMEM((rows, dim), F32)],
    )
    return pl.pallas_call(
        functools.partial(fc_kernel, n),
        grid_spec=grid_spec,
        out_shape=[jax.ShapeDtypeStruct((rows, width), BF16), jax.ShapeDtypeStruct((rows, dim), F32)],
        compiler_params=params(1),
        cost_estimate=pl.CostEstimate(flops=11_000_000_000, bytes_accessed=dim * width * 2, transcendentals=rows * width),
        name="fc",
    )(info, *own, *got, *([x_view] * n), b_o[None], gain[None], shift[None], w_fc, b_fc.reshape(width // block, 1, block))


def proj_kernel(g_ref, w_ref, out_ref):
    out_ref[...] = dot(g_ref[...], w_ref[...])


def second_mlp(g, w_proj):
    rows, width = g.shape
    dim = w_proj.shape[1]
    block = 256
    return pl.pallas_call(
        proj_kernel,
        grid=(dim // block,),
        in_specs=[pl.BlockSpec((rows, width), lambda j: (0, 0)), pl.BlockSpec((width, block), lambda j: (0, j))],
        out_specs=pl.BlockSpec((rows, block), lambda j: (0, j)),
        out_shape=jax.ShapeDtypeStruct((rows, dim), F32),
        compiler_params=params(1),
        cost_estimate=pl.CostEstimate(flops=11_000_000_000, bytes_accessed=dim * width * 2, transcendentals=0),
        name="proj",
    )(g, w_proj)


def y_kernel(x1_ref, own_ref, got_ref, bias_ref, out_ref):
    out_ref[...] = (x1_ref[...] + (own_ref[...] + got_ref[...]) + bias_ref[...].astype(F32)).astype(BF16).astype(F32)


def finish_y(x1, own, got, bias):
    return pl.pallas_call(
        y_kernel,
        out_shape=jax.ShapeDtypeStruct(x1.shape, F32),
        compiler_params=pltpu.CompilerParams(vmem_limit_bytes=VMEM_LIMIT),
        cost_estimate=pl.CostEstimate(flops=1_000_000_000, bytes_accessed=x1.size * 16, transcendentals=0),
        name="finish_y",
    )(x1, own, got, bias[None])


def assemble_kernel(groups, info_ref, *refs):
    out_ref = refs[-1]
    me = info_ref[0]
    at = 0
    for ids in groups:
        for rel in range(4):
            for i, c in enumerate(ids):
                out_ref[0, c, jnp.bitwise_xor(me, rel)] = refs[at][i, 0].astype(BF16)
            at += 1


def assemble(info, groups, pieces, chunks):
    dim = pieces[0].shape[-1]
    specs, views = [], []
    for g, ids in enumerate(groups):
        for rel in range(4):
            specs.append(pl.BlockSpec((len(ids), 1, QB, dim), lambda s, info_ref: (0, s, 0, 0)))
            views.append(pieces[g * 4 + rel].reshape(len(ids), 4, QB, dim))
    grid_spec = pltpu.PrefetchScalarGridSpec(
        num_scalar_prefetch=1, grid=(4,), in_specs=specs,
        out_specs=pl.BlockSpec((1, chunks, SQ, QB, dim), lambda s, info_ref: (s, 0, 0, 0, 0)),
    )
    return pl.pallas_call(
        functools.partial(assemble_kernel, groups),
        grid_spec=grid_spec,
        out_shape=jax.ShapeDtypeStruct((4, chunks, SQ, QB, dim), BF16),
        compiler_params=params(1),
        name="assemble",
    )(info, *views)


def solution(mesh):
    act_spec = P(None, "dp", None)
    cache_spec = P("dp", "sq", "tp", None)
    col_spec = P(None, "tp")
    row_spec = P("tp", None)
    vec_spec = P("tp")
    rep_spec = P(None)
    in_specs = (act_spec, P("dp"), cache_spec, cache_spec, col_spec, vec_spec, col_spec, vec_spec,
                col_spec, vec_spec, row_spec, rep_spec, rep_spec, rep_spec, rep_spec, rep_spec,
                col_spec, vec_spec, row_spec, rep_spec)
    out_specs = (act_spec, cache_spec, cache_spec)

    def swap_sq(value, mask):
        return lax.ppermute(value, "sq", [(i, i ^ mask) for i in range(SQ)])

    def swap_tp(value):
        return lax.ppermute(value, "tp", [(0, 1), (1, 0)])

    def per_device(x_steps, positions, key_buf, val_buf, w_q, b_q, w_k, b_k, w_v, b_v, w_o, b_o,
                   ln1_gain, ln1_bias, ln2_gain, ln2_bias, w_fc, b_fc, w_proj, b_proj):
        steps, batch, dim = x_steps.shape
        local = key_buf.shape[1]
        slots = local * SQ
        chunks = batch // CHUNK
        me = lax.axis_index("sq").astype(jnp.int32)
        info = jnp.concatenate([me[None], positions])
        inv_freq = jnp.power(F32(ROPE_BASE), -2.0 * jnp.arange(HEAD // 2, dtype=F32) / HEAD)
        cur = positions[None, :] + jnp.arange(steps, dtype=jnp.int32)[:, None]
        angle = cur.reshape(-1).astype(F32)[:, None] * inv_freq
        cos_t, sin_t = jnp.cos(angle), jnp.sin(angle)
        cos_t = jnp.concatenate([cos_t, cos_t], axis=-1)
        sin_t = jnp.concatenate([-sin_t, sin_t], axis=-1)
        q, kn, vn = qkv(x_steps, ln1_gain, ln1_bias, w_q, b_q, w_k, b_k, w_v, b_v, cos_t, sin_t)
        k_old, v_old = key_buf.reshape(batch, local, HEAD), val_buf.reshape(batch, local, HEAD)
        x_view = x_steps.reshape(steps, chunks, SQ, QB, dim)

        caches = None
        own, got = [], []
        for c in range(chunks):
            res = attention(c, slots, info, q, kn, vn, k_old, v_old, caches)
            caches = res[:2]
            parts = list(res[2:])
            moved = [parts[0]] + [swap_sq(parts[r], r) for r in range(1, SQ)]
            own.append(combine(moved, w_o))
            got.append(swap_tp(own[-1]))

        groups = [list(range(0, chunks // 2)), list(range(chunks // 2, chunks))]
        pieces = []
        for ids in groups:
            g, x1 = first_mlp(info, ids, [own[c] for c in ids], [got[c] for c in ids], x_view, b_o, ln2_gain, ln2_bias, w_fc, b_fc)
            part = second_mlp(g, w_proj)
            y = finish_y(x1, part, swap_tp(part), b_proj)
            across = swap_sq(y, 2)
            pieces += [y, swap_sq(y, 1), across, swap_sq(across, 1)]
        ys = assemble(info, groups, pieces, chunks).reshape(steps, batch, dim)
        return ys, caches[0].reshape(key_buf.shape), caches[1].reshape(val_buf.shape)

    return jax.shard_map(per_device, mesh=mesh, in_specs=in_specs, out_specs=out_specs, check_vma=False)
```

```python
import functools
import math

import jax
import jax.numpy as jnp
from jax import lax
from jax.experimental import pallas as pl
from jax.experimental.pallas import tpu as pltpu
from jax.sharding import PartitionSpec as P

ROPE_BASE = 1000000.0
LN_EPS = 1e-5
NEG_BIG = -1e30
F32 = jnp.float32
BF16 = jnp.bfloat16
SQ = 4
QB = 8
NB = 4
CHUNK = SQ * QB
HEAD = 128
VMEM_LIMIT = 60 * 1024 * 1024


def dot(a, b):
    return lax.dot_general(a, b, (((1,), (0,)), ((), ())), preferred_element_type=F32)


def dot_nt(a, b):
    return lax.dot_general(a, b, (((1,), (1,)), ((), ())), preferred_element_type=F32)


def layer_norm(vectors, gain, shift):
    row_mean = jnp.mean(vectors, axis=-1, keepdims=True)
    centered = vectors - row_mean
    row_var = jnp.mean(centered * centered, axis=-1, keepdims=True)
    return centered * lax.rsqrt(row_var + LN_EPS) * gain + shift


def params(n_grid, **kw):
    return pltpu.CompilerParams(dimension_semantics=("arbitrary",) * n_grid, vmem_limit_bytes=VMEM_LIMIT, **kw)


def qkv_kernel(n_q, x_ref, vec_ref, wq_ref, wk_ref, wv_ref, cos_ref, sin_ref, q_ref, k_ref, v_ref, h_ref):
    step = pl.program_id(0)
    steps, batch = x_ref.shape[0], x_ref.shape[1]
    chunks = batch // CHUNK

    @pl.when(step == 0)
    def _():
        gain, shift = vec_ref[V_LN1G:V_LN1G + 1, :], vec_ref[V_LN1B:V_LN1B + 1, :]
        for s in range(steps):
            for r in range(0, batch, 32):
                h_ref[s * batch + r:s * batch + r + 32, :] = layer_norm(x_ref[s, r:r + 32, :].astype(F32), gain, shift).astype(BF16)

    def rope(vec, rows):
        vec = vec.astype(BF16).astype(F32)
        out = vec * cos_ref[rows, :] + pltpu.roll(vec, HEAD // 2, 1) * sin_ref[rows, :]
        return out.astype(BF16).astype(F32)

    @pl.when(step < n_q)
    def _():
        for s in range(steps):
            rows = slice(s * batch, (s + 1) * batch)
            acc = dot(h_ref[rows, :], wq_ref[...]) + vec_ref[V_QKV:V_QKV + 1, pl.ds(pl.multiple_of(step * 2 * HEAD, HEAD), 2 * HEAD)]
            for h in range(2):
                rot = rope(acc[:, h * HEAD:(h + 1) * HEAD], rows)
                for c in range(chunks):
                    q_ref[c, s, h] = rot[c * CHUNK:(c + 1) * CHUNK, :]

    @pl.when(step == n_q)
    def _():
        for s in range(steps):
            rows = slice(s * batch, (s + 1) * batch)
            hid = h_ref[rows, :]
            rot = rope(dot(hid, wk_ref[...]) + vec_ref[V_QKV:V_QKV + 1, 2 * n_q * HEAD:(2 * n_q + 1) * HEAD], rows)
            val = (dot(hid, wv_ref[...]) + vec_ref[V_QKV:V_QKV + 1, (2 * n_q + 1) * HEAD:(2 * n_q + 2) * HEAD]).astype(BF16).astype(F32)
            for c in range(chunks):
                k_ref[c, s] = rot[c * CHUNK:(c + 1) * CHUNK, :]
                v_ref[c, s] = val[c * CHUNK:(c + 1) * CHUNK, :]
        for s in range(steps, 8):
            for c in range(chunks):
                k_ref[c, s] = jnp.zeros((CHUNK, HEAD), F32)
                v_ref[c, s] = jnp.zeros((CHUNK, HEAD), F32)


def qkv(x_steps, vecs, w_q, w_k, w_v, cos_t, sin_t):
    steps, batch, dim = x_steps.shape
    chunks = batch // CHUNK
    heads = w_q.shape[1] // HEAD
    n_q = heads // 2
    whole = lambda *shape: pl.BlockSpec(shape, lambda j: (0,) * len(shape))
    last = n_q - 1
    return pl.pallas_call(
        functools.partial(qkv_kernel, n_q),
        grid=(n_q + 1,),
        in_specs=[
            whole(steps, batch, dim), whole(*vecs.shape),
            pl.BlockSpec((dim, 2 * HEAD), lambda j: (0, jnp.minimum(j, last))),
            whole(dim, HEAD), whole(dim, HEAD),
            whole(steps * batch, HEAD), whole(steps * batch, HEAD),
        ],
        out_specs=[
            pl.BlockSpec((chunks, steps, 2, CHUNK, HEAD), lambda j: (0, 0, jnp.minimum(j, last), 0, 0)),
            whole(chunks, 8, CHUNK, HEAD), whole(chunks, 8, CHUNK, HEAD),
        ],
        out_shape=[
            jax.ShapeDtypeStruct((chunks, steps, heads, CHUNK, HEAD), F32),
            jax.ShapeDtypeStruct((chunks, 8, CHUNK, HEAD), F32),
            jax.ShapeDtypeStruct((chunks, 8, CHUNK, HEAD), F32),
        ],
        scratch_shapes=[pltpu.VMEM((steps * batch, dim), BF16)],
        compiler_params=params(1),
        cost_estimate=pl.CostEstimate(flops=2 * steps * batch * dim * (w_q.shape[1] + 2 * HEAD), bytes_accessed=20_000_000, transcendentals=0),
        name="qkv",
    )(x_steps, vecs, w_q, w_k, w_v, cos_t, sin_t)


def attn_kernel(chunk, group, slots, n_any, info_ref, q_ref, kn_ref, vn_ref, k_ref, v_ref, *rest):
    ko_ref, vo_ref, o0_ref, o1_ref, o2_ref, o3_ref, o_scr = rest[n_any:]
    jj = pl.program_id(0)
    me = info_ref[0]
    rel = 3 - jj // 2
    part = jj % 2
    grp = jnp.bitwise_xor(me, rel) * 2 + part
    local = k_ref.shape[1]
    rows = 4 * group
    first_slot = me * local
    exp_scale = math.log2(math.e) * HEAD ** -0.5
    step_col = lax.broadcasted_iota(jnp.int32, (rows, 1), 0) // group
    lane = lax.broadcasted_iota(jnp.int32, (1, local), 1) + first_slot
    new_lane = lax.broadcasted_iota(jnp.int32, (1, 8), 1)
    diag = lax.broadcasted_iota(jnp.int32, (rows, HEAD), 0) == lax.broadcasted_iota(jnp.int32, (rows, HEAD), 1)
    order = [jnp.bitwise_and(jb + me, NB - 1) for jb in range(NB)]

    for jb in range(NB):
        bl = order[jb]
        seq = grp * NB + bl
        pos = info_ref[1 + chunk * CHUNK + seq]
        query = q_ref[0, pl.ds(seq, rows, stride=CHUNK), :].astype(BF16)
        keys = k_ref[bl]
        vals = v_ref[bl]
        ko_ref[bl] = keys
        vo_ref[bl] = vals
        age = jnp.where(lane < pos, jnp.bitwise_and(lane - pos, slots - 1), 0)
        scores = jnp.where(age > step_col, dot_nt(query, keys), NEG_BIG)
        part_max = jnp.max(scores, axis=1, keepdims=True)
        if jb == 0:
            new_keys = kn_ref[0, pl.ds(seq, 8, stride=CHUNK), :].astype(BF16)
            new_vals = vn_ref[0, pl.ds(seq, 8, stride=CHUNK), :].astype(BF16)
            new_scores = jnp.where(new_lane <= step_col, dot_nt(query, new_keys), NEG_BIG)
            part_max = jnp.maximum(part_max, jnp.max(new_scores, axis=1, keepdims=True))
        weights = jnp.exp2((scores - part_max) * exp_scale)
        part_sum = jnp.sum(weights, axis=1, keepdims=True)
        out = dot(weights.astype(BF16), vals)
        if jb == 0:
            new_weights = jnp.exp2((new_scores - part_max) * exp_scale)
            part_sum = part_sum + jnp.sum(new_weights, axis=1, keepdims=True)
            out = out + dot(new_weights.astype(BF16), new_vals)
        o_scr[pl.ds(pl.multiple_of(bl * rows, 8), rows), :] = out
        o_scr[pl.ds(NB * rows + bl, 1), :] = jnp.sum(jnp.where(diag, part_max, 0.0), axis=0, keepdims=True)
        o_scr[pl.ds(NB * rows + NB + bl, 1), :] = jnp.sum(jnp.where(diag, part_sum, 0.0), axis=0, keepdims=True)

    for r, o_ref in enumerate((o0_ref, o1_ref, o2_ref, o3_ref)):
        @pl.when(rel == r)
        def _(o_ref=o_ref):
            o_ref[part] = o_scr[...]

    row16 = lax.broadcasted_iota(jnp.int32, (16, HEAD), 0)
    for bl in range(NB):
        seq = grp * NB + bl
        pos = info_ref[1 + chunk * CHUNK + seq]
        begin = jnp.bitwise_and(pos, slots - 1) - first_slot
        near = jnp.bitwise_and(begin, slots - 1)

        @pl.when((near < local) | (near > slots - 4))
        def _(bl=bl, seq=seq, begin=begin):
            for t in range(4):
                slot = jnp.bitwise_and(begin + t, slots - 1)

                @pl.when(slot < local)
                def _(t=t, slot=slot):
                    base = pl.multiple_of(slot // 16 * 16, 16)
                    hit = row16 == slot % 16
                    for out_ref, new_ref in ((ko_ref, kn_ref), (vo_ref, vn_ref)):
                        new = new_ref[0, pl.ds(t * CHUNK + seq, 1), :]
                        old = out_ref[bl, pl.ds(base, 16), :].astype(F32)
                        out_ref[bl, pl.ds(base, 16), :] = jnp.where(hit, new, old).astype(BF16)


def attention(chunk, slots, info, q, kn, vn, k_cache, v_cache, outs, after):
    batch, local, _ = k_cache.shape
    chunks = batch // CHUNK
    group = q.shape[2]
    rows = 4 * group
    width = NB * rows + 2 * NB
    n_alias = 0 if outs is None else 2
    n_any = n_alias + len(after)

    def cache_map(jj, info_ref):
        rel = 3 - jj // 2
        return (chunk * (CHUNK // NB) + jnp.bitwise_xor(info_ref[0], rel) * 2 + jj % 2, 0, 0)

    cache_spec = pl.BlockSpec((NB, local, HEAD), cache_map)
    pick = lambda n: pl.BlockSpec((1, n, HEAD), lambda jj, info_ref: (chunk, 0, 0))
    part_spec = pl.BlockSpec((2, width, HEAD), lambda jj, info_ref: (0, 0, 0))
    part_shape = jax.ShapeDtypeStruct((2, width, HEAD), F32)
    cache_shape = jax.ShapeDtypeStruct(k_cache.shape, BF16)
    grid_spec = pltpu.PrefetchScalarGridSpec(
        num_scalar_prefetch=1,
        grid=(CHUNK // NB,),
        in_specs=[pick(rows * CHUNK), pick(8 * CHUNK), pick(8 * CHUNK), cache_spec, cache_spec] + [pl.BlockSpec(memory_space=pl.ANY)] * n_any,
        out_specs=[cache_spec, cache_spec] + [part_spec] * 4,
        scratch_shapes=[pltpu.VMEM((width, HEAD), F32)],
    )
    return pl.pallas_call(
        functools.partial(attn_kernel, chunk, group, slots, n_any),
        grid_spec=grid_spec,
        out_shape=[cache_shape, cache_shape] + [part_shape] * 4,
        input_output_aliases={6: 0, 7: 1} if n_alias else {},
        compiler_params=params(1),
        cost_estimate=pl.CostEstimate(flops=10_000_000_000, bytes_accessed=CHUNK * local * HEAD * 8, transcendentals=CHUNK * rows * local),
        name="attn",
    )(info, q.reshape(chunks, rows * CHUNK, HEAD), kn.reshape(chunks, 8 * CHUNK, HEAD), vn.reshape(chunks, 8 * CHUNK, HEAD), k_cache, v_cache, *(outs or ()), *after)


def combine_kernel(group, p0_ref, p1_ref, p2_ref, p3_ref, wo_ref, *rest):
    out_ref, a_scr, a32_scr, abf_scr = rest[-4:]
    rows = 4 * group
    exp_scale = math.log2(math.e) * HEAD ** -0.5

    @pl.when(pl.program_id(0) == 0)
    def _():
        parts = (p0_ref, p1_ref, p2_ref, p3_ref)
        for g in range(2):
            stats = [p[g, NB * rows:NB * rows + 2 * NB, :] for p in parts]
            top = functools.reduce(jnp.maximum, stats)
            scale = [jnp.exp2((st - top) * exp_scale) for st in stats]
            total = sum(sc * pltpu.roll(st, NB, 0) for sc, st in zip(scale, stats))
            scale = [(sc / total).T for sc in scale]
            for b in range(NB):
                acc = sum(p[g, b * rows:(b + 1) * rows, :] * sc[:rows, b:b + 1] for p, sc in zip(parts, scale))
                a_scr[pl.ds((g * NB + b) * rows, rows), :] = acc
        for s in range(4):
            for h in range(group):
                a32_scr[s * QB:(s + 1) * QB, h * HEAD:(h + 1) * HEAD] = a_scr[pl.ds(s * group + h, QB, stride=rows), :]
        abf_scr[...] = a32_scr[...].astype(BF16)

    out_ref[...] = dot(abf_scr[...], wo_ref[...])


def combine(parts, w_o, after):
    depth, dim = w_o.shape
    group = depth // HEAD
    n, block = 4, dim // 4
    part_spec = pl.BlockSpec(parts[0].shape, lambda j: (0, 0, 0))
    return pl.pallas_call(
        functools.partial(combine_kernel, group),
        grid=(n,),
        in_specs=[part_spec] * 4 + [pl.BlockSpec((depth, block), lambda j: (0, j))] + [pl.BlockSpec(memory_space=pl.ANY)] * len(after),
        out_specs=pl.BlockSpec((4 * QB, block), lambda j: (0, j)),
        out_shape=jax.ShapeDtypeStruct((4 * QB, dim), F32),
        scratch_shapes=[pltpu.VMEM((4 * group * QB, HEAD), F32), pltpu.VMEM((4 * QB, depth), F32), pltpu.VMEM((4 * QB, depth), BF16)],
        compiler_params=params(1),
        cost_estimate=pl.CostEstimate(flops=2_500_000_000, bytes_accessed=depth * dim * 2, transcendentals=0),
        name="combine_wo",
    )(*parts, w_o, *after)


MESH = pl.DeviceIdType.MESH
BLK = 512
V_LN1G, V_LN1B, V_BO, V_LN2G, V_LN2B, V_BPROJ, V_QKV, V_FC = range(8)


def tail_kernel(chunks, n_blk, x_ref, vec_ref, *refs):
    own, got = refs[:chunks], refs[chunks:2 * chunks]
    (wfc_ref, wproj_ref, ys_ref, xs, x1, hsend, hrecv, hall, g, wbuf, part, recv1, sums, recv2, ybuf, recv3, recv4, recv5,
     xsem, wsem, hs, hr, s1, r1, s2, r2, s3, r3, s4, r4, s5, r5) = refs[2 * chunks:]
    me = lax.axis_index("sq")
    core = lax.rem(me, 2)
    sib = {"sq": me + 1 - 2 * core}
    across = {"sq": lax.rem(me + 2, SQ)}
    partner = {"tp": 1 - lax.axis_index("tp")}
    rows = 4 * QB * chunks
    span = 4 * QB

    def remote(src, dst, send, recv, device):
        return pltpu.make_async_remote_copy(src_ref=src, dst_ref=dst, send_sem=send, recv_sem=recv, device_id=device, device_id_type=MESH)

    def weights(n, slot):
        if n < n_blk:
            src = wfc_ref.at[:, pl.ds(pl.multiple_of((core * n_blk + n) * BLK, BLK), BLK)]
        else:
            src = wproj_ref.at[pl.ds(pl.multiple_of(core * n_blk * BLK, BLK), n_blk * BLK), pl.ds((n - n_blk) * BLK, BLK)]
        return pltpu.make_async_copy(src, wbuf.at[slot], wsem.at[slot])

    x_copy = pltpu.make_async_copy(x_ref.at[:, :, me], xs, xsem)
    x_copy.start()
    for n in range(n_blk):
        weights(n, n).start()

    barrier = pltpu.get_barrier_semaphore()
    for device in (sib, across, partner):
        pl.semaphore_signal(barrier, inc=1, device_id=device, device_id_type=MESH)
    pl.semaphore_wait(barrier, 3)

    x_copy.wait()
    bias = vec_ref[V_BO:V_BO + 1, :]
    gain, shift = vec_ref[V_LN2G:V_LN2G + 1, :], vec_ref[V_LN2B:V_LN2B + 1, :]

    def send_h(c):
        return remote(hsend.at[c], hrecv.at[c], hs.at[c], hr.at[c], sib)

    for c in range(chunks):
        for s in range(4):
            at = slice(s * QB, (s + 1) * QB)
            mid = xs[s, c].astype(F32) + (own[c][at, :] + got[c][at, :]) + bias
            x1[c * span + s * QB:c * span + (s + 1) * QB, :] = mid.astype(BF16).astype(F32)
        h = layer_norm(x1[c * span:(c + 1) * span, :], gain, shift).astype(BF16)
        hall[c * span:(c + 1) * span, :] = h
        hsend[c] = h.astype(F32)
        send_h(c).start()
    for c in range(chunks):
        send_h(c).wait_recv()
        hall[rows + c * span:rows + (c + 1) * span, :] = hrecv[c].astype(BF16)

    for n in range(n_blk):
        weights(n, n).wait()
        cols = slice(n * BLK, (n + 1) * BLK)
        acc = dot(hall[...], wbuf[n]) + vec_ref[pl.ds(V_FC + core, 1), cols]
        g[:, cols] = jax.nn.gelu(acc, approximate=True).astype(BF16)
        weights(n_blk + n, n).start()

    def send1(j):
        return remote(part.at[j], recv1.at[j], s1.at[j], r1.at[j], sib)

    def send2(j):
        return remote(sums.at[j], recv2.at[j], s2.at[j], r2.at[j], partner)

    def send3(j):
        return remote(ybuf.at[j], recv3.at[j], s3.at[j], r3.at[j], across)

    def send4(j):
        return remote(ybuf.at[j], recv4.at[j], s4.at[j], r4.at[j], sib)

    def send5(j):
        return remote(recv3.at[j], recv5.at[j], s5.at[j], r5.at[j], sib)

    def reduce_cores(j):
        send1(j).wait_recv()
        sums[j] = sums[j] + recv1[j]
        send2(j).start()

    for j in range(n_blk):
        weights(n_blk + j, j).wait()
        acc = dot(g[...], wbuf[j])
        part[j] = acc[rows:, :]
        send1(j).start()
        sums[j] = acc[:rows, :]
        if j:
            reduce_cores(j - 1)
    reduce_cores(n_blk - 1)

    def store_rows(j, value, owner):
        for c in range(chunks):
            for s in range(4):
                ys_ref[s, c, owner, :, j * BLK:(j + 1) * BLK] = value[c * span + s * QB:c * span + (s + 1) * QB, :].astype(BF16)

    def late(j):
        send3(j).wait_recv()
        send5(j).start()
        store_rows(j, recv3[j], lax.rem(me + 2, SQ))
        send4(j).wait_recv()
        store_rows(j, recv4[j], me + 1 - 2 * core)
        send5(j).wait_recv()
        store_rows(j, recv5[j], lax.rem(me + 1 - 2 * core + 2, SQ))

    for j in range(n_blk):
        cols = slice(j * BLK, (j + 1) * BLK)
        send2(j).wait_recv()
        ybuf[j] = (x1[:, cols] + (sums[j] + recv2[j]) + vec_ref[V_BPROJ:V_BPROJ + 1, cols]).astype(BF16).astype(F32)
        send3(j).start()
        send4(j).start()
        store_rows(j, ybuf[j], me)
        if j:
            late(j - 1)
    late(n_blk - 1)

    for c in range(chunks):
        send_h(c).wait_send()
    for j in range(n_blk):
        for send in (send1, send2, send3, send4, send5):
            send(j).wait_send()


def tail(x_view, vecs, own, got, w_fc, w_proj):
    steps, chunks, _, _, dim = x_view.shape
    half = w_fc.shape[1] // 2
    n_blk = half // BLK
    rows = 4 * QB * chunks
    any_spec = pl.BlockSpec(memory_space=pl.ANY)
    vmem = pl.BlockSpec(memory_space=pltpu.VMEM)
    blocks = lambda: pltpu.VMEM((n_blk, rows, BLK), F32)
    sem = lambda n: pltpu.SemaphoreType.DMA((n,))
    return pl.pallas_call(
        functools.partial(tail_kernel, chunks, n_blk),
        in_specs=[any_spec, vmem] + [vmem] * (2 * chunks) + [any_spec, any_spec],
        out_specs=vmem,
        out_shape=jax.ShapeDtypeStruct((steps, chunks, SQ, QB, dim), BF16),
        scratch_shapes=[
            pltpu.VMEM((steps, chunks, QB, dim), BF16), pltpu.VMEM((rows, dim), F32),
            pltpu.VMEM((chunks, 4 * QB, dim), F32), pltpu.VMEM((chunks, 4 * QB, dim), F32),
            pltpu.VMEM((2 * rows, dim), BF16), pltpu.VMEM((2 * rows, half), BF16), pltpu.VMEM((n_blk, dim, BLK), BF16),
        ] + [blocks() for _ in range(8)] + [pltpu.SemaphoreType.DMA, sem(n_blk), sem(chunks), sem(chunks)] + [sem(n_blk) for _ in range(10)],
        compiler_params=pltpu.CompilerParams(vmem_limit_bytes=VMEM_LIMIT, collective_id=0, has_side_effects=True),
        cost_estimate=pl.CostEstimate(flops=40_000_000_000, bytes_accessed=dim * half * 4, transcendentals=0),
        name="tail",
    )(x_view, vecs, *own, *got, w_fc, w_proj)


def solution(mesh):
    act_spec = P(None, "dp", None)
    cache_spec = P("dp", "sq", "tp", None)
    col_spec = P(None, "tp")
    row_spec = P("tp", None)
    vec_spec = P("tp")
    rep_spec = P(None)
    in_specs = (act_spec, P("dp"), cache_spec, cache_spec, col_spec, vec_spec, col_spec, vec_spec,
                col_spec, vec_spec, row_spec, rep_spec, rep_spec, rep_spec, rep_spec, rep_spec,
                col_spec, vec_spec, row_spec, rep_spec)
    out_specs = (act_spec, cache_spec, cache_spec)

    def swap_sq(value, mask):
        return lax.ppermute(value, "sq", [(i, i ^ mask) for i in range(SQ)])

    def swap_tp(value):
        return lax.ppermute(value, "tp", [(0, 1), (1, 0)])

    def per_device(x_steps, positions, key_buf, val_buf, w_q, b_q, w_k, b_k, w_v, b_v, w_o, b_o,
                   ln1_gain, ln1_bias, ln2_gain, ln2_bias, w_fc, b_fc, w_proj, b_proj):
        steps, batch, dim = x_steps.shape
        local = key_buf.shape[1]
        slots = local * SQ
        chunks = batch // CHUNK
        me = lax.axis_index("sq").astype(jnp.int32)
        info = jnp.concatenate([me[None], positions])
        inv_freq = jnp.power(F32(ROPE_BASE), -2.0 * jnp.arange(HEAD // 2, dtype=F32) / HEAD)
        cur = positions[None, :] + jnp.arange(steps, dtype=jnp.int32)[:, None]
        angle = cur.reshape(-1).astype(F32)[:, None] * inv_freq
        cos_t, sin_t = jnp.cos(angle), jnp.sin(angle)
        cos_t = jnp.concatenate([cos_t, cos_t], axis=-1)
        sin_t = jnp.concatenate([-sin_t, sin_t], axis=-1)
        row = lambda *vs: jnp.pad(jnp.concatenate(vs), (0, -sum(v.shape[0] for v in vs) % dim))
        vecs = jnp.concatenate([ln1_gain, ln1_bias, b_o, ln2_gain, ln2_bias, b_proj, row(b_q, b_k, b_v), b_fc]).astype(F32).reshape(-1, dim)
        q, kn, vn = qkv(x_steps, vecs, w_q, w_k, w_v, cos_t, sin_t)
        k_old, v_old = key_buf.reshape(batch, local, HEAD), val_buf.reshape(batch, local, HEAD)
        x_view = x_steps.reshape(steps, chunks, SQ, QB, dim)

        caches = None
        own, got = [], []
        waiting = None
        for c in range(chunks):
            res = attention(c, slots, info, q, kn, vn, k_old, v_old, caches, own[c - 2:c - 1] if c >= 2 else [])
            caches = res[:2]
            if waiting is not None:
                own.append(combine(waiting, w_o, res[2:3]))
                got.append(swap_tp(own[-1]))
            waiting = [res[2]] + [swap_sq(res[2 + r], r) for r in range(1, SQ)]
        own.append(combine(waiting, w_o, []))
        got.append(swap_tp(own[-1]))
        ys = tail(x_view, vecs, own, got, w_fc, w_proj).reshape(steps, batch, dim)
        return ys, caches[0].reshape(key_buf.shape), caches[1].reshape(val_buf.shape)

    return jax.shard_map(per_device, mesh=mesh, in_specs=in_specs, out_specs=out_specs, check_vma=False)
```

```python
import functools
import math

import jax
import jax.numpy as jnp
from jax import lax
from jax.experimental import pallas as pl
from jax.experimental.pallas import tpu as pltpu
from jax.sharding import PartitionSpec as P

ROPE_BASE = 1000000.0
LN_EPS = 1e-5
NEG_BIG = -1e30
F32 = jnp.float32
BF16 = jnp.bfloat16
SQ = 4
QB = 8
NB = 4
CHUNK = SQ * QB
HEAD = 128
VMEM_LIMIT = 60 * 1024 * 1024


def dot(a, b):
    return lax.dot_general(a, b, (((1,), (0,)), ((), ())), preferred_element_type=F32)


def dot_nt(a, b):
    return lax.dot_general(a, b, (((1,), (1,)), ((), ())), preferred_element_type=F32)


def layer_norm(vectors, gain, shift):
    row_mean = jnp.mean(vectors, axis=-1, keepdims=True)
    centered = vectors - row_mean
    row_var = jnp.mean(centered * centered, axis=-1, keepdims=True)
    return centered * lax.rsqrt(row_var + LN_EPS) * gain + shift


def params(n_grid, **kw):
    return pltpu.CompilerParams(dimension_semantics=("arbitrary",) * n_grid, vmem_limit_bytes=VMEM_LIMIT, **kw)


def as_row(ref):
    return ref[...].astype(F32).reshape(1, -1)


def qkv_kernel(n_q, x_ref, gain_ref, shift_ref, wq_ref, bq_ref, wk_ref, bk_ref, wv_ref, bv_ref, cos_ref, sin_ref,
               q_ref, k_ref, v_ref, h_ref, bias, cos_t, sin_t):
    step = pl.program_id(0)
    steps, batch = x_ref.shape[0], x_ref.shape[1]
    chunks = batch // CHUNK

    @pl.when(step == 0)
    def _():
        gain, shift = as_row(gain_ref), as_row(shift_ref)
        bias[...] = as_row(bq_ref)
        cos_t[...] = jnp.concatenate([cos_ref[...], cos_ref[...]], axis=1)
        sin_t[...] = jnp.concatenate([-sin_ref[...], sin_ref[...]], axis=1)
        for s in range(steps):
            for r in range(0, batch, 32):
                h_ref[s * batch + r:s * batch + r + 32, :] = layer_norm(x_ref[s, r:r + 32, :].astype(F32), gain, shift).astype(BF16)

    def rope(vec, rows):
        vec = vec.astype(BF16).astype(F32)
        out = vec * cos_t[rows, :] + pltpu.roll(vec, HEAD // 2, 1) * sin_t[rows, :]
        return out.astype(BF16).astype(F32)

    @pl.when(step < n_q)
    def _():
        acc = dot(h_ref[...], wq_ref[...]) + bias[:, pl.ds(pl.multiple_of(step * 2 * HEAD, HEAD), 2 * HEAD)]
        for s in range(steps):
            for c in range(chunks):
                rows = slice(s * batch + c * CHUNK, s * batch + (c + 1) * CHUNK)
                for h in range(2):
                    q_ref[c, s, h] = rope(acc[rows, h * HEAD:(h + 1) * HEAD], rows)

    @pl.when(step == n_q)
    def _():
        acc = dot(h_ref[...], jnp.concatenate([wk_ref[...], wv_ref[...]], axis=1))
        acc = acc + jnp.concatenate([as_row(bk_ref), as_row(bv_ref)], axis=1)
        for s in range(steps):
            for c in range(chunks):
                rows = slice(s * batch + c * CHUNK, s * batch + (c + 1) * CHUNK)
                k_ref[c, s] = rope(acc[rows, :HEAD], rows)
                v_ref[c, s] = acc[rows, HEAD:].astype(BF16).astype(F32)
        for s in range(steps, 8):
            for c in range(chunks):
                k_ref[c, s] = jnp.zeros((CHUNK, HEAD), F32)
                v_ref[c, s] = jnp.zeros((CHUNK, HEAD), F32)


def qkv(x_steps, gain, shift, w_q, b_q, w_k, b_k, w_v, b_v, cos_t, sin_t):
    steps, batch, dim = x_steps.shape
    chunks = batch // CHUNK
    heads = w_q.shape[1] // HEAD
    n_q = heads // 2
    whole = lambda *shape: pl.BlockSpec(shape, lambda j: (0,) * len(shape))
    last = n_q - 1
    rows = steps * batch
    return pl.pallas_call(
        functools.partial(qkv_kernel, n_q),
        grid=(n_q + 1,),
        in_specs=[
            whole(steps, batch, dim), whole(dim), whole(dim),
            pl.BlockSpec((dim, 2 * HEAD), lambda j: (0, jnp.minimum(j, last))), whole(heads * HEAD),
            whole(dim, HEAD), whole(HEAD), whole(dim, HEAD), whole(HEAD),
            whole(rows, HEAD // 2), whole(rows, HEAD // 2),
        ],
        out_specs=[
            pl.BlockSpec((chunks, steps, 2, CHUNK, HEAD), lambda j: (0, 0, jnp.minimum(j, last), 0, 0)),
            whole(chunks, 8, CHUNK, HEAD), whole(chunks, 8, CHUNK, HEAD),
        ],
        out_shape=[
            jax.ShapeDtypeStruct((chunks, steps, heads, CHUNK, HEAD), F32),
            jax.ShapeDtypeStruct((chunks, 8, CHUNK, HEAD), F32),
            jax.ShapeDtypeStruct((chunks, 8, CHUNK, HEAD), F32),
        ],
        scratch_shapes=[pltpu.VMEM((rows, dim), BF16), pltpu.VMEM((1, heads * HEAD), F32), pltpu.VMEM((rows, HEAD), F32), pltpu.VMEM((rows, HEAD), F32)],
        compiler_params=params(1),
        cost_estimate=pl.CostEstimate(flops=2 * rows * dim * (heads + 2) * HEAD, bytes_accessed=20_000_000, transcendentals=0),
        name="qkv",
    )(x_steps, gain, shift, w_q, b_q, w_k, b_k, w_v, b_v, cos_t, sin_t)


def attn_kernel(chunk, group, slots, n_any, pos_ref, q_hbm, kn_hbm, vn_hbm, k_hbm, v_hbm, *rest):
    ko_hbm, vo_hbm, *outs = rest[n_any:n_any + 6]
    kbuf, vbuf, q_ref, kn_ref, vn_ref, o_all, in_sem, out_sem, small_sem = rest[n_any + 6:]
    me = lax.axis_index("sq").astype(jnp.int32)
    n = CHUNK // NB
    local = kbuf.shape[2]
    rows = 4 * group
    first_slot = me * local
    exp_scale = math.log2(math.e) * HEAD ** -0.5
    step_col = lax.broadcasted_iota(jnp.int32, (rows, 1), 0) // group
    lane = lax.broadcasted_iota(jnp.int32, (1, local), 1) + first_slot
    new_lane = lax.broadcasted_iota(jnp.int32, (1, 8), 1)
    diag = lax.broadcasted_iota(jnp.int32, (rows, HEAD), 0) == lax.broadcasted_iota(jnp.int32, (rows, HEAD), 1)
    row16 = lax.broadcasted_iota(jnp.int32, (16, HEAD), 0)

    def place(i):
        rel = 3 - i // 2
        return jnp.bitwise_xor(me, rel) * 2 + i % 2

    def seqs(i):
        return pl.ds(chunk * CHUNK + place(i) * NB, NB)

    def loads(i):
        return (pltpu.make_async_copy(k_hbm.at[seqs(i)], kbuf.at[i], in_sem.at[0, i]),
                pltpu.make_async_copy(v_hbm.at[seqs(i)], vbuf.at[i], in_sem.at[1, i]))

    def stores(i):
        return (pltpu.make_async_copy(kbuf.at[i], ko_hbm.at[seqs(i)], out_sem.at[0, i]),
                pltpu.make_async_copy(vbuf.at[i], vo_hbm.at[seqs(i)], out_sem.at[1, i]))

    small = [pltpu.make_async_copy(src.at[chunk], dst, small_sem.at[4 + t]) for t, (src, dst) in enumerate(((q_hbm, q_ref), (kn_hbm, kn_ref), (vn_hbm, vn_ref)))]
    for copy in small:
        copy.start()
    for i in range(n):
        for copy in loads(i):
            copy.start()
    for copy in small:
        copy.wait()

    def body(i, carry):
        for copy in loads(i):
            copy.wait()

        @pl.when(i > 0)
        def _():
            for copy in stores(i - 1):
                copy.start()

        grp = place(i)
        out_at = o_all.at[3 - i // 2, i % 2]
        for jb in range(NB):
            bl = jnp.bitwise_and(jb + me, NB - 1)
            seq = grp * NB + bl
            pos = pos_ref[chunk * CHUNK + seq]
            query = q_ref[pl.ds(seq, rows, stride=CHUNK), :].astype(BF16)
            keys = kbuf[i, bl]
            vals = vbuf[i, bl]
            age = jnp.where(lane < pos, jnp.bitwise_and(lane - pos, slots - 1), 0)
            scores = jnp.where(age > step_col, dot_nt(query, keys), NEG_BIG)
            part_max = jnp.max(scores, axis=1, keepdims=True)
            if jb == 0:
                new_keys = kn_ref[pl.ds(seq, 8, stride=CHUNK), :].astype(BF16)
                new_vals = vn_ref[pl.ds(seq, 8, stride=CHUNK), :].astype(BF16)
                new_scores = jnp.where(new_lane <= step_col, dot_nt(query, new_keys), NEG_BIG)
                part_max = jnp.maximum(part_max, jnp.max(new_scores, axis=1, keepdims=True))
            weights = jnp.exp2((scores - part_max) * exp_scale)
            part_sum = jnp.sum(weights, axis=1, keepdims=True)
            out = dot(weights.astype(BF16), vals)
            if jb == 0:
                new_weights = jnp.exp2((new_scores - part_max) * exp_scale)
                part_sum = part_sum + jnp.sum(new_weights, axis=1, keepdims=True)
                out = out + dot(new_weights.astype(BF16), new_vals)
            out_at[pl.ds(pl.multiple_of(bl * rows, 8), rows), :] = out
            out_at[pl.ds(NB * rows + bl, 1), :] = jnp.sum(jnp.where(diag, part_max, 0.0), axis=0, keepdims=True)
            out_at[pl.ds(NB * rows + NB + bl, 1), :] = jnp.sum(jnp.where(diag, part_sum, 0.0), axis=0, keepdims=True)

        for bl in range(NB):
            seq = grp * NB + bl
            begin = jnp.bitwise_and(pos_ref[chunk * CHUNK + seq], slots - 1) - first_slot
            near = jnp.bitwise_and(begin, slots - 1)

            @pl.when((near < local) | (near > slots - 4))
            def _(bl=bl, seq=seq, begin=begin):
                for t in range(4):
                    slot = jnp.bitwise_and(begin + t, slots - 1)

                    @pl.when(slot < local)
                    def _(t=t, slot=slot):
                        window = pl.ds(pl.multiple_of(slot // 16 * 16, 16), 16)
                        hit = row16 == slot % 16
                        for buf, new_ref in ((kbuf, kn_ref), (vbuf, vn_ref)):
                            new = new_ref[pl.ds(t * CHUNK + seq, 1), :]
                            buf[i, bl, window, :] = jnp.where(hit, new, buf[i, bl, window, :].astype(F32)).astype(BF16)

        return carry

    lax.fori_loop(0, n, body, 0)
    tails = [pltpu.make_async_copy(o_all.at[r], outs[r], small_sem.at[r]) for r in range(4)]
    for copy in tails + list(stores(n - 1)):
        copy.start()
    for i in range(n):
        for copy in stores(i):
            copy.wait()
    for copy in tails:
        copy.wait()


def attention(chunk, slots, positions, q, kn, vn, k_cache, v_cache, outs, after):
    batch, local, _ = k_cache.shape
    chunks = batch // CHUNK
    group = q.shape[2]
    rows = 4 * group
    n = CHUNK // NB
    width = NB * rows + 2 * NB
    n_alias = 0 if outs is None else 2
    n_any = n_alias + len(after)
    any_spec = pl.BlockSpec(memory_space=pl.ANY)
    part_shape = jax.ShapeDtypeStruct((2, width, HEAD), F32)
    cache_shape = jax.ShapeDtypeStruct(k_cache.shape, BF16)
    return pl.pallas_call(
        functools.partial(attn_kernel, chunk, group, slots, n_any),
        in_specs=[pl.BlockSpec(memory_space=pltpu.SMEM)] + [any_spec] * (5 + n_any),
        out_specs=[any_spec] * 6,
        out_shape=[cache_shape, cache_shape] + [part_shape] * 4,
        scratch_shapes=[
            pltpu.VMEM((n, NB, local, HEAD), BF16), pltpu.VMEM((n, NB, local, HEAD), BF16),
            pltpu.VMEM((rows * CHUNK, HEAD), F32), pltpu.VMEM((8 * CHUNK, HEAD), F32), pltpu.VMEM((8 * CHUNK, HEAD), F32),
            pltpu.VMEM((4, 2, width, HEAD), F32),
            pltpu.SemaphoreType.DMA((2, n)), pltpu.SemaphoreType.DMA((2, n)), pltpu.SemaphoreType.DMA((7,)),
        ],
        input_output_aliases={6: 0, 7: 1} if n_alias else {},
        compiler_params=pltpu.CompilerParams(vmem_limit_bytes=VMEM_LIMIT),
        cost_estimate=pl.CostEstimate(flops=10_000_000_000, bytes_accessed=CHUNK * local * HEAD * 8, transcendentals=CHUNK * rows * local),
        name="attn",
    )(positions, q.reshape(chunks, rows * CHUNK, HEAD), kn.reshape(chunks, 8 * CHUNK, HEAD), vn.reshape(chunks, 8 * CHUNK, HEAD), k_cache, v_cache, *(outs or ()), *after)


def combine_kernel(group, p0_hbm, p1_hbm, p2_hbm, p3_hbm, wo_hbm, *rest):
    out_ref, parts, a_scr, a32_scr, wbuf, psem, wsem = rest[-7:]
    rows = 4 * group
    exp_scale = math.log2(math.e) * HEAD ** -0.5
    n, _, block = wbuf.shape
    gets = [pltpu.make_async_copy(p, parts.at[i], psem.at[i]) for i, p in enumerate((p0_hbm, p1_hbm, p2_hbm, p3_hbm))]
    weights = [pltpu.make_async_copy(wo_hbm.at[:, pl.ds(j * block, block)], wbuf.at[j], wsem.at[j]) for j in range(n)]
    for copy in gets + weights:
        copy.start()
    for copy in gets:
        copy.wait()
    for g in range(2):
        stats = [parts[i, g, NB * rows:NB * rows + 2 * NB, :] for i in range(SQ)]
        top = functools.reduce(jnp.maximum, stats)
        scale = [jnp.exp2((st - top) * exp_scale) for st in stats]
        total = sum(sc * pltpu.roll(st, NB, 0) for sc, st in zip(scale, stats))
        scale = [(sc / total).T for sc in scale]
        for b in range(NB):
            acc = sum(parts[i, g, b * rows:(b + 1) * rows, :] * sc[:rows, b:b + 1] for i, sc in enumerate(scale))
            a_scr[pl.ds((g * NB + b) * rows, rows), :] = acc
    for s in range(4):
        for h in range(group):
            a32_scr[s * QB:(s + 1) * QB, h * HEAD:(h + 1) * HEAD] = a_scr[pl.ds(s * group + h, QB, stride=rows), :]
    for j in range(n):
        weights[j].wait()
        out_ref[:, j * block:(j + 1) * block] = dot(a32_scr[...].astype(BF16), wbuf[j])


def combine(parts, w_o, after):
    depth, dim = w_o.shape
    group = depth // HEAD
    n, block = 6, dim // 6
    any_spec = pl.BlockSpec(memory_space=pl.ANY)
    return pl.pallas_call(
        functools.partial(combine_kernel, group),
        in_specs=[any_spec] * (5 + len(after)),
        out_specs=pl.BlockSpec(memory_space=pltpu.VMEM),
        out_shape=jax.ShapeDtypeStruct((4 * QB, dim), F32),
        scratch_shapes=[
            pltpu.VMEM((SQ,) + parts[0].shape, F32), pltpu.VMEM((4 * group * QB, HEAD), F32), pltpu.VMEM((4 * QB, depth), F32),
            pltpu.VMEM((n, depth, block), BF16), pltpu.SemaphoreType.DMA((SQ,)), pltpu.SemaphoreType.DMA((n,)),
        ],
        compiler_params=pltpu.CompilerParams(vmem_limit_bytes=VMEM_LIMIT),
        cost_estimate=pl.CostEstimate(flops=2_500_000_000, bytes_accessed=depth * dim * 2, transcendentals=0),
        name="combine_wo",
    )(*parts, w_o, *after)


MESH = pl.DeviceIdType.MESH
BLK = 512


def tail_kernel(chunks, n_blk, x_ref, bo_ref, gain_ref, shift_ref, bproj_ref, bfc_ref, *refs):
    own, got = refs[:chunks], refs[chunks:2 * chunks]
    (wfc_ref, wproj_ref, ys_ref, xs, x1, hsend, hrecv, hall, g, wbuf, bproj, bfc, part, recv1, sums, recv2, ybuf, recv3, recv4, recv5,
     xsem, wsem, hs, hr, s1, r1, s2, r2, s3, r3, s4, r4, s5, r5) = refs[2 * chunks:]
    me = lax.axis_index("sq")
    core = lax.rem(me, 2)
    sib = {"sq": me + 1 - 2 * core}
    across = {"sq": lax.rem(me + 2, SQ)}
    partner = {"tp": 1 - lax.axis_index("tp")}
    rows = 4 * QB * chunks
    span = 4 * QB

    def remote(src, dst, send, recv, device):
        return pltpu.make_async_remote_copy(src_ref=src, dst_ref=dst, send_sem=send, recv_sem=recv, device_id=device, device_id_type=MESH)

    def weights(n, slot):
        if n < n_blk:
            src = wfc_ref.at[:, pl.ds(pl.multiple_of((core * n_blk + n) * BLK, BLK), BLK)]
        else:
            src = wproj_ref.at[pl.ds(pl.multiple_of(core * n_blk * BLK, BLK), n_blk * BLK), pl.ds((n - n_blk) * BLK, BLK)]
        return pltpu.make_async_copy(src, wbuf.at[slot], wsem.at[slot])

    x_copy = pltpu.make_async_copy(x_ref.at[:, :, me], xs, xsem)
    x_copy.start()
    for n in range(n_blk):
        weights(n, n).start()

    barrier = pltpu.get_barrier_semaphore()
    for device in (sib, across, partner):
        pl.semaphore_signal(barrier, inc=1, device_id=device, device_id_type=MESH)
    pl.semaphore_wait(barrier, 3)

    x_copy.wait()
    bias, gain, shift = as_row(bo_ref), as_row(gain_ref), as_row(shift_ref)
    bproj[...] = as_row(bproj_ref)
    bfc[...] = as_row(bfc_ref)

    def send_h(c):
        return remote(hsend.at[c], hrecv.at[c], hs.at[c], hr.at[c], sib)

    for c in range(chunks):
        for s in range(4):
            at = slice(s * QB, (s + 1) * QB)
            mid = xs[s, c].astype(F32) + (own[c][at, :] + got[c][at, :]) + bias
            x1[c * span + s * QB:c * span + (s + 1) * QB, :] = mid.astype(BF16).astype(F32)
        h = layer_norm(x1[c * span:(c + 1) * span, :], gain, shift).astype(BF16)
        hall[c * span:(c + 1) * span, :] = h
        hsend[c] = h.astype(F32)
        send_h(c).start()
    for c in range(chunks):
        send_h(c).wait_recv()
        hall[rows + c * span:rows + (c + 1) * span, :] = hrecv[c].astype(BF16)

    for n in range(n_blk):
        weights(n, n).wait()
        cols = slice(n * BLK, (n + 1) * BLK)
        acc = dot(hall[...], wbuf[n]) + bfc[:, pl.ds(pl.multiple_of((core * n_blk + n) * BLK, BLK), BLK)]
        g[:, cols] = jax.nn.gelu(acc, approximate=True).astype(BF16)
        weights(n_blk + n, n).start()

    def send1(j):
        return remote(part.at[j], recv1.at[j], s1.at[j], r1.at[j], sib)

    def send2(j):
        return remote(sums.at[j], recv2.at[j], s2.at[j], r2.at[j], partner)

    def send3(j):
        return remote(ybuf.at[j], recv3.at[j], s3.at[j], r3.at[j], across)

    def send4(j):
        return remote(ybuf.at[j], recv4.at[j], s4.at[j], r4.at[j], sib)

    def send5(j):
        return remote(recv3.at[j], recv5.at[j], s5.at[j], r5.at[j], sib)

    def reduce_cores(j):
        send1(j).wait_recv()
        sums[j] = sums[j] + recv1[j]
        send2(j).start()

    for j in range(n_blk):
        weights(n_blk + j, j).wait()
        acc = dot(g[...], wbuf[j])
        part[j] = acc[rows:, :]
        send1(j).start()
        sums[j] = acc[:rows, :]
        if j:
            reduce_cores(j - 1)
    reduce_cores(n_blk - 1)

    def store_rows(j, value, owner):
        for c in range(chunks):
            for s in range(4):
                ys_ref[s, c, owner, :, j * BLK:(j + 1) * BLK] = value[c * span + s * QB:c * span + (s + 1) * QB, :].astype(BF16)

    def late(j):
        send3(j).wait_recv()
        send5(j).start()
        store_rows(j, recv3[j], lax.rem(me + 2, SQ))
        send4(j).wait_recv()
        store_rows(j, recv4[j], me + 1 - 2 * core)
        send5(j).wait_recv()
        store_rows(j, recv5[j], lax.rem(me + 1 - 2 * core + 2, SQ))

    for j in range(n_blk):
        cols = slice(j * BLK, (j + 1) * BLK)
        send2(j).wait_recv()
        ybuf[j] = (x1[:, cols] + (sums[j] + recv2[j]) + bproj[:, cols]).astype(BF16).astype(F32)
        send3(j).start()
        send4(j).start()
        store_rows(j, ybuf[j], me)
        if j:
            late(j - 1)
    late(n_blk - 1)

    for c in range(chunks):
        send_h(c).wait_send()
    for j in range(n_blk):
        for send in (send1, send2, send3, send4, send5):
            send(j).wait_send()


def tail(x_view, vectors, own, got, w_fc, w_proj):
    steps, chunks, _, _, dim = x_view.shape
    half = w_fc.shape[1] // 2
    n_blk = half // BLK
    rows = 4 * QB * chunks
    any_spec = pl.BlockSpec(memory_space=pl.ANY)
    vmem = pl.BlockSpec(memory_space=pltpu.VMEM)
    blocks = lambda: pltpu.VMEM((n_blk, rows, BLK), F32)
    sem = lambda n: pltpu.SemaphoreType.DMA((n,))
    return pl.pallas_call(
        functools.partial(tail_kernel, chunks, n_blk),
        in_specs=[any_spec] + [vmem] * len(vectors) + [vmem] * (2 * chunks) + [any_spec, any_spec],
        out_specs=vmem,
        out_shape=jax.ShapeDtypeStruct((steps, chunks, SQ, QB, dim), BF16),
        scratch_shapes=[
            pltpu.VMEM((steps, chunks, QB, dim), BF16), pltpu.VMEM((rows, dim), F32),
            pltpu.VMEM((chunks, 4 * QB, dim), F32), pltpu.VMEM((chunks, 4 * QB, dim), F32),
            pltpu.VMEM((2 * rows, dim), BF16), pltpu.VMEM((2 * rows, half), BF16), pltpu.VMEM((n_blk, dim, BLK), BF16),
            pltpu.VMEM((1, dim), F32), pltpu.VMEM((1, 2 * half), F32),
        ] + [blocks() for _ in range(8)] + [pltpu.SemaphoreType.DMA, sem(n_blk), sem(chunks), sem(chunks)] + [sem(n_blk) for _ in range(10)],
        compiler_params=pltpu.CompilerParams(vmem_limit_bytes=VMEM_LIMIT, collective_id=0, has_side_effects=True),
        cost_estimate=pl.CostEstimate(flops=40_000_000_000, bytes_accessed=dim * half * 4, transcendentals=0),
        name="tail",
    )(x_view, *vectors, *own, *got, w_fc, w_proj)


def solution(mesh):
    act_spec = P(None, "dp", None)
    cache_spec = P("dp", "sq", "tp", None)
    col_spec = P(None, "tp")
    row_spec = P("tp", None)
    vec_spec = P("tp")
    rep_spec = P(None)
    in_specs = (act_spec, P("dp"), cache_spec, cache_spec, col_spec, vec_spec, col_spec, vec_spec,
                col_spec, vec_spec, row_spec, rep_spec, rep_spec, rep_spec, rep_spec, rep_spec,
                col_spec, vec_spec, row_spec, rep_spec)
    out_specs = (act_spec, cache_spec, cache_spec)

    def swap_sq(value, mask):
        return lax.ppermute(value, "sq", [(i, i ^ mask) for i in range(SQ)])

    def swap_tp(value):
        return lax.ppermute(value, "tp", [(0, 1), (1, 0)])

    def per_device(x_steps, positions, key_buf, val_buf, w_q, b_q, w_k, b_k, w_v, b_v, w_o, b_o,
                   ln1_gain, ln1_bias, ln2_gain, ln2_bias, w_fc, b_fc, w_proj, b_proj):
        steps, batch, dim = x_steps.shape
        local = key_buf.shape[1]
        slots = local * SQ
        chunks = batch // CHUNK
        inv_freq = jnp.power(F32(ROPE_BASE), -2.0 * jnp.arange(HEAD // 2, dtype=F32) / HEAD)
        cur = positions[None, :] + jnp.arange(steps, dtype=jnp.int32)[:, None]
        angle = cur.reshape(-1).astype(F32)[:, None] * inv_freq
        q, kn, vn = qkv(x_steps, ln1_gain, ln1_bias, w_q, b_q, w_k, b_k, w_v, b_v, jnp.cos(angle), jnp.sin(angle))
        k_old, v_old = key_buf.reshape(batch, local, HEAD), val_buf.reshape(batch, local, HEAD)
        x_view = x_steps.reshape(steps, chunks, SQ, QB, dim)

        caches = None
        own, got = [], []
        waiting = None
        for c in range(chunks):
            res = attention(c, slots, positions, q, kn, vn, k_old, v_old, caches, own[c - 2:c - 1] if c >= 2 else [])
            caches = res[:2]
            if waiting is not None:
                own.append(combine(waiting, w_o, res[2:3]))
                got.append(swap_tp(own[-1]))
            waiting = [res[2]] + [swap_sq(res[2 + r], r) for r in range(1, SQ)]
        own.append(combine(waiting, w_o, []))
        got.append(swap_tp(own[-1]))
        ys = tail(x_view, (b_o, ln2_gain, ln2_bias, b_proj, b_fc), own, got, w_fc, w_proj).reshape(steps, batch, dim)
        return ys, caches[0].reshape(key_buf.shape), caches[1].reshape(val_buf.shape)

    return jax.shard_map(per_device, mesh=mesh, in_specs=in_specs, out_specs=out_specs, check_vma=False)
```

```python
import functools
import math

import jax
import jax.numpy as jnp
from jax import lax
from jax.experimental import pallas as pl
from jax.experimental.pallas import tpu as pltpu
from jax.sharding import PartitionSpec as P

ROPE_BASE = 1000000.0
LN_EPS = 1e-5
NEG_BIG = -1e30
F32 = jnp.float32
BF16 = jnp.bfloat16
SQ = 4
QB = 8
NB = 4
CHUNK = SQ * QB
AHEAD = 3
HEAD = 128
VMEM_LIMIT = 60 * 1024 * 1024


def dot(a, b):
    return lax.dot_general(a, b, (((1,), (0,)), ((), ())), preferred_element_type=F32)


def dot_nt(a, b):
    return lax.dot_general(a, b, (((1,), (1,)), ((), ())), preferred_element_type=F32)


def layer_norm(vectors, gain, shift):
    row_mean = jnp.mean(vectors, axis=-1, keepdims=True)
    centered = vectors - row_mean
    row_var = jnp.mean(centered * centered, axis=-1, keepdims=True)
    return centered * lax.rsqrt(row_var + LN_EPS) * gain + shift


def params(n_grid, **kw):
    return pltpu.CompilerParams(dimension_semantics=("arbitrary",) * n_grid, vmem_limit_bytes=VMEM_LIMIT, **kw)


def as_row(ref):
    return ref[...].astype(F32).reshape(1, -1)


def qkv_kernel(n_q, x_ref, gain_ref, shift_ref, wq_ref, bq_ref, wk_ref, bk_ref, wv_ref, bv_ref, cos_ref, sin_ref,
               q_ref, k_ref, v_ref, h_ref, bias, cos_t, sin_t):
    step = pl.program_id(0)
    steps, batch = x_ref.shape[0], x_ref.shape[1]
    chunks = batch // CHUNK

    @pl.when(step == 0)
    def _():
        gain, shift = as_row(gain_ref), as_row(shift_ref)
        bias[...] = as_row(bq_ref)
        cos_t[...] = jnp.concatenate([cos_ref[...], cos_ref[...]], axis=1)
        sin_t[...] = jnp.concatenate([-sin_ref[...], sin_ref[...]], axis=1)
        for s in range(steps):
            for r in range(0, batch, 32):
                h_ref[s * batch + r:s * batch + r + 32, :] = layer_norm(x_ref[s, r:r + 32, :].astype(F32), gain, shift).astype(BF16)

    def rope(vec, rows):
        vec = vec.astype(BF16).astype(F32)
        out = vec * cos_t[rows, :] + pltpu.roll(vec, HEAD // 2, 1) * sin_t[rows, :]
        return out.astype(BF16).astype(F32)

    @pl.when(step < n_q)
    def _():
        acc = dot(h_ref[...], wq_ref[...]) + bias[:, pl.ds(pl.multiple_of(step * 2 * HEAD, HEAD), 2 * HEAD)]
        for s in range(steps):
            for c in range(chunks):
                rows = slice(s * batch + c * CHUNK, s * batch + (c + 1) * CHUNK)
                for h in range(2):
                    q_ref[c, s, h] = rope(acc[rows, h * HEAD:(h + 1) * HEAD], rows)

    @pl.when(step == n_q)
    def _():
        acc = dot(h_ref[...], jnp.concatenate([wk_ref[...], wv_ref[...]], axis=1))
        acc = acc + jnp.concatenate([as_row(bk_ref), as_row(bv_ref)], axis=1)
        for s in range(steps):
            for c in range(chunks):
                rows = slice(s * batch + c * CHUNK, s * batch + (c + 1) * CHUNK)
                k_ref[c, s] = rope(acc[rows, :HEAD], rows)
                v_ref[c, s] = acc[rows, HEAD:].astype(BF16).astype(F32)
        for s in range(steps, 8):
            for c in range(chunks):
                k_ref[c, s] = jnp.zeros((CHUNK, HEAD), F32)
                v_ref[c, s] = jnp.zeros((CHUNK, HEAD), F32)


def qkv(x_steps, gain, shift, w_q, b_q, w_k, b_k, w_v, b_v, cos_t, sin_t):
    steps, batch, dim = x_steps.shape
    chunks = batch // CHUNK
    heads = w_q.shape[1] // HEAD
    n_q = heads // 2
    whole = lambda *shape: pl.BlockSpec(shape, lambda j: (0,) * len(shape))
    last = n_q - 1
    rows = steps * batch
    return pl.pallas_call(
        functools.partial(qkv_kernel, n_q),
        grid=(n_q + 1,),
        in_specs=[
            whole(steps, batch, dim), whole(dim), whole(dim),
            pl.BlockSpec((dim, 2 * HEAD), lambda j: (0, jnp.minimum(j, last))), whole(heads * HEAD),
            whole(dim, HEAD), whole(HEAD), whole(dim, HEAD), whole(HEAD),
            whole(rows, HEAD // 2), whole(rows, HEAD // 2),
        ],
        out_specs=[
            pl.BlockSpec((chunks, steps, 2, CHUNK, HEAD), lambda j: (0, 0, jnp.minimum(j, last), 0, 0)),
            whole(chunks, 8, CHUNK, HEAD), whole(chunks, 8, CHUNK, HEAD),
        ],
        out_shape=[
            jax.ShapeDtypeStruct((chunks, steps, heads, CHUNK, HEAD), F32),
            jax.ShapeDtypeStruct((chunks, 8, CHUNK, HEAD), F32),
            jax.ShapeDtypeStruct((chunks, 8, CHUNK, HEAD), F32),
        ],
        scratch_shapes=[pltpu.VMEM((rows, dim), BF16), pltpu.VMEM((1, heads * HEAD), F32), pltpu.VMEM((rows, HEAD), F32), pltpu.VMEM((rows, HEAD), F32)],
        compiler_params=params(1),
        cost_estimate=pl.CostEstimate(flops=2 * rows * dim * (heads + 2) * HEAD, bytes_accessed=20_000_000, transcendentals=0),
        name="qkv",
    )(x_steps, gain, shift, w_q, b_q, w_k, b_k, w_v, b_v, cos_t, sin_t)


def attn_kernel(chunk, group, slots, n_any, pos_ref, q_hbm, kn_hbm, vn_hbm, k_hbm, v_hbm, *rest):
    ko_hbm, vo_hbm, *outs = rest[n_any:n_any + 6]
    kbuf, vbuf, q_ref, kn_ref, vn_ref, o_all, in_sem, out_sem, small_sem = rest[n_any + 6:]
    me = lax.axis_index("sq").astype(jnp.int32)
    n = CHUNK // NB
    local = kbuf.shape[2]
    rows = 4 * group
    first_slot = me * local
    exp_scale = math.log2(math.e) * HEAD ** -0.5
    step_col = lax.broadcasted_iota(jnp.int32, (rows, 1), 0) // group
    lane = lax.broadcasted_iota(jnp.int32, (1, local), 1) + first_slot
    new_lane = lax.broadcasted_iota(jnp.int32, (1, 8), 1)
    diag = lax.broadcasted_iota(jnp.int32, (rows, HEAD), 0) == lax.broadcasted_iota(jnp.int32, (rows, HEAD), 1)
    row16 = lax.broadcasted_iota(jnp.int32, (16, HEAD), 0)

    def place(i):
        rel = 3 - i // 2
        return jnp.bitwise_xor(me, rel) * 2 + i % 2

    def seqs(i):
        return pl.ds(chunk * CHUNK + place(i) * NB, NB)

    def loads(i):
        return (pltpu.make_async_copy(k_hbm.at[seqs(i)], kbuf.at[i], in_sem.at[0, i]),
                pltpu.make_async_copy(v_hbm.at[seqs(i)], vbuf.at[i], in_sem.at[1, i]))

    def stores(i):
        return (pltpu.make_async_copy(kbuf.at[i], ko_hbm.at[seqs(i)], out_sem.at[0, i]),
                pltpu.make_async_copy(vbuf.at[i], vo_hbm.at[seqs(i)], out_sem.at[1, i]))

    small = [pltpu.make_async_copy(src.at[chunk], dst, small_sem.at[4 + t]) for t, (src, dst) in enumerate(((q_hbm, q_ref), (kn_hbm, kn_ref), (vn_hbm, vn_ref)))]
    for copy in small:
        copy.start()
    for i in range(AHEAD):
        for copy in loads(i):
            copy.start()
    for copy in small:
        copy.wait()

    def body(i, carry):
        @pl.when(i + AHEAD < n)
        def _():
            for copy in loads(i + AHEAD):
                copy.start()

        for copy in loads(i):
            copy.wait()

        @pl.when(i > 0)
        def _():
            for copy in stores(i - 1):
                copy.start()

        grp = place(i)
        out_at = o_all.at[3 - i // 2, i % 2]
        bls = [jnp.bitwise_and(jb + me, NB - 1) for jb in range(NB)]
        ids = [grp * NB + bl for bl in bls]
        queries = [q_ref[pl.ds(seq, rows, stride=CHUNK), :].astype(BF16) for seq in ids]
        new_keys = kn_ref[pl.ds(ids[0], 8, stride=CHUNK), :].astype(BF16)
        new_vals = vn_ref[pl.ds(ids[0], 8, stride=CHUNK), :].astype(BF16)
        scores = []
        for bl, seq, query in zip(bls, ids, queries):
            pos = pos_ref[chunk * CHUNK + seq]
            age = jnp.where(lane < pos, jnp.bitwise_and(lane - pos, slots - 1), 0)
            scores.append(jnp.where(age > step_col, dot_nt(query, kbuf[i, bl]), NEG_BIG))
        new_scores = jnp.where(new_lane <= step_col, dot_nt(queries[0], new_keys), NEG_BIG)
        tops = [jnp.max(sc, axis=1, keepdims=True) for sc in scores]
        tops[0] = jnp.maximum(tops[0], jnp.max(new_scores, axis=1, keepdims=True))
        results = []
        for jb, bl in enumerate(bls):
            weights = jnp.exp2((scores[jb] - tops[jb]) * exp_scale)
            part_sum = jnp.sum(weights, axis=1, keepdims=True)
            out = dot(weights.astype(BF16), vbuf[i, bl])
            if jb == 0:
                new_weights = jnp.exp2((new_scores - tops[0]) * exp_scale)
                part_sum = part_sum + jnp.sum(new_weights, axis=1, keepdims=True)
                out = out + dot(new_weights.astype(BF16), new_vals)
            results.append((bl, out, tops[jb], part_sum))
        for bl, out, top, part_sum in results:
            out_at[pl.ds(pl.multiple_of(bl * rows, 8), rows), :] = out
            out_at[pl.ds(NB * rows + bl, 1), :] = jnp.sum(jnp.where(diag, top, 0.0), axis=0, keepdims=True)
            out_at[pl.ds(NB * rows + NB + bl, 1), :] = jnp.sum(jnp.where(diag, part_sum, 0.0), axis=0, keepdims=True)

        for bl in range(NB):
            seq = grp * NB + bl
            begin = jnp.bitwise_and(pos_ref[chunk * CHUNK + seq], slots - 1) - first_slot
            near = jnp.bitwise_and(begin, slots - 1)

            @pl.when((near < local) | (near > slots - 4))
            def _(bl=bl, seq=seq, begin=begin):
                for t in range(4):
                    slot = jnp.bitwise_and(begin + t, slots - 1)

                    @pl.when(slot < local)
                    def _(t=t, slot=slot):
                        window = pl.ds(pl.multiple_of(slot // 16 * 16, 16), 16)
                        hit = row16 == slot % 16
                        for buf, new_ref in ((kbuf, kn_ref), (vbuf, vn_ref)):
                            new = new_ref[pl.ds(t * CHUNK + seq, 1), :]
                            buf[i, bl, window, :] = jnp.where(hit, new, buf[i, bl, window, :].astype(F32)).astype(BF16)

        return carry

    lax.fori_loop(0, n, body, 0)
    tails = [pltpu.make_async_copy(o_all.at[r], outs[r], small_sem.at[r]) for r in range(4)]
    for copy in tails + list(stores(n - 1)):
        copy.start()
    for i in range(n):
        for copy in stores(i):
            copy.wait()
    for copy in tails:
        copy.wait()


def attention(chunk, slots, positions, q, kn, vn, k_cache, v_cache, outs, after):
    batch, local, _ = k_cache.shape
    chunks = batch // CHUNK
    group = q.shape[2]
    rows = 4 * group
    n = CHUNK // NB
    width = NB * rows + 2 * NB
    n_alias = 0 if outs is None else 2
    n_any = n_alias + len(after)
    any_spec = pl.BlockSpec(memory_space=pl.ANY)
    part_shape = jax.ShapeDtypeStruct((2, width, HEAD), F32)
    cache_shape = jax.ShapeDtypeStruct(k_cache.shape, BF16)
    return pl.pallas_call(
        functools.partial(attn_kernel, chunk, group, slots, n_any),
        in_specs=[pl.BlockSpec(memory_space=pltpu.SMEM)] + [any_spec] * (5 + n_any),
        out_specs=[any_spec] * 6,
        out_shape=[cache_shape, cache_shape] + [part_shape] * 4,
        scratch_shapes=[
            pltpu.VMEM((n, NB, local, HEAD), BF16), pltpu.VMEM((n, NB, local, HEAD), BF16),
            pltpu.VMEM((rows * CHUNK, HEAD), F32), pltpu.VMEM((8 * CHUNK, HEAD), F32), pltpu.VMEM((8 * CHUNK, HEAD), F32),
            pltpu.VMEM((4, 2, width, HEAD), F32),
            pltpu.SemaphoreType.DMA((2, n)), pltpu.SemaphoreType.DMA((2, n)), pltpu.SemaphoreType.DMA((7,)),
        ],
        input_output_aliases={6: 0, 7: 1} if n_alias else {},
        compiler_params=pltpu.CompilerParams(vmem_limit_bytes=VMEM_LIMIT),
        cost_estimate=pl.CostEstimate(flops=10_000_000_000, bytes_accessed=CHUNK * local * HEAD * 8, transcendentals=CHUNK * rows * local),
        name="attn",
    )(positions, q.reshape(chunks, rows * CHUNK, HEAD), kn.reshape(chunks, 8 * CHUNK, HEAD), vn.reshape(chunks, 8 * CHUNK, HEAD), k_cache, v_cache, *(outs or ()), *after)


def combine_kernel(group, p0_hbm, p1_hbm, p2_hbm, p3_hbm, wo_hbm, *rest):
    out_ref, parts, a_scr, a32_scr, wbuf, psem, wsem = rest[-7:]
    rows = 4 * group
    exp_scale = math.log2(math.e) * HEAD ** -0.5
    n, _, block = wbuf.shape
    gets = [pltpu.make_async_copy(p, parts.at[i], psem.at[i]) for i, p in enumerate((p0_hbm, p1_hbm, p2_hbm, p3_hbm))]
    weights = [pltpu.make_async_copy(wo_hbm.at[:, pl.ds(j * block, block)], wbuf.at[j], wsem.at[j]) for j in range(n)]
    for copy in gets + weights:
        copy.start()
    for copy in gets:
        copy.wait()
    for g in range(2):
        stats = [parts[i, g, NB * rows:NB * rows + 2 * NB, :] for i in range(SQ)]
        top = functools.reduce(jnp.maximum, stats)
        scale = [jnp.exp2((st - top) * exp_scale) for st in stats]
        total = sum(sc * pltpu.roll(st, NB, 0) for sc, st in zip(scale, stats))
        scale = [(sc / total).T for sc in scale]
        for b in range(NB):
            acc = sum(parts[i, g, b * rows:(b + 1) * rows, :] * sc[:rows, b:b + 1] for i, sc in enumerate(scale))
            a_scr[pl.ds((g * NB + b) * rows, rows), :] = acc
    for s in range(4):
        for h in range(group):
            a32_scr[s * QB:(s + 1) * QB, h * HEAD:(h + 1) * HEAD] = a_scr[pl.ds(s * group + h, QB, stride=rows), :]
    for j in range(n):
        weights[j].wait()
        out_ref[:, j * block:(j + 1) * block] = dot(a32_scr[...].astype(BF16), wbuf[j])


def combine(parts, w_o, after):
    depth, dim = w_o.shape
    group = depth // HEAD
    n, block = 6, dim // 6
    any_spec = pl.BlockSpec(memory_space=pl.ANY)
    return pl.pallas_call(
        functools.partial(combine_kernel, group),
        in_specs=[any_spec] * (5 + len(after)),
        out_specs=pl.BlockSpec(memory_space=pltpu.VMEM),
        out_shape=jax.ShapeDtypeStruct((4 * QB, dim), F32),
        scratch_shapes=[
            pltpu.VMEM((SQ,) + parts[0].shape, F32), pltpu.VMEM((4 * group * QB, HEAD), F32), pltpu.VMEM((4 * QB, depth), F32),
            pltpu.VMEM((n, depth, block), BF16), pltpu.SemaphoreType.DMA((SQ,)), pltpu.SemaphoreType.DMA((n,)),
        ],
        compiler_params=pltpu.CompilerParams(vmem_limit_bytes=VMEM_LIMIT),
        cost_estimate=pl.CostEstimate(flops=2_500_000_000, bytes_accessed=depth * dim * 2, transcendentals=0),
        name="combine_wo",
    )(*parts, w_o, *after)


MESH = pl.DeviceIdType.MESH
BLK = 512


def tail_kernel(chunks, n_blk, x_ref, bo_ref, gain_ref, shift_ref, bproj_ref, bfc_ref, *refs):
    own, got = refs[:chunks], refs[chunks:2 * chunks]
    (wfc_ref, wproj_ref, ys_ref, xs, x1, hsend, hrecv, hall, g, wbuf, bproj, bfc, part, recv1, sums, recv2, ybuf, recv3, recv4, recv5,
     xsem, wsem, hs, hr, s1, r1, s2, r2, s3, r3, s4, r4, s5, r5) = refs[2 * chunks:]
    me = lax.axis_index("sq")
    core = lax.rem(me, 2)
    sib = {"sq": me + 1 - 2 * core}
    across = {"sq": lax.rem(me + 2, SQ)}
    partner = {"tp": 1 - lax.axis_index("tp")}
    rows = 4 * QB * chunks
    span = 4 * QB

    def remote(src, dst, send, recv, device):
        return pltpu.make_async_remote_copy(src_ref=src, dst_ref=dst, send_sem=send, recv_sem=recv, device_id=device, device_id_type=MESH)

    def weights(n, slot):
        if n < n_blk:
            src = wfc_ref.at[:, pl.ds(pl.multiple_of((core * n_blk + n) * BLK, BLK), BLK)]
        else:
            src = wproj_ref.at[pl.ds(pl.multiple_of(core * n_blk * BLK, BLK), n_blk * BLK), pl.ds((n - n_blk) * BLK, BLK)]
        return pltpu.make_async_copy(src, wbuf.at[slot], wsem.at[slot])

    x_copy = pltpu.make_async_copy(x_ref.at[:, :, me], xs, xsem)
    x_copy.start()
    for n in range(n_blk):
        weights(n, n).start()

    barrier = pltpu.get_barrier_semaphore()
    for device in (sib, across, partner):
        pl.semaphore_signal(barrier, inc=1, device_id=device, device_id_type=MESH)
    pl.semaphore_wait(barrier, 3)

    x_copy.wait()
    bias, gain, shift = as_row(bo_ref), as_row(gain_ref), as_row(shift_ref)
    bproj[...] = as_row(bproj_ref)
    bfc[...] = as_row(bfc_ref)

    def send_h(c):
        return remote(hsend.at[c], hrecv.at[c], hs.at[c], hr.at[c], sib)

    for c in range(chunks):
        for s in range(4):
            at = slice(s * QB, (s + 1) * QB)
            mid = xs[s, c].astype(F32) + (own[c][at, :] + got[c][at, :]) + bias
            x1[c * span + s * QB:c * span + (s + 1) * QB, :] = mid.astype(BF16).astype(F32)
        h = layer_norm(x1[c * span:(c + 1) * span, :], gain, shift).astype(BF16)
        hall[c * span:(c + 1) * span, :] = h
        hsend[c] = h.astype(F32)
        send_h(c).start()
    for c in range(chunks):
        send_h(c).wait_recv()
        hall[rows + c * span:rows + (c + 1) * span, :] = hrecv[c].astype(BF16)

    for n in range(n_blk):
        weights(n, n).wait()
        cols = slice(n * BLK, (n + 1) * BLK)
        acc = dot(hall[...], wbuf[n]) + bfc[:, pl.ds(pl.multiple_of((core * n_blk + n) * BLK, BLK), BLK)]
        g[:, cols] = jax.nn.gelu(acc, approximate=True).astype(BF16)
        weights(n_blk + n, n).start()

    def send1(j):
        return remote(part.at[j], recv1.at[j], s1.at[j], r1.at[j], sib)

    def send2(j):
        return remote(sums.at[j], recv2.at[j], s2.at[j], r2.at[j], partner)

    def send3(j):
        return remote(ybuf.at[j], recv3.at[j], s3.at[j], r3.at[j], across)

    def send4(j):
        return remote(ybuf.at[j], recv4.at[j], s4.at[j], r4.at[j], sib)

    def send5(j):
        return remote(recv3.at[j], recv5.at[j], s5.at[j], r5.at[j], sib)

    def reduce_cores(j):
        send1(j).wait_recv()
        sums[j] = sums[j] + recv1[j]
        send2(j).start()

    for j in range(n_blk):
        weights(n_blk + j, j).wait()
        acc = dot(g[...], wbuf[j])
        part[j] = acc[rows:, :]
        send1(j).start()
        sums[j] = acc[:rows, :]
        if j:
            reduce_cores(j - 1)
    reduce_cores(n_blk - 1)

    def store_rows(j, value, owner):
        for c in range(chunks):
            for s in range(4):
                ys_ref[s, c, owner, :, j * BLK:(j + 1) * BLK] = value[c * span + s * QB:c * span + (s + 1) * QB, :].astype(BF16)

    def late(j):
        send3(j).wait_recv()
        send5(j).start()
        store_rows(j, recv3[j], lax.rem(me + 2, SQ))
        send4(j).wait_recv()
        store_rows(j, recv4[j], me + 1 - 2 * core)
        send5(j).wait_recv()
        store_rows(j, recv5[j], lax.rem(me + 1 - 2 * core + 2, SQ))

    for j in range(n_blk):
        cols = slice(j * BLK, (j + 1) * BLK)
        send2(j).wait_recv()
        ybuf[j] = (x1[:, cols] + (sums[j] + recv2[j]) + bproj[:, cols]).astype(BF16).astype(F32)
        send3(j).start()
        send4(j).start()
        store_rows(j, ybuf[j], me)
        if j:
            late(j - 1)
    late(n_blk - 1)

    for c in range(chunks):
        send_h(c).wait_send()
    for j in range(n_blk):
        for send in (send1, send2, send3, send4, send5):
            send(j).wait_send()


def tail(x_view, vectors, own, got, w_fc, w_proj):
    steps, chunks, _, _, dim = x_view.shape
    half = w_fc.shape[1] // 2
    n_blk = half // BLK
    rows = 4 * QB * chunks
    any_spec = pl.BlockSpec(memory_space=pl.ANY)
    vmem = pl.BlockSpec(memory_space=pltpu.VMEM)
    blocks = lambda: pltpu.VMEM((n_blk, rows, BLK), F32)
    sem = lambda n: pltpu.SemaphoreType.DMA((n,))
    return pl.pallas_call(
        functools.partial(tail_kernel, chunks, n_blk),
        in_specs=[any_spec] + [vmem] * len(vectors) + [vmem] * (2 * chunks) + [any_spec, any_spec],
        out_specs=vmem,
        out_shape=jax.ShapeDtypeStruct((steps, chunks, SQ, QB, dim), BF16),
        scratch_shapes=[
            pltpu.VMEM((steps, chunks, QB, dim), BF16), pltpu.VMEM((rows, dim), F32),
            pltpu.VMEM((chunks, 4 * QB, dim), F32), pltpu.VMEM((chunks, 4 * QB, dim), F32),
            pltpu.VMEM((2 * rows, dim), BF16), pltpu.VMEM((2 * rows, half), BF16), pltpu.VMEM((n_blk, dim, BLK), BF16),
            pltpu.VMEM((1, dim), F32), pltpu.VMEM((1, 2 * half), F32),
        ] + [blocks() for _ in range(8)] + [pltpu.SemaphoreType.DMA, sem(n_blk), sem(chunks), sem(chunks)] + [sem(n_blk) for _ in range(10)],
        compiler_params=pltpu.CompilerParams(vmem_limit_bytes=VMEM_LIMIT, collective_id=0, has_side_effects=True),
        cost_estimate=pl.CostEstimate(flops=40_000_000_000, bytes_accessed=dim * half * 4, transcendentals=0),
        name="tail",
    )(x_view, *vectors, *own, *got, w_fc, w_proj)


def solution(mesh):
    act_spec = P(None, "dp", None)
    cache_spec = P("dp", "sq", "tp", None)
    col_spec = P(None, "tp")
    row_spec = P("tp", None)
    vec_spec = P("tp")
    rep_spec = P(None)
    in_specs = (act_spec, P("dp"), cache_spec, cache_spec, col_spec, vec_spec, col_spec, vec_spec,
                col_spec, vec_spec, row_spec, rep_spec, rep_spec, rep_spec, rep_spec, rep_spec,
                col_spec, vec_spec, row_spec, rep_spec)
    out_specs = (act_spec, cache_spec, cache_spec)

    def swap_sq(value, mask):
        return lax.ppermute(value, "sq", [(i, i ^ mask) for i in range(SQ)])

    def swap_tp(value):
        return lax.ppermute(value, "tp", [(0, 1), (1, 0)])

    def per_device(x_steps, positions, key_buf, val_buf, w_q, b_q, w_k, b_k, w_v, b_v, w_o, b_o,
                   ln1_gain, ln1_bias, ln2_gain, ln2_bias, w_fc, b_fc, w_proj, b_proj):
        steps, batch, dim = x_steps.shape
        local = key_buf.shape[1]
        slots = local * SQ
        chunks = batch // CHUNK
        inv_freq = jnp.power(F32(ROPE_BASE), -2.0 * jnp.arange(HEAD // 2, dtype=F32) / HEAD)
        cur = positions[None, :] + jnp.arange(steps, dtype=jnp.int32)[:, None]
        angle = cur.reshape(-1).astype(F32)[:, None] * inv_freq
        q, kn, vn = qkv(x_steps, ln1_gain, ln1_bias, w_q, b_q, w_k, b_k, w_v, b_v, jnp.cos(angle), jnp.sin(angle))
        k_old, v_old = key_buf.reshape(batch, local, HEAD), val_buf.reshape(batch, local, HEAD)
        x_view = x_steps.reshape(steps, chunks, SQ, QB, dim)

        caches = None
        own, got = [], []
        waiting = None
        for c in range(chunks):
            res = attention(c, slots, positions, q, kn, vn, k_old, v_old, caches, own[c - 2:c - 1] if c >= 2 else [])
            caches = res[:2]
            if waiting is not None:
                own.append(combine(waiting, w_o, res[2:3]))
                got.append(swap_tp(own[-1]))
            waiting = [res[2]] + [swap_sq(res[2 + r], r) for r in range(1, SQ)]
        own.append(combine(waiting, w_o, []))
        got.append(swap_tp(own[-1]))
        ys = tail(x_view, (b_o, ln2_gain, ln2_bias, b_proj, b_fc), own, got, w_fc, w_proj).reshape(steps, batch, dim)
        return ys, caches[0].reshape(key_buf.shape), caches[1].reshape(val_buf.shape)

    return jax.shard_map(per_device, mesh=mesh, in_specs=in_specs, out_specs=out_specs, check_vma=False)
```

```python
import functools
import math

import jax
import jax.numpy as jnp
from jax import lax
from jax.experimental import pallas as pl
from jax.experimental.pallas import tpu as pltpu
from jax.sharding import PartitionSpec as P

ROPE_BASE = 1000000.0
LN_EPS = 1e-5
NEG_BIG = -1e30
F32 = jnp.float32
BF16 = jnp.bfloat16
SQ = 4
QB = 8
NB = 4
CHUNK = SQ * QB
AHEAD = 3
HEAD = 128
VMEM_LIMIT = 60 * 1024 * 1024


def dot(a, b):
    return lax.dot_general(a, b, (((1,), (0,)), ((), ())), preferred_element_type=F32)


def dot_nt(a, b):
    return lax.dot_general(a, b, (((1,), (1,)), ((), ())), preferred_element_type=F32)


def layer_norm(vectors, gain, shift):
    row_mean = jnp.mean(vectors, axis=-1, keepdims=True)
    centered = vectors - row_mean
    row_var = jnp.mean(centered * centered, axis=-1, keepdims=True)
    return centered * lax.rsqrt(row_var + LN_EPS) * gain + shift


def params(n_grid, **kw):
    return pltpu.CompilerParams(dimension_semantics=("arbitrary",) * n_grid, vmem_limit_bytes=VMEM_LIMIT, **kw)


def as_row(ref):
    return ref[...].astype(F32).reshape(1, -1)


def qkv_kernel(n_q, x_ref, gain_ref, shift_ref, wq_ref, bq_ref, wk_ref, bk_ref, wv_ref, bv_ref, cos_ref, sin_ref,
               q_ref, k_ref, v_ref, h_ref, bias, cos_t, sin_t):
    step = pl.program_id(0)
    steps, batch = x_ref.shape[0], x_ref.shape[1]
    chunks = batch // CHUNK

    @pl.when(step == 0)
    def _():
        gain, shift = as_row(gain_ref), as_row(shift_ref)
        bias[...] = as_row(bq_ref)
        cos_t[...] = jnp.concatenate([cos_ref[...], cos_ref[...]], axis=1)
        sin_t[...] = jnp.concatenate([-sin_ref[...], sin_ref[...]], axis=1)
        for s in range(steps):
            for r in range(0, batch, 32):
                h_ref[s * batch + r:s * batch + r + 32, :] = layer_norm(x_ref[s, r:r + 32, :].astype(F32), gain, shift).astype(BF16)

    def rope(vec, rows):
        vec = vec.astype(BF16).astype(F32)
        out = vec * cos_t[rows, :] + pltpu.roll(vec, HEAD // 2, 1) * sin_t[rows, :]
        return out.astype(BF16).astype(F32)

    @pl.when(step < n_q)
    def _():
        acc = dot(h_ref[...], wq_ref[...]) + bias[:, pl.ds(pl.multiple_of(step * 2 * HEAD, HEAD), 2 * HEAD)]
        for s in range(steps):
            for c in range(chunks):
                rows = slice(s * batch + c * CHUNK, s * batch + (c + 1) * CHUNK)
                for h in range(2):
                    q_ref[c, s, h] = rope(acc[rows, h * HEAD:(h + 1) * HEAD], rows)

    @pl.when(step == n_q)
    def _():
        acc = dot(h_ref[...], jnp.concatenate([wk_ref[...], wv_ref[...]], axis=1))
        acc = acc + jnp.concatenate([as_row(bk_ref), as_row(bv_ref)], axis=1)
        for s in range(steps):
            for c in range(chunks):
                rows = slice(s * batch + c * CHUNK, s * batch + (c + 1) * CHUNK)
                k_ref[c, s] = rope(acc[rows, :HEAD], rows)
                v_ref[c, s] = acc[rows, HEAD:].astype(BF16).astype(F32)
        for s in range(steps, 8):
            for c in range(chunks):
                k_ref[c, s] = jnp.zeros((CHUNK, HEAD), F32)
                v_ref[c, s] = jnp.zeros((CHUNK, HEAD), F32)


def qkv(x_steps, gain, shift, w_q, b_q, w_k, b_k, w_v, b_v, cos_t, sin_t):
    steps, batch, dim = x_steps.shape
    chunks = batch // CHUNK
    heads = w_q.shape[1] // HEAD
    n_q = heads // 2
    whole = lambda *shape: pl.BlockSpec(shape, lambda j: (0,) * len(shape))
    last = n_q - 1
    rows = steps * batch
    return pl.pallas_call(
        functools.partial(qkv_kernel, n_q),
        grid=(n_q + 1,),
        in_specs=[
            whole(steps, batch, dim), whole(dim), whole(dim),
            pl.BlockSpec((dim, 2 * HEAD), lambda j: (0, jnp.minimum(j, last))), whole(heads * HEAD),
            whole(dim, HEAD), whole(HEAD), whole(dim, HEAD), whole(HEAD),
            whole(rows, HEAD // 2), whole(rows, HEAD // 2),
        ],
        out_specs=[
            pl.BlockSpec((chunks, steps, 2, CHUNK, HEAD), lambda j: (0, 0, jnp.minimum(j, last), 0, 0)),
            whole(chunks, 8, CHUNK, HEAD), whole(chunks, 8, CHUNK, HEAD),
        ],
        out_shape=[
            jax.ShapeDtypeStruct((chunks, steps, heads, CHUNK, HEAD), F32),
            jax.ShapeDtypeStruct((chunks, 8, CHUNK, HEAD), F32),
            jax.ShapeDtypeStruct((chunks, 8, CHUNK, HEAD), F32),
        ],
        scratch_shapes=[pltpu.VMEM((rows, dim), BF16), pltpu.VMEM((1, heads * HEAD), F32), pltpu.VMEM((rows, HEAD), F32), pltpu.VMEM((rows, HEAD), F32)],
        compiler_params=params(1),
        cost_estimate=pl.CostEstimate(flops=2 * rows * dim * (heads + 2) * HEAD, bytes_accessed=20_000_000, transcendentals=0),
        name="qkv",
    )(x_steps, gain, shift, w_q, b_q, w_k, b_k, w_v, b_v, cos_t, sin_t)


def attn_kernel(chunk, group, slots, n_any, pos_ref, q_hbm, kn_hbm, vn_hbm, k_hbm, v_hbm, *rest):
    ko_hbm, vo_hbm, *outs = rest[n_any:n_any + 6]
    kbuf, vbuf, q_ref, kn_ref, vn_ref, o_all, in_sem, out_sem, small_sem = rest[n_any + 6:]
    me = lax.axis_index("sq").astype(jnp.int32)
    n = CHUNK // NB
    local = kbuf.shape[2]
    rows = 4 * group
    first_slot = me * local
    exp_scale = math.log2(math.e) * HEAD ** -0.5
    step_col = lax.broadcasted_iota(jnp.int32, (rows, 1), 0) // group
    lane = lax.broadcasted_iota(jnp.int32, (1, local), 1) + first_slot
    new_lane = lax.broadcasted_iota(jnp.int32, (1, 8), 1)
    diag = lax.broadcasted_iota(jnp.int32, (rows, HEAD), 0) == lax.broadcasted_iota(jnp.int32, (rows, HEAD), 1)
    row16 = lax.broadcasted_iota(jnp.int32, (16, HEAD), 0)

    def place(i):
        rel = 3 - i // 2
        return jnp.bitwise_xor(me, rel) * 2 + i % 2

    def seqs(i):
        return pl.ds(chunk * CHUNK + place(i) * NB, NB)

    def loads(i):
        return (pltpu.make_async_copy(k_hbm.at[seqs(i)], kbuf.at[i], in_sem.at[0, i]),
                pltpu.make_async_copy(v_hbm.at[seqs(i)], vbuf.at[i], in_sem.at[1, i]))

    def stores(i):
        return (pltpu.make_async_copy(kbuf.at[i], ko_hbm.at[seqs(i)], out_sem.at[0, i]),
                pltpu.make_async_copy(vbuf.at[i], vo_hbm.at[seqs(i)], out_sem.at[1, i]))

    small = [pltpu.make_async_copy(src.at[chunk], dst, small_sem.at[4 + t]) for t, (src, dst) in enumerate(((q_hbm, q_ref), (kn_hbm, kn_ref), (vn_hbm, vn_ref)))]
    for copy in small:
        copy.start()
    for i in range(AHEAD):
        for copy in loads(i):
            copy.start()
    for copy in small:
        copy.wait()

    def body(i, carry):
        @pl.when(i + AHEAD < n)
        def _():
            for copy in loads(i + AHEAD):
                copy.start()

        for copy in loads(i):
            copy.wait()

        @pl.when(i > 0)
        def _():
            for copy in stores(i - 1):
                copy.start()

        grp = place(i)
        out_at = o_all.at[3 - i // 2, i % 2]
        bls = [jnp.bitwise_and(jb + me, NB - 1) for jb in range(NB)]
        ids = [grp * NB + bl for bl in bls]
        queries = [q_ref[pl.ds(seq, rows, stride=CHUNK), :].astype(BF16) for seq in ids]
        new_keys = kn_ref[pl.ds(ids[0], 8, stride=CHUNK), :].astype(BF16)
        new_vals = vn_ref[pl.ds(ids[0], 8, stride=CHUNK), :].astype(BF16)
        scores = []
        for bl, seq, query in zip(bls, ids, queries):
            pos = pos_ref[chunk * CHUNK + seq]
            age = jnp.where(lane < pos, jnp.bitwise_and(lane - pos, slots - 1), 0)
            scores.append(jnp.where(age > step_col, dot_nt(query, kbuf[i, bl]), NEG_BIG))
        new_scores = jnp.where(new_lane <= step_col, dot_nt(queries[0], new_keys), NEG_BIG)
        tops = [jnp.max(sc, axis=1, keepdims=True) for sc in scores]
        tops[0] = jnp.maximum(tops[0], jnp.max(new_scores, axis=1, keepdims=True))
        results = []
        for jb, bl in enumerate(bls):
            weights = jnp.exp2((scores[jb] - tops[jb]) * exp_scale)
            part_sum = jnp.sum(weights, axis=1, keepdims=True)
            out = dot(weights.astype(BF16), vbuf[i, bl])
            if jb == 0:
                new_weights = jnp.exp2((new_scores - tops[0]) * exp_scale)
                part_sum = part_sum + jnp.sum(new_weights, axis=1, keepdims=True)
                out = out + dot(new_weights.astype(BF16), new_vals)
            results.append((bl, out, tops[jb], part_sum))
        for bl, out, top, part_sum in results:
            out_at[pl.ds(pl.multiple_of(bl * rows, 8), rows), :] = out
            out_at[pl.ds(NB * rows + bl, 1), :] = jnp.sum(jnp.where(diag, top, 0.0), axis=0, keepdims=True)
            out_at[pl.ds(NB * rows + NB + bl, 1), :] = jnp.sum(jnp.where(diag, part_sum, 0.0), axis=0, keepdims=True)

        for bl in range(NB):
            seq = grp * NB + bl
            begin = jnp.bitwise_and(pos_ref[chunk * CHUNK + seq], slots - 1) - first_slot
            near = jnp.bitwise_and(begin, slots - 1)

            @pl.when((near < local) | (near > slots - 4))
            def _(bl=bl, seq=seq, begin=begin):
                for t in range(4):
                    slot = jnp.bitwise_and(begin + t, slots - 1)

                    @pl.when(slot < local)
                    def _(t=t, slot=slot):
                        window = pl.ds(pl.multiple_of(slot // 16 * 16, 16), 16)
                        hit = row16 == slot % 16
                        for buf, new_ref in ((kbuf, kn_ref), (vbuf, vn_ref)):
                            new = new_ref[pl.ds(t * CHUNK + seq, 1), :]
                            buf[i, bl, window, :] = jnp.where(hit, new, buf[i, bl, window, :].astype(F32)).astype(BF16)

        return carry

    lax.fori_loop(0, n, body, 0)
    tails = [pltpu.make_async_copy(o_all.at[r], outs[r], small_sem.at[r]) for r in range(4)]
    for copy in tails + list(stores(n - 1)):
        copy.start()
    for i in range(n):
        for copy in stores(i):
            copy.wait()
    for copy in tails:
        copy.wait()


def attention(chunk, slots, positions, q, kn, vn, k_cache, v_cache, outs, after):
    batch, local, _ = k_cache.shape
    chunks = batch // CHUNK
    group = q.shape[2]
    rows = 4 * group
    n = CHUNK // NB
    width = NB * rows + 2 * NB
    n_alias = 0 if outs is None else 2
    n_any = n_alias + len(after)
    any_spec = pl.BlockSpec(memory_space=pl.ANY)
    part_shape = jax.ShapeDtypeStruct((2, width, HEAD), F32)
    cache_shape = jax.ShapeDtypeStruct(k_cache.shape, BF16)
    return pl.pallas_call(
        functools.partial(attn_kernel, chunk, group, slots, n_any),
        in_specs=[pl.BlockSpec(memory_space=pltpu.SMEM)] + [any_spec] * (5 + n_any),
        out_specs=[any_spec] * 6,
        out_shape=[cache_shape, cache_shape] + [part_shape] * 4,
        scratch_shapes=[
            pltpu.VMEM((n, NB, local, HEAD), BF16), pltpu.VMEM((n, NB, local, HEAD), BF16),
            pltpu.VMEM((rows * CHUNK, HEAD), F32), pltpu.VMEM((8 * CHUNK, HEAD), F32), pltpu.VMEM((8 * CHUNK, HEAD), F32),
            pltpu.VMEM((4, 2, width, HEAD), F32),
            pltpu.SemaphoreType.DMA((2, n)), pltpu.SemaphoreType.DMA((2, n)), pltpu.SemaphoreType.DMA((7,)),
        ],
        input_output_aliases={6: 0, 7: 1} if n_alias else {},
        compiler_params=pltpu.CompilerParams(vmem_limit_bytes=VMEM_LIMIT),
        cost_estimate=pl.CostEstimate(flops=10_000_000_000, bytes_accessed=CHUNK * local * HEAD * 8, transcendentals=CHUNK * rows * local),
        name="attn",
    )(positions, q.reshape(chunks, rows * CHUNK, HEAD), kn.reshape(chunks, 8 * CHUNK, HEAD), vn.reshape(chunks, 8 * CHUNK, HEAD), k_cache, v_cache, *(outs or ()), *after)


def combine_rows(group, parts, a_scr, a32_scr):
    rows = 4 * group
    exp_scale = math.log2(math.e) * HEAD ** -0.5
    for g in range(2):
        stats = [parts[i, g, NB * rows:NB * rows + 2 * NB, :] for i in range(SQ)]
        top = functools.reduce(jnp.maximum, stats)
        scale = [jnp.exp2((st - top) * exp_scale) for st in stats]
        total = sum(sc * pltpu.roll(st, NB, 0) for sc, st in zip(scale, stats))
        scale = [(sc / total).T for sc in scale]
        sums = [sum(parts[i, g, b * rows:(b + 1) * rows, :] * sc[:rows, b:b + 1] for i, sc in enumerate(scale)) for b in range(NB)]
        for b, acc in enumerate(sums):
            a_scr[pl.ds((g * NB + b) * rows, rows), :] = acc
    for s in range(4):
        for h in range(group):
            a32_scr[s * QB:(s + 1) * QB, h * HEAD:(h + 1) * HEAD] = a_scr[pl.ds(s * group + h, QB, stride=rows), :]


def combine_kernel(group, p0_hbm, p1_hbm, p2_hbm, p3_hbm, wo_hbm, *rest):
    out_ref, parts, a_scr, a32_scr, wbuf, psem, wsem = rest[-7:]
    n, _, block = wbuf.shape
    gets = [pltpu.make_async_copy(p, parts.at[i], psem.at[i]) for i, p in enumerate((p0_hbm, p1_hbm, p2_hbm, p3_hbm))]
    weights = [pltpu.make_async_copy(wo_hbm.at[:, pl.ds(j * block, block)], wbuf.at[j], wsem.at[j]) for j in range(n)]
    for copy in gets + weights:
        copy.start()
    for copy in gets:
        copy.wait()
    combine_rows(group, parts, a_scr, a32_scr)
    for j in range(n):
        weights[j].wait()
        out_ref[:, j * block:(j + 1) * block] = dot(a32_scr[...].astype(BF16), wbuf[j])


def combine(parts, w_o, after):
    depth, dim = w_o.shape
    group = depth // HEAD
    n, block = 6, dim // 6
    any_spec = pl.BlockSpec(memory_space=pl.ANY)
    return pl.pallas_call(
        functools.partial(combine_kernel, group),
        in_specs=[any_spec] * (5 + len(after)),
        out_specs=pl.BlockSpec(memory_space=pltpu.VMEM),
        out_shape=jax.ShapeDtypeStruct((4 * QB, dim), F32),
        scratch_shapes=[
            pltpu.VMEM((SQ,) + parts[0].shape, F32), pltpu.VMEM((4 * group * QB, HEAD), F32), pltpu.VMEM((4 * QB, depth), F32),
            pltpu.VMEM((n, depth, block), BF16), pltpu.SemaphoreType.DMA((SQ,)), pltpu.SemaphoreType.DMA((n,)),
        ],
        compiler_params=pltpu.CompilerParams(vmem_limit_bytes=VMEM_LIMIT),
        cost_estimate=pl.CostEstimate(flops=2_500_000_000, bytes_accessed=depth * dim * 2, transcendentals=0),
        name="combine_wo",
    )(*parts, w_o, *after)


MESH = pl.DeviceIdType.MESH
BLK = 512
TAIL_VMEM = 67_000_000


def tail_kernel(n_blk, group, x_ref, bo_ref, gain_ref, shift_ref, bproj_ref, bfc_ref, own0, got0, own1, got1, *refs):
    ready, fresh = refs[:SQ], refs[SQ:2 * SQ]
    (wo_ref, wfc_ref, wproj_ref, ys_ref, xs, pbuf, a_scr, a32_scr, wo, own_buf, got_buf, x1, hsend, hrecv, hall, g, wbuf, bproj, bfc,
     part, recv1, sums, recv2, ybuf, recv3, recv4, recv5,
     xsem, psem, fs, fr, wosem, wsem, os, og, hs, hr, s1, r1, s2, r2, s3, r3, s4, r4, s5, r5) = refs[2 * SQ:]
    me = lax.axis_index("sq").astype(jnp.int32)
    core = lax.rem(me, 2)
    peers = [me, me + 1 - 2 * core, lax.rem(me + 2, SQ), lax.rem(me + 3 - 2 * core, SQ)]
    sib, across = {"sq": peers[1]}, {"sq": peers[2]}
    partner = {"tp": 1 - lax.axis_index("tp")}
    span = 4 * QB
    half = 2 * span
    n_wo = wo.shape[0]

    def remote(src, dst, send, recv, device):
        return pltpu.make_async_remote_copy(src_ref=src, dst_ref=dst, send_sem=send, recv_sem=recv, device_id=device, device_id_type=MESH)

    def cols(j):
        return pl.ds(pl.multiple_of(j * BLK, BLK), BLK)

    def weights(kind, j):
        if kind % 2 == 0:
            src = wfc_ref.at[:, cols(core * n_blk + j)]
        else:
            src = wproj_ref.at[pl.ds(pl.multiple_of(core * n_blk * BLK, BLK), n_blk * BLK), cols(j)]
        return pltpu.make_async_copy(src, wbuf.at[j], wsem.at[j])

    def get_wo(j):
        return pltpu.make_async_copy(wo_ref.at[:, cols(j)], wo.at[j], wosem.at[j])

    def send_part(r):
        return remote(fresh[r], pbuf.at[1, r], fs.at[r], fr.at[r], {"sq": peers[r]})

    local = [pltpu.make_async_copy(ready[r], pbuf.at[0, r], psem.at[r]) for r in range(SQ)]
    local.append(pltpu.make_async_copy(fresh[0], pbuf.at[1, 0], psem.at[SQ]))
    x_copy = pltpu.make_async_copy(x_ref.at[:, :, me], xs, xsem)

    barrier = pltpu.get_barrier_semaphore()
    for device in ({"sq": peers[1]}, {"sq": peers[2]}, {"sq": peers[3]}, partner):
        pl.semaphore_signal(barrier, inc=1, device_id=device, device_id_type=MESH)
    for copy in local:
        copy.start()
    x_copy.start()
    for j in range(n_wo):
        get_wo(j).start()
    for j in range(n_blk):
        weights(0, j).start()
    pl.semaphore_wait(barrier, 4)
    for r in (2, 3, 1):
        send_part(r).start()

    bias, gain, shift = as_row(bo_ref), as_row(gain_ref), as_row(shift_ref)
    bproj[...] = as_row(bproj_ref)
    bfc[...] = as_row(bfc_ref)

    def swap_own(i):
        return remote(own_buf.at[i], got_buf.at[i], os.at[i], og.at[i], partner)

    def project(i):
        combine_rows(group, pbuf.at[i], a_scr, a32_scr)

        def body(j, carry):
            if i == 0:
                get_wo(j).wait()
            own_buf[i, :, cols(j)] = dot(a32_scr[...].astype(BF16), wo[j])
            return carry

        lax.fori_loop(0, n_wo, body, 0)
        swap_own(i).start()

    def send_h(c):
        return remote(hsend.at[c], hrecv.at[c], hs.at[c], hr.at[c], sib)

    def enter(hf, own, got):
        for i in range(2):
            for s in range(4):
                at = slice(s * QB, (s + 1) * QB)
                mid = xs[s, 2 * hf + i].astype(F32) + (own[i][at, :] + got[i][at, :]) + bias
                x1[hf, i * span + s * QB:i * span + (s + 1) * QB, :] = mid.astype(BF16).astype(F32)
            h = layer_norm(x1[hf, i * span:(i + 1) * span, :], gain, shift).astype(BF16)
            hall[i * span:(i + 1) * span, :] = h
            hsend[2 * hf + i] = h.astype(F32)
            send_h(2 * hf + i).start()

    def gather_h(hf):
        for i in range(2):
            send_h(2 * hf + i).wait_recv()
            hall[half + i * span:half + (i + 1) * span, :] = hrecv[2 * hf + i].astype(BF16)

    def first(hf):
        def body(j, carry):
            weights(2 * hf, j).wait()
            acc = dot(hall[...], wbuf[j]) + bfc[:, cols(core * n_blk + j)]
            g[:, cols(j)] = jax.nn.gelu(acc, approximate=True).astype(BF16)
            weights(2 * hf + 1, j).start()
            return carry

        lax.fori_loop(0, n_blk, body, 0)

    def send1(hf, j):
        return remote(part.at[hf, j], recv1.at[hf, j], s1.at[hf, j], r1.at[hf, j], sib)

    def send2(hf, j):
        return remote(sums.at[hf, j], recv2.at[hf, j], s2.at[hf, j], r2.at[hf, j], partner)

    def send3(hf, j):
        return remote(ybuf.at[hf, j], recv3.at[hf, j], s3.at[hf, j], r3.at[hf, j], across)

    def send4(hf, j):
        return remote(ybuf.at[hf, j], recv4.at[hf, j], s4.at[hf, j], r4.at[hf, j], sib)

    def send5(hf, j):
        return remote(recv3.at[hf, j], recv5.at[hf, j], s5.at[hf, j], r5.at[hf, j], sib)

    def reduce_cores(hf, j):
        send1(hf, j).wait_recv()
        sums[hf, j] = sums[hf, j] + recv1[hf, j]
        send2(hf, j).start()

    def store_rows(hf, j, value, owner):
        for i in range(2):
            for s in range(4):
                ys_ref[s, 2 * hf + i, owner, :, cols(j)] = value[i * span + s * QB:i * span + (s + 1) * QB, :].astype(BF16)

    def finish(hf, j):
        send2(hf, j).wait_recv()
        ybuf[hf, j] = (x1[hf, :, cols(j)] + (sums[hf, j] + recv2[hf, j]) + bproj[:, cols(j)]).astype(BF16).astype(F32)
        send3(hf, j).start()
        send4(hf, j).start()
        store_rows(hf, j, ybuf[hf, j], me)

    def late(hf, j):
        send3(hf, j).wait_recv()
        send5(hf, j).start()
        store_rows(hf, j, recv3[hf, j], peers[2])
        send4(hf, j).wait_recv()
        store_rows(hf, j, recv4[hf, j], peers[1])
        send5(hf, j).wait_recv()
        store_rows(hf, j, recv5[hf, j], peers[3])

    def second(hf):
        def body(j, carry):
            weights(2 * hf + 1, j).wait()
            acc = dot(g[...], wbuf[j])
            part[hf, j] = acc[half:, :]
            send1(hf, j).start()
            sums[hf, j] = acc[:half, :]
            if hf == 0:
                weights(2, j).start()

            @pl.when(j > 0)
            def _():
                reduce_cores(hf, j - 1)

            if hf == 1:
                finish(0, j)
            return carry

        lax.fori_loop(0, n_blk, body, 0)
        reduce_cores(hf, n_blk - 1)

    for copy in local[:SQ]:
        copy.wait()
    project(0)
    x_copy.wait()
    enter(0, (own0, own1), (got0, got1))
    local[SQ].wait()
    for r in (1, 2, 3):
        send_part(r).wait_recv()
    project(1)
    gather_h(0)
    first(0)
    second(0)
    for i in range(2):
        swap_own(i).wait_recv()
    enter(1, (own_buf.at[0], own_buf.at[1]), (got_buf.at[0], got_buf.at[1]))
    gather_h(1)
    first(1)
    second(1)

    def drain(j, carry):
        late(0, j)
        finish(1, j)

        @pl.when(j > 0)
        def _():
            late(1, j - 1)

        return carry

    lax.fori_loop(0, n_blk, drain, 0)
    late(1, n_blk - 1)

    for r in range(1, SQ):
        send_part(r).wait_send()
    for i in range(2):
        swap_own(i).wait_send()
    for c in range(4):
        send_h(c).wait_send()

    def sent(j, carry):
        for hf in range(2):
            for send in (send1, send2, send3, send4, send5):
                send(hf, j).wait_send()
        return carry

    lax.fori_loop(0, n_blk, sent, 0)


def tail(x_view, vectors, own, got, ready, fresh, w_o, w_fc, w_proj):
    steps, chunks, _, _, dim = x_view.shape
    depth = w_o.shape[0]
    width = w_fc.shape[1] // 2
    n_blk = width // BLK
    span = 4 * QB
    any_spec = pl.BlockSpec(memory_space=pl.ANY)
    vmem = pl.BlockSpec(memory_space=pltpu.VMEM)
    blocks = lambda: pltpu.VMEM((2, n_blk, 2 * span, BLK), F32)
    sem = lambda *n: pltpu.SemaphoreType.DMA(n)
    return pl.pallas_call(
        functools.partial(tail_kernel, n_blk, depth // HEAD),
        in_specs=[any_spec] + [vmem] * (len(vectors) + 4) + [any_spec] * (2 * SQ + 3),
        out_specs=vmem,
        out_shape=jax.ShapeDtypeStruct((steps, chunks, SQ, QB, dim), BF16),
        scratch_shapes=[
            pltpu.VMEM((steps, chunks, QB, dim), BF16), pltpu.VMEM((2, SQ) + ready[0].shape, F32),
            pltpu.VMEM((span * depth // HEAD, HEAD), F32), pltpu.VMEM((span, depth), F32), pltpu.VMEM((dim // BLK, depth, BLK), BF16),
            pltpu.VMEM((2, span, dim), F32), pltpu.VMEM((2, span, dim), F32), pltpu.VMEM((2, 2 * span, dim), F32),
            pltpu.VMEM((chunks, span, dim), F32), pltpu.VMEM((chunks, span, dim), F32),
            pltpu.VMEM((4 * span, dim), BF16), pltpu.VMEM((4 * span, width), BF16), pltpu.VMEM((n_blk, dim, BLK), BF16),
            pltpu.VMEM((1, dim), F32), pltpu.VMEM((1, 2 * width), F32),
        ] + [blocks() for _ in range(8)]
        + [pltpu.SemaphoreType.DMA, sem(SQ + 1), sem(SQ), sem(SQ), sem(dim // BLK), sem(n_blk), sem(2), sem(2), sem(chunks), sem(chunks)]
        + [sem(2, n_blk) for _ in range(10)],
        compiler_params=pltpu.CompilerParams(vmem_limit_bytes=TAIL_VMEM, collective_id=0, has_side_effects=True),
        cost_estimate=pl.CostEstimate(flops=40_000_000_000, bytes_accessed=dim * width * 8, transcendentals=0),
        name="tail",
    )(x_view, *vectors, own[0], got[0], own[1], got[1], *ready, *fresh, w_o, w_fc, w_proj)


def solution(mesh):
    act_spec = P(None, "dp", None)
    cache_spec = P("dp", "sq", "tp", None)
    col_spec = P(None, "tp")
    row_spec = P("tp", None)
    vec_spec = P("tp")
    rep_spec = P(None)
    in_specs = (act_spec, P("dp"), cache_spec, cache_spec, col_spec, vec_spec, col_spec, vec_spec,
                col_spec, vec_spec, row_spec, rep_spec, rep_spec, rep_spec, rep_spec, rep_spec,
                col_spec, vec_spec, row_spec, rep_spec)
    out_specs = (act_spec, cache_spec, cache_spec)

    def swap_sq(value, mask):
        return lax.ppermute(value, "sq", [(i, i ^ mask) for i in range(SQ)])

    def swap_tp(value):
        return lax.ppermute(value, "tp", [(0, 1), (1, 0)])

    def per_device(x_steps, positions, key_buf, val_buf, w_q, b_q, w_k, b_k, w_v, b_v, w_o, b_o,
                   ln1_gain, ln1_bias, ln2_gain, ln2_bias, w_fc, b_fc, w_proj, b_proj):
        steps, batch, dim = x_steps.shape
        local = key_buf.shape[1]
        slots = local * SQ
        chunks = batch // CHUNK
        inv_freq = jnp.power(F32(ROPE_BASE), -2.0 * jnp.arange(HEAD // 2, dtype=F32) / HEAD)
        cur = positions[None, :] + jnp.arange(steps, dtype=jnp.int32)[:, None]
        angle = cur.reshape(-1).astype(F32)[:, None] * inv_freq
        q, kn, vn = qkv(x_steps, ln1_gain, ln1_bias, w_q, b_q, w_k, b_k, w_v, b_v, jnp.cos(angle), jnp.sin(angle))
        k_old, v_old = key_buf.reshape(batch, local, HEAD), val_buf.reshape(batch, local, HEAD)
        x_view = x_steps.reshape(steps, chunks, SQ, QB, dim)

        caches = None
        own, got = [], []
        waiting = None
        for c in range(chunks):
            res = attention(c, slots, positions, q, kn, vn, k_old, v_old, caches, own[c - 2:c - 1] if c >= 2 else [])
            caches = res[:2]
            if 1 <= c < chunks - 1:
                own.append(combine(waiting, w_o, res[2:3]))
                got.append(swap_tp(own[-1]))
            if c < chunks - 1:
                waiting = [res[2]] + [swap_sq(res[2 + r], r) for r in range(1, SQ)]
        ys = tail(x_view, (b_o, ln2_gain, ln2_bias, b_proj, b_fc), own, got, waiting, res[2:], w_o, w_fc, w_proj).reshape(steps, batch, dim)
        return ys, caches[0].reshape(key_buf.shape), caches[1].reshape(val_buf.shape)

    return jax.shard_map(per_device, mesh=mesh, in_specs=in_specs, out_specs=out_specs, check_vma=False)
```

```python
import functools
import math

import jax
import jax.numpy as jnp
from jax import lax
from jax.experimental import pallas as pl
from jax.experimental.pallas import tpu as pltpu
from jax.sharding import PartitionSpec as P

ROPE_BASE = 1000000.0
LN_EPS = 1e-5
NEG_BIG = -1e30
F32 = jnp.float32
BF16 = jnp.bfloat16
SQ = 4
QB = 8
NB = 4
CHUNK = SQ * QB
AHEAD = 3
HEAD = 128
VMEM_LIMIT = 60 * 1024 * 1024


def dot(a, b):
    return lax.dot_general(a, b, (((1,), (0,)), ((), ())), preferred_element_type=F32)


def dot_nt(a, b):
    return lax.dot_general(a, b, (((1,), (1,)), ((), ())), preferred_element_type=F32)


def layer_norm(vectors, gain, shift):
    row_mean = jnp.mean(vectors, axis=-1, keepdims=True)
    centered = vectors - row_mean
    row_var = jnp.mean(centered * centered, axis=-1, keepdims=True)
    return centered * lax.rsqrt(row_var + LN_EPS) * gain + shift


def params(n_grid, **kw):
    return pltpu.CompilerParams(dimension_semantics=("arbitrary",) * n_grid, vmem_limit_bytes=VMEM_LIMIT, **kw)


def as_row(ref):
    return ref[...].astype(F32).reshape(1, -1)


def qkv_kernel(x_hbm, gain_ref, shift_ref, wq_hbm, bq_ref, wk_hbm, bk_ref, wv_hbm, bv_ref, cos_ref, sin_ref,
               q_ref, k_ref, v_ref, x_ref, h_ref, wq, wkv, cos_t, sin_t, x_sem, w_sem):
    steps, batch = x_ref.shape[0], x_ref.shape[1]
    chunks = batch // CHUNK
    n_q = wq.shape[0]
    x_copies = [pltpu.make_async_copy(x_hbm.at[s], x_ref.at[s], x_sem.at[s]) for s in range(steps)]
    w_copies = [pltpu.make_async_copy(wq_hbm.at[:, pl.ds(j * 2 * HEAD, 2 * HEAD)], wq.at[j], w_sem.at[j]) for j in range(n_q)]
    w_copies += [pltpu.make_async_copy(src, wkv.at[:, pl.ds(i * HEAD, HEAD)], w_sem.at[n_q + i]) for i, src in enumerate((wk_hbm, wv_hbm))]
    for copy in x_copies:
        copy.start()
    gain, shift = as_row(gain_ref), as_row(shift_ref)
    cos_t[...] = jnp.concatenate([cos_ref[...], cos_ref[...]], axis=1)
    sin_t[...] = jnp.concatenate([-sin_ref[...], sin_ref[...]], axis=1)
    bias_q = as_row(bq_ref)
    bias_kv = jnp.concatenate([as_row(bk_ref), as_row(bv_ref)], axis=1)
    for s in range(steps):
        x_copies[s].wait()
        if s == 0:
            for copy in w_copies[n_q:] + w_copies[:n_q]:
                copy.start()
        for r in range(0, batch, 32):
            h_ref[s * batch + r:s * batch + r + 32, :] = layer_norm(x_ref[s, r:r + 32, :].astype(F32), gain, shift).astype(BF16)

    def rope(vec, rows):
        vec = vec.astype(BF16).astype(F32)
        out = vec * cos_t[rows, :] + pltpu.roll(vec, HEAD // 2, 1) * sin_t[rows, :]
        return out.astype(BF16).astype(F32)

    for copy in w_copies[n_q:]:
        copy.wait()
    acc = dot(h_ref[...], wkv[...]) + bias_kv
    for s in range(steps):
        for c in range(chunks):
            rows = slice(s * batch + c * CHUNK, s * batch + (c + 1) * CHUNK)
            k_ref[c, s] = rope(acc[rows, :HEAD], rows)
            v_ref[c, s] = acc[rows, HEAD:].astype(BF16).astype(F32)
    for s in range(steps, 8):
        for c in range(chunks):
            k_ref[c, s] = jnp.zeros((CHUNK, HEAD), F32)
            v_ref[c, s] = jnp.zeros((CHUNK, HEAD), F32)
    for j in range(n_q):
        w_copies[j].wait()
        acc = dot(h_ref[...], wq[j]) + bias_q[:, j * 2 * HEAD:(j + 1) * 2 * HEAD]
        for s in range(steps):
            for c in range(chunks):
                rows = slice(s * batch + c * CHUNK, s * batch + (c + 1) * CHUNK)
                for h in range(2):
                    q_ref[c, s, 2 * j + h] = rope(acc[rows, h * HEAD:(h + 1) * HEAD], rows)


def qkv(x_steps, gain, shift, w_q, b_q, w_k, b_k, w_v, b_v, cos_t, sin_t):
    steps, batch, dim = x_steps.shape
    chunks = batch // CHUNK
    heads = w_q.shape[1] // HEAD
    n_q = heads // 2
    rows = steps * batch
    any_spec = pl.BlockSpec(memory_space=pl.ANY)
    vmem = pl.BlockSpec(memory_space=pltpu.VMEM)
    return pl.pallas_call(
        qkv_kernel,
        in_specs=[any_spec, vmem, vmem, any_spec, vmem, any_spec, vmem, any_spec, vmem, vmem, vmem],
        out_specs=[vmem] * 3,
        out_shape=[
            jax.ShapeDtypeStruct((chunks, steps, heads, CHUNK, HEAD), F32),
            jax.ShapeDtypeStruct((chunks, 8, CHUNK, HEAD), F32),
            jax.ShapeDtypeStruct((chunks, 8, CHUNK, HEAD), F32),
        ],
        scratch_shapes=[
            pltpu.VMEM((steps, batch, dim), BF16), pltpu.VMEM((rows, dim), BF16), pltpu.VMEM((n_q, dim, 2 * HEAD), BF16), pltpu.VMEM((dim, 2 * HEAD), BF16),
            pltpu.VMEM((rows, HEAD), F32), pltpu.VMEM((rows, HEAD), F32), pltpu.SemaphoreType.DMA((steps,)), pltpu.SemaphoreType.DMA((n_q + 2,)),
        ],
        compiler_params=pltpu.CompilerParams(vmem_limit_bytes=VMEM_LIMIT),
        cost_estimate=pl.CostEstimate(flops=2 * rows * dim * (heads + 2) * HEAD, bytes_accessed=20_000_000, transcendentals=0),
        name="qkv",
    )(x_steps, gain, shift, w_q, b_q, w_k, b_k, w_v, b_v, cos_t, sin_t)


def attn_kernel(first, count, group, slots, n_any, pos_ref, q_hbm, kn_hbm, vn_hbm, k_hbm, v_hbm, *rest):
    ko_hbm, vo_hbm, *outs = rest[n_any:n_any + 6]
    kbuf, vbuf, q_ref, kn_ref, vn_ref, o_all, in_sem, out_sem, small_sem = rest[n_any + 6:]
    me = lax.axis_index("sq").astype(jnp.int32)
    per = CHUNK // NB
    n = count * per
    local = kbuf.shape[2]
    rows = 4 * group
    first_slot = me * local
    exp_scale = math.log2(math.e) * HEAD ** -0.5
    step_col = lax.broadcasted_iota(jnp.int32, (rows, 1), 0) // group
    lane = lax.broadcasted_iota(jnp.int32, (1, local), 1) + first_slot
    new_lane = lax.broadcasted_iota(jnp.int32, (1, 8), 1)
    diag = lax.broadcasted_iota(jnp.int32, (rows, HEAD), 0) == lax.broadcasted_iota(jnp.int32, (rows, HEAD), 1)
    row16 = lax.broadcasted_iota(jnp.int32, (16, HEAD), 0)

    def place(i):
        rel = 3 - i % per // 2
        return jnp.bitwise_xor(me, rel) * 2 + i % 2

    def seqs(i):
        return pl.ds((first + i // per) * CHUNK + place(i) * NB, NB)

    def loads(i):
        return (pltpu.make_async_copy(k_hbm.at[seqs(i)], kbuf.at[i], in_sem.at[0, i]),
                pltpu.make_async_copy(v_hbm.at[seqs(i)], vbuf.at[i], in_sem.at[1, i]))

    def stores(i):
        return (pltpu.make_async_copy(kbuf.at[i], ko_hbm.at[seqs(i)], out_sem.at[0, i]),
                pltpu.make_async_copy(vbuf.at[i], vo_hbm.at[seqs(i)], out_sem.at[1, i]))

    small = [pltpu.make_async_copy(src.at[pl.ds(first, count)], dst, small_sem.at[4 + t]) for t, (src, dst) in enumerate(((q_hbm, q_ref), (kn_hbm, kn_ref), (vn_hbm, vn_ref)))]
    for copy in small:
        copy.start()
    for i in range(AHEAD):
        for copy in loads(i):
            copy.start()
    for copy in small:
        copy.wait()

    def body(i, carry):
        @pl.when(i + AHEAD < n)
        def _():
            for copy in loads(i + AHEAD):
                copy.start()

        for copy in loads(i):
            copy.wait()

        @pl.when(i > 0)
        def _():
            for copy in stores(i - 1):
                copy.start()

        grp = place(i)
        chunk = first + i // per
        here = i // per
        out_at = o_all.at[3 - i % per // 2, here * 2 + i % 2]
        bls = [jnp.bitwise_and(jb + me, NB - 1) for jb in range(NB)]
        ids = [grp * NB + bl for bl in bls]
        queries = [q_ref[here, pl.ds(seq, rows, stride=CHUNK), :].astype(BF16) for seq in ids]
        new_keys = kn_ref[here, pl.ds(ids[0], 8, stride=CHUNK), :].astype(BF16)
        new_vals = vn_ref[here, pl.ds(ids[0], 8, stride=CHUNK), :].astype(BF16)
        scores = []
        for bl, seq, query in zip(bls, ids, queries):
            pos = pos_ref[chunk * CHUNK + seq]
            age = jnp.where(lane < pos, jnp.bitwise_and(lane - pos, slots - 1), 0)
            scores.append(jnp.where(age > step_col, dot_nt(query, kbuf[i, bl]), NEG_BIG))
        new_scores = jnp.where(new_lane <= step_col, dot_nt(queries[0], new_keys), NEG_BIG)
        tops = [jnp.max(sc, axis=1, keepdims=True) for sc in scores]
        tops[0] = jnp.maximum(tops[0], jnp.max(new_scores, axis=1, keepdims=True))
        results = []
        for jb, bl in enumerate(bls):
            weights = jnp.exp2((scores[jb] - tops[jb]) * exp_scale)
            part_sum = jnp.sum(weights, axis=1, keepdims=True)
            out = dot(weights.astype(BF16), vbuf[i, bl])
            if jb == 0:
                new_weights = jnp.exp2((new_scores - tops[0]) * exp_scale)
                part_sum = part_sum + jnp.sum(new_weights, axis=1, keepdims=True)
                out = out + dot(new_weights.astype(BF16), new_vals)
            results.append((bl, out, tops[jb], part_sum))
        for bl, out, top, part_sum in results:
            out_at[pl.ds(pl.multiple_of(bl * rows, 8), rows), :] = out
            out_at[pl.ds(NB * rows + bl, 1), :] = jnp.sum(jnp.where(diag, top, 0.0), axis=0, keepdims=True)
            out_at[pl.ds(NB * rows + NB + bl, 1), :] = jnp.sum(jnp.where(diag, part_sum, 0.0), axis=0, keepdims=True)

        for bl in range(NB):
            seq = grp * NB + bl
            begin = jnp.bitwise_and(pos_ref[chunk * CHUNK + seq], slots - 1) - first_slot
            near = jnp.bitwise_and(begin, slots - 1)

            @pl.when((near < local) | (near > slots - 4))
            def _(bl=bl, seq=seq, begin=begin):
                for t in range(4):
                    slot = jnp.bitwise_and(begin + t, slots - 1)

                    @pl.when(slot < local)
                    def _(t=t, slot=slot):
                        window = pl.ds(pl.multiple_of(slot // 16 * 16, 16), 16)
                        hit = row16 == slot % 16
                        for buf, new_ref in ((kbuf, kn_ref), (vbuf, vn_ref)):
                            new = new_ref[here, pl.ds(t * CHUNK + seq, 1), :]
                            buf[i, bl, window, :] = jnp.where(hit, new, buf[i, bl, window, :].astype(F32)).astype(BF16)

        return carry

    lax.fori_loop(0, n, body, 0)
    tails = [pltpu.make_async_copy(o_all.at[r], outs[r], small_sem.at[r]) for r in range(4)]
    for copy in tails + list(stores(n - 1)):
        copy.start()
    for i in range(n):
        for copy in stores(i):
            copy.wait()
    for copy in tails:
        copy.wait()


def attention(first, count, slots, positions, q, kn, vn, k_cache, v_cache, outs, after):
    batch, local, _ = k_cache.shape
    chunks = batch // CHUNK
    group = q.shape[2]
    rows = 4 * group
    n = count * CHUNK // NB
    width = NB * rows + 2 * NB
    n_alias = 0 if outs is None else 2
    n_any = n_alias + len(after)
    any_spec = pl.BlockSpec(memory_space=pl.ANY)
    part_shape = jax.ShapeDtypeStruct((2 * count, width, HEAD), F32)
    cache_shape = jax.ShapeDtypeStruct(k_cache.shape, BF16)
    return pl.pallas_call(
        functools.partial(attn_kernel, first, count, group, slots, n_any),
        in_specs=[pl.BlockSpec(memory_space=pltpu.SMEM)] + [any_spec] * (5 + n_any),
        out_specs=[any_spec] * 6,
        out_shape=[cache_shape, cache_shape] + [part_shape] * 4,
        scratch_shapes=[
            pltpu.VMEM((n, NB, local, HEAD), BF16), pltpu.VMEM((n, NB, local, HEAD), BF16),
            pltpu.VMEM((count, rows * CHUNK, HEAD), F32), pltpu.VMEM((count, 8 * CHUNK, HEAD), F32), pltpu.VMEM((count, 8 * CHUNK, HEAD), F32),
            pltpu.VMEM((4, 2 * count, width, HEAD), F32),
            pltpu.SemaphoreType.DMA((2, n)), pltpu.SemaphoreType.DMA((2, n)), pltpu.SemaphoreType.DMA((7,)),
        ],
        input_output_aliases={6: 0, 7: 1} if n_alias else {},
        compiler_params=pltpu.CompilerParams(vmem_limit_bytes=VMEM_LIMIT),
        cost_estimate=pl.CostEstimate(flops=10_000_000_000 * count, bytes_accessed=count * CHUNK * local * HEAD * 8, transcendentals=CHUNK * rows * local),
        name="attn",
    )(positions, q.reshape(chunks, rows * CHUNK, HEAD), kn.reshape(chunks, 8 * CHUNK, HEAD), vn.reshape(chunks, 8 * CHUNK, HEAD), k_cache, v_cache, *(outs or ()), *after)


def combine_rows(group, parts, at, a_scr, a32_scr):
    rows = 4 * group
    exp_scale = math.log2(math.e) * HEAD ** -0.5
    for g in range(2):
        stats = [parts[i, 2 * at + g, NB * rows:NB * rows + 2 * NB, :] for i in range(SQ)]
        top = functools.reduce(jnp.maximum, stats)
        scale = [jnp.exp2((st - top) * exp_scale) for st in stats]
        total = sum(sc * pltpu.roll(st, NB, 0) for sc, st in zip(scale, stats))
        scale = [(sc / total).T for sc in scale]
        sums = [sum(parts[i, 2 * at + g, b * rows:(b + 1) * rows, :] * sc[:rows, b:b + 1] for i, sc in enumerate(scale)) for b in range(NB)]
        for b, acc in enumerate(sums):
            a_scr[pl.ds((g * NB + b) * rows, rows), :] = acc
    for s in range(4):
        for h in range(group):
            a32_scr[(4 * at + s) * QB:(4 * at + s + 1) * QB, h * HEAD:(h + 1) * HEAD] = a_scr[pl.ds(s * group + h, QB, stride=rows), :]


def combine_kernel(group, p0_hbm, p1_hbm, p2_hbm, p3_hbm, wo_hbm, *rest):
    out_ref, parts, a_scr, a32_scr, wbuf, psem, wsem = rest[-7:]
    n, _, block = wbuf.shape
    gets = [pltpu.make_async_copy(p, parts.at[i], psem.at[i]) for i, p in enumerate((p0_hbm, p1_hbm, p2_hbm, p3_hbm))]
    weights = [pltpu.make_async_copy(wo_hbm.at[:, pl.ds(j * block, block)], wbuf.at[j], wsem.at[j]) for j in range(n)]
    for copy in gets + weights:
        copy.start()
    for copy in gets:
        copy.wait()
    for at in range(parts.shape[1] // 2):
        combine_rows(group, parts, at, a_scr, a32_scr)
    for j in range(n):
        weights[j].wait()
        out_ref[:, j * block:(j + 1) * block] = dot(a32_scr[...].astype(BF16), wbuf[j])


def combine(parts, w_o, after):
    depth, dim = w_o.shape
    group = depth // HEAD
    n, block = 6, dim // 6
    out_rows = parts[0].shape[0] * 2 * QB
    any_spec = pl.BlockSpec(memory_space=pl.ANY)
    return pl.pallas_call(
        functools.partial(combine_kernel, group),
        in_specs=[any_spec] * (5 + len(after)),
        out_specs=pl.BlockSpec(memory_space=pltpu.VMEM),
        out_shape=jax.ShapeDtypeStruct((out_rows, dim), F32),
        scratch_shapes=[
            pltpu.VMEM((SQ,) + parts[0].shape, F32), pltpu.VMEM((4 * group * QB, HEAD), F32), pltpu.VMEM((out_rows, depth), F32),
            pltpu.VMEM((n, depth, block), BF16), pltpu.SemaphoreType.DMA((SQ,)), pltpu.SemaphoreType.DMA((n,)),
        ],
        compiler_params=pltpu.CompilerParams(vmem_limit_bytes=VMEM_LIMIT),
        cost_estimate=pl.CostEstimate(flops=2_500_000_000, bytes_accessed=depth * dim * 2, transcendentals=0),
        name="combine_wo",
    )(*parts, w_o, *after)


MESH = pl.DeviceIdType.MESH
BLK = 512
TAIL_VMEM = 67_000_000


def tail_kernel(n_blk, group, x_ref, bo_ref, gain_ref, shift_ref, bproj_ref, bfc_ref, own_a, got_a, *refs):
    ready, fresh = refs[:SQ], refs[SQ:2 * SQ]
    (wo_ref, wfc_ref, wproj_ref, ys_ref, xs, pbuf, a_scr, a32_scr, wo, own_buf, got_buf, x1, hsend, hrecv, hall, g, wbuf, bproj, bfc,
     part, recv1, sums, recv2, ybuf, recv3, recv4, recv5,
     xsem, psem, fs, fr, wosem, wsem, os, og, hs, hr, s1, r1, s2, r2, s3, r3, s4, r4, s5, r5) = refs[2 * SQ:]
    me = lax.axis_index("sq").astype(jnp.int32)
    core = lax.rem(me, 2)
    peers = [me, me + 1 - 2 * core, lax.rem(me + 2, SQ), lax.rem(me + 3 - 2 * core, SQ)]
    sib, across = {"sq": peers[1]}, {"sq": peers[2]}
    partner = {"tp": 1 - lax.axis_index("tp")}
    span = 4 * QB
    half = 2 * span
    n_wo = wo.shape[0]

    def remote(src, dst, send, recv, device):
        return pltpu.make_async_remote_copy(src_ref=src, dst_ref=dst, send_sem=send, recv_sem=recv, device_id=device, device_id_type=MESH)

    def cols(j):
        return pl.ds(pl.multiple_of(j * BLK, BLK), BLK)

    def weights(kind, j):
        if kind % 2 == 0:
            src = wfc_ref.at[:, cols(core * n_blk + j)]
        else:
            src = wproj_ref.at[pl.ds(pl.multiple_of(core * n_blk * BLK, BLK), n_blk * BLK), cols(j)]
        return pltpu.make_async_copy(src, wbuf.at[j], wsem.at[j])

    def get_wo(j):
        return pltpu.make_async_copy(wo_ref.at[:, cols(j)], wo.at[j], wosem.at[j])

    def send_part(r):
        return remote(fresh[r], pbuf.at[1, r], fs.at[r], fr.at[r], {"sq": peers[r]})

    local = [pltpu.make_async_copy(ready[r], pbuf.at[0, r], psem.at[r]) for r in range(SQ)]
    local.append(pltpu.make_async_copy(fresh[0], pbuf.at[1, 0], psem.at[SQ]))
    x_copy = pltpu.make_async_copy(x_ref.at[:, :, me], xs, xsem)

    barrier = pltpu.get_barrier_semaphore()
    for device in ({"sq": peers[1]}, {"sq": peers[2]}, {"sq": peers[3]}, partner):
        pl.semaphore_signal(barrier, inc=1, device_id=device, device_id_type=MESH)
    for copy in local:
        copy.start()
    x_copy.start()
    for j in range(n_wo):
        get_wo(j).start()
    for j in range(n_blk):
        weights(0, j).start()
    pl.semaphore_wait(barrier, 4)
    for r in (2, 3, 1):
        send_part(r).start()

    bias, gain, shift = as_row(bo_ref), as_row(gain_ref), as_row(shift_ref)
    bproj[...] = as_row(bproj_ref)
    bfc[...] = as_row(bfc_ref)

    def swap_own(i, j):
        return remote(own_buf.at[i, j], got_buf.at[i, j], os.at[i, j], og.at[i, j], partner)

    def project(i):
        combine_rows(group, pbuf.at[i], 0, a_scr, a32_scr)

        def body(j, carry):
            if i == 0:
                get_wo(j).wait()
            own_buf[i, j] = dot(a32_scr[...].astype(BF16), wo[j])
            swap_own(i, j).start()
            return carry

        lax.fori_loop(0, n_wo, body, 0)

    def send_h(c):
        return remote(hsend.at[c], hrecv.at[c], hs.at[c], hr.at[c], sib)

    def enter(hf):
        for i in range(2):
            if hf == 0:
                delta = own_a[i * span:(i + 1) * span, :] + got_a[i * span:(i + 1) * span, :]
            else:
                for j in range(n_wo):
                    swap_own(i, j).wait_recv()
                delta = jnp.concatenate([own_buf[i, j] + got_buf[i, j] for j in range(n_wo)], axis=1)
            for s in range(4):
                mid = xs[s, 2 * hf + i].astype(F32) + delta[s * QB:(s + 1) * QB, :] + bias
                x1[hf, i * span + s * QB:i * span + (s + 1) * QB, :] = mid.astype(BF16).astype(F32)
            h = layer_norm(x1[hf, i * span:(i + 1) * span, :], gain, shift).astype(BF16)
            hall[i * span:(i + 1) * span, :] = h
            hsend[2 * hf + i] = h.astype(F32)
            send_h(2 * hf + i).start()

    def gather_h(hf):
        for i in range(2):
            send_h(2 * hf + i).wait_recv()
            hall[half + i * span:half + (i + 1) * span, :] = hrecv[2 * hf + i].astype(BF16)

    def first(hf):
        def body(j, carry):
            weights(2 * hf, j).wait()
            acc = dot(hall[...], wbuf[j]) + bfc[:, cols(core * n_blk + j)]
            g[:, cols(j)] = jax.nn.gelu(acc, approximate=True).astype(BF16)
            weights(2 * hf + 1, j).start()
            return carry

        lax.fori_loop(0, n_blk, body, 0)

    def send1(hf, j):
        return remote(part.at[hf, j], recv1.at[hf, j], s1.at[hf, j], r1.at[hf, j], sib)

    def send2(hf, j):
        return remote(sums.at[hf, j], recv2.at[hf, j], s2.at[hf, j], r2.at[hf, j], partner)

    def send3(hf, j):
        return remote(ybuf.at[hf, j], recv3.at[hf, j], s3.at[hf, j], r3.at[hf, j], across)

    def send4(hf, j):
        return remote(ybuf.at[hf, j], recv4.at[hf, j], s4.at[hf, j], r4.at[hf, j], sib)

    def send5(hf, j):
        return remote(recv3.at[hf, j], recv5.at[hf, j], s5.at[hf, j], r5.at[hf, j], sib)

    def reduce_cores(hf, j):
        send1(hf, j).wait_recv()
        sums[hf, j] = sums[hf, j] + recv1[hf, j]
        send2(hf, j).start()

    def store_rows(hf, j, value, owner):
        for i in range(2):
            for s in range(4):
                ys_ref[s, 2 * hf + i, owner, :, cols(j)] = value[i * span + s * QB:i * span + (s + 1) * QB, :].astype(BF16)

    def finish(hf, j):
        send2(hf, j).wait_recv()
        ybuf[hf, j] = (x1[hf, :, cols(j)] + (sums[hf, j] + recv2[hf, j]) + bproj[:, cols(j)]).astype(BF16).astype(F32)
        send3(hf, j).start()
        send4(hf, j).start()
        store_rows(hf, j, ybuf[hf, j], me)

    def late(hf, j):
        send3(hf, j).wait_recv()
        send5(hf, j).start()
        store_rows(hf, j, recv3[hf, j], peers[2])
        send4(hf, j).wait_recv()
        store_rows(hf, j, recv4[hf, j], peers[1])
        send5(hf, j).wait_recv()
        store_rows(hf, j, recv5[hf, j], peers[3])

    def second(hf):
        def body(j, carry):
            weights(2 * hf + 1, j).wait()
            acc = dot(g[...], wbuf[j])
            part[hf, j] = acc[half:, :]
            send1(hf, j).start()
            sums[hf, j] = acc[:half, :]
            if hf == 0:
                weights(2, j).start()

            @pl.when(j > 0)
            def _():
                reduce_cores(hf, j - 1)

            if hf == 1:
                finish(0, j)
            return carry

        lax.fori_loop(0, n_blk, body, 0)
        reduce_cores(hf, n_blk - 1)

    for copy in local[:SQ]:
        copy.wait()
    project(0)
    x_copy.wait()
    enter(0)
    local[SQ].wait()
    for r in (1, 2, 3):
        send_part(r).wait_recv()
    project(1)
    gather_h(0)
    first(0)
    second(0)
    enter(1)
    gather_h(1)
    first(1)
    second(1)

    def drain(j, carry):
        late(0, j)
        finish(1, j)

        @pl.when(j > 0)
        def _():
            late(1, j - 1)

        return carry

    lax.fori_loop(0, n_blk, drain, 0)
    late(1, n_blk - 1)

    for r in range(1, SQ):
        send_part(r).wait_send()
    for i in range(2):
        for j in range(n_wo):
            swap_own(i, j).wait_send()
    for c in range(4):
        send_h(c).wait_send()

    def sent(j, carry):
        for hf in range(2):
            for send in (send1, send2, send3, send4, send5):
                send(hf, j).wait_send()
        return carry

    lax.fori_loop(0, n_blk, sent, 0)


def tail(x_view, vectors, own, got, ready, fresh, w_o, w_fc, w_proj):
    steps, chunks, _, _, dim = x_view.shape
    depth = w_o.shape[0]
    width = w_fc.shape[1] // 2
    n_blk = width // BLK
    span = 4 * QB
    any_spec = pl.BlockSpec(memory_space=pl.ANY)
    vmem = pl.BlockSpec(memory_space=pltpu.VMEM)
    blocks = lambda: pltpu.VMEM((2, n_blk, 2 * span, BLK), F32)
    sem = lambda *n: pltpu.SemaphoreType.DMA(n)
    return pl.pallas_call(
        functools.partial(tail_kernel, n_blk, depth // HEAD),
        in_specs=[any_spec] + [vmem] * (len(vectors) + 2) + [any_spec] * (2 * SQ + 3),
        out_specs=vmem,
        out_shape=jax.ShapeDtypeStruct((steps, chunks, SQ, QB, dim), BF16),
        scratch_shapes=[
            pltpu.VMEM((steps, chunks, QB, dim), BF16), pltpu.VMEM((2, SQ) + ready[0].shape, F32),
            pltpu.VMEM((span * depth // HEAD, HEAD), F32), pltpu.VMEM((span, depth), F32), pltpu.VMEM((dim // BLK, depth, BLK), BF16),
            pltpu.VMEM((2, dim // BLK, span, BLK), F32), pltpu.VMEM((2, dim // BLK, span, BLK), F32), pltpu.VMEM((2, 2 * span, dim), F32),
            pltpu.VMEM((chunks, span, dim), F32), pltpu.VMEM((chunks, span, dim), F32),
            pltpu.VMEM((4 * span, dim), BF16), pltpu.VMEM((4 * span, width), BF16), pltpu.VMEM((n_blk, dim, BLK), BF16),
            pltpu.VMEM((1, dim), F32), pltpu.VMEM((1, 2 * width), F32),
        ] + [blocks() for _ in range(8)]
        + [pltpu.SemaphoreType.DMA, sem(SQ + 1), sem(SQ), sem(SQ), sem(dim // BLK), sem(n_blk), sem(2, dim // BLK), sem(2, dim // BLK), sem(chunks), sem(chunks)]
        + [sem(2, n_blk) for _ in range(10)],
        compiler_params=pltpu.CompilerParams(vmem_limit_bytes=TAIL_VMEM, collective_id=0, has_side_effects=True),
        cost_estimate=pl.CostEstimate(flops=40_000_000_000, bytes_accessed=dim * width * 8, transcendentals=0),
        name="tail",
    )(x_view, *vectors, own, got, *ready, *fresh, w_o, w_fc, w_proj)


def solution(mesh):
    act_spec = P(None, "dp", None)
    cache_spec = P("dp", "sq", "tp", None)
    col_spec = P(None, "tp")
    row_spec = P("tp", None)
    vec_spec = P("tp")
    rep_spec = P(None)
    in_specs = (act_spec, P("dp"), cache_spec, cache_spec, col_spec, vec_spec, col_spec, vec_spec,
                col_spec, vec_spec, row_spec, rep_spec, rep_spec, rep_spec, rep_spec, rep_spec,
                col_spec, vec_spec, row_spec, rep_spec)
    out_specs = (act_spec, cache_spec, cache_spec)

    def swap_sq(value, mask):
        return lax.ppermute(value, "sq", [(i, i ^ mask) for i in range(SQ)])

    def swap_tp(value):
        return lax.ppermute(value, "tp", [(0, 1), (1, 0)])

    def per_device(x_steps, positions, key_buf, val_buf, w_q, b_q, w_k, b_k, w_v, b_v, w_o, b_o,
                   ln1_gain, ln1_bias, ln2_gain, ln2_bias, w_fc, b_fc, w_proj, b_proj):
        steps, batch, dim = x_steps.shape
        local = key_buf.shape[1]
        slots = local * SQ
        chunks = batch // CHUNK
        inv_freq = jnp.power(F32(ROPE_BASE), -2.0 * jnp.arange(HEAD // 2, dtype=F32) / HEAD)
        cur = positions[None, :] + jnp.arange(steps, dtype=jnp.int32)[:, None]
        angle = cur.reshape(-1).astype(F32)[:, None] * inv_freq
        q, kn, vn = qkv(x_steps, ln1_gain, ln1_bias, w_q, b_q, w_k, b_k, w_v, b_v, jnp.cos(angle), jnp.sin(angle))
        k_old, v_old = key_buf.reshape(batch, local, HEAD), val_buf.reshape(batch, local, HEAD)
        x_view = x_steps.reshape(steps, chunks, SQ, QB, dim)

        half = chunks // 2

        def moved(parts):
            return [parts[0]] + [swap_sq(parts[r], r) for r in range(1, SQ)]

        first = attention(0, half, slots, positions, q, kn, vn, k_old, v_old, None, [])
        early = moved(first[2:])
        third = attention(half, 1, slots, positions, q, kn, vn, k_old, v_old, first[:2], [])
        own = combine(early, w_o, third[2:3])
        got = swap_tp(own)
        waiting = moved(third[2:])
        res = attention(half + 1, 1, slots, positions, q, kn, vn, k_old, v_old, third[:2], [own])
        caches = res[:2]
        ys = tail(x_view, (b_o, ln2_gain, ln2_bias, b_proj, b_fc), own, got, waiting, res[2:], w_o, w_fc, w_proj).reshape(steps, batch, dim)
        return ys, caches[0].reshape(key_buf.shape), caches[1].reshape(val_buf.shape)

    return jax.shard_map(per_device, mesh=mesh, in_specs=in_specs, out_specs=out_specs, check_vma=False)
```

```python
import functools
import math

import jax
import jax.numpy as jnp
from jax import lax
from jax.experimental import pallas as pl
from jax.experimental.pallas import tpu as pltpu
from jax.sharding import PartitionSpec as P

ROPE_BASE = 1000000.0
LN_EPS = 1e-5
NEG_BIG = -1e30
F32 = jnp.float32
BF16 = jnp.bfloat16
SQ = 4
QB = 8
NB = 4
CHUNK = SQ * QB
AHEAD = 3
HEAD = 128
VMEM_LIMIT = 60 * 1024 * 1024


def dot(a, b):
    return lax.dot_general(a, b, (((1,), (0,)), ((), ())), preferred_element_type=F32)


def dot_nt(a, b):
    return lax.dot_general(a, b, (((1,), (1,)), ((), ())), preferred_element_type=F32)


def layer_norm(vectors, gain, shift):
    row_mean = jnp.mean(vectors, axis=-1, keepdims=True)
    centered = vectors - row_mean
    row_var = jnp.mean(centered * centered, axis=-1, keepdims=True)
    return centered * lax.rsqrt(row_var + LN_EPS) * gain + shift


def params(n_grid, **kw):
    return pltpu.CompilerParams(dimension_semantics=("arbitrary",) * n_grid, vmem_limit_bytes=VMEM_LIMIT, **kw)


def as_row(ref):
    return ref[...].astype(F32).reshape(1, -1)


def qkv_kernel(x_hbm, gain_ref, shift_ref, wq_hbm, bq_ref, wk_hbm, bk_ref, wv_hbm, bv_ref, cos_ref, sin_ref,
               q_hbm, k_ref, v_ref, x_ref, h_ref, wq, wkv, cos_t, sin_t, bias_q, q_buf, x_sem, w_sem, q_sem):
    steps, batch = x_ref.shape[0], x_ref.shape[1]
    chunks = batch // CHUNK
    n_q = wq.shape[0]
    x_copies = [pltpu.make_async_copy(x_hbm.at[s], x_ref.at[s], x_sem.at[s]) for s in range(steps)]
    w_copies = [pltpu.make_async_copy(wq_hbm.at[:, pl.ds(j * 2 * HEAD, 2 * HEAD)], wq.at[j], w_sem.at[j]) for j in range(n_q)]
    w_copies += [pltpu.make_async_copy(src, wkv.at[:, pl.ds(i * HEAD, HEAD)], w_sem.at[n_q + i]) for i, src in enumerate((wk_hbm, wv_hbm))]
    for copy in x_copies:
        copy.start()
    gain, shift = as_row(gain_ref), as_row(shift_ref)
    cos_t[...] = jnp.concatenate([cos_ref[...], cos_ref[...]], axis=1)
    sin_t[...] = jnp.concatenate([-sin_ref[...], sin_ref[...]], axis=1)
    bias_q[...] = as_row(bq_ref)
    bias_kv = jnp.concatenate([as_row(bk_ref), as_row(bv_ref)], axis=1)
    tile = 64
    per = batch // tile

    def normalize(i, carry):
        s = i // per

        @pl.when(i % per == 0)
        def _():
            pltpu.make_async_copy(x_hbm.at[s], x_ref.at[s], x_sem.at[s]).wait()

        @pl.when(i == 0)
        def _():
            for copy in w_copies[n_q:] + w_copies[:n_q]:
                copy.start()

        rows = x_ref[s, pl.ds(pl.multiple_of(i % per * tile, tile), tile), :].astype(F32)
        h_ref[pl.ds(pl.multiple_of(i * tile, tile), tile), :] = layer_norm(rows, gain, shift).astype(BF16)
        return carry

    lax.fori_loop(0, steps * per, normalize, 0)

    def rope(vec, rows):
        vec = vec.astype(BF16).astype(F32)
        out = vec * cos_t[rows, :] + pltpu.roll(vec, HEAD // 2, 1) * sin_t[rows, :]
        return out.astype(BF16).astype(F32)

    for copy in w_copies[n_q:]:
        copy.wait()
    acc = dot(h_ref[...], wkv[...]) + bias_kv
    for s in range(steps):
        for c in range(chunks):
            rows = slice(s * batch + c * CHUNK, s * batch + (c + 1) * CHUNK)
            k_ref[c, s] = rope(acc[rows, :HEAD], rows)
            v_ref[c, s] = acc[rows, HEAD:].astype(BF16).astype(F32)
    for s in range(steps, 8):
        for c in range(chunks):
            k_ref[c, s] = jnp.zeros((CHUNK, HEAD), F32)
            v_ref[c, s] = jnp.zeros((CHUNK, HEAD), F32)

    def q_copy(j):
        return pltpu.make_async_copy(q_buf.at[j], q_hbm.at[:, :, pl.ds(2 * j, 2)], q_sem.at[j])

    def project(j, carry):
        pltpu.make_async_copy(wq_hbm.at[:, pl.ds(pl.multiple_of(j * 2 * HEAD, 2 * HEAD), 2 * HEAD)], wq.at[j], w_sem.at[j]).wait()
        acc = dot(h_ref[...], wq[j]) + bias_q[:, pl.ds(pl.multiple_of(j * 2 * HEAD, 2 * HEAD), 2 * HEAD)]
        for s in range(steps):
            for c in range(chunks):
                rows = slice(s * batch + c * CHUNK, s * batch + (c + 1) * CHUNK)
                for h in range(2):
                    q_buf[j, c, s, h] = rope(acc[rows, h * HEAD:(h + 1) * HEAD], rows)

        @pl.when(j > 0)
        def _():
            q_copy(j - 1).start()

        return carry

    lax.fori_loop(0, n_q, project, 0)
    q_copy(n_q - 1).start()
    for j in range(n_q):
        q_copy(j).wait()


def qkv(x_steps, gain, shift, w_q, b_q, w_k, b_k, w_v, b_v, cos_t, sin_t):
    steps, batch, dim = x_steps.shape
    chunks = batch // CHUNK
    heads = w_q.shape[1] // HEAD
    n_q = heads // 2
    rows = steps * batch
    any_spec = pl.BlockSpec(memory_space=pl.ANY)
    vmem = pl.BlockSpec(memory_space=pltpu.VMEM)
    return pl.pallas_call(
        qkv_kernel,
        in_specs=[any_spec, vmem, vmem, any_spec, vmem, any_spec, vmem, any_spec, vmem, vmem, vmem],
        out_specs=[any_spec, vmem, vmem],
        out_shape=[
            jax.ShapeDtypeStruct((chunks, steps, heads, CHUNK, HEAD), F32),
            jax.ShapeDtypeStruct((chunks, 8, CHUNK, HEAD), F32),
            jax.ShapeDtypeStruct((chunks, 8, CHUNK, HEAD), F32),
        ],
        scratch_shapes=[
            pltpu.VMEM((steps, batch, dim), BF16), pltpu.VMEM((rows, dim), BF16), pltpu.VMEM((n_q, dim, 2 * HEAD), BF16), pltpu.VMEM((dim, 2 * HEAD), BF16),
            pltpu.VMEM((rows, HEAD), F32), pltpu.VMEM((rows, HEAD), F32), pltpu.VMEM((1, heads * HEAD), F32), pltpu.VMEM((n_q, chunks, steps, 2, CHUNK, HEAD), F32),
            pltpu.SemaphoreType.DMA((steps,)), pltpu.SemaphoreType.DMA((n_q + 2,)), pltpu.SemaphoreType.DMA((n_q,)),
        ],
        compiler_params=pltpu.CompilerParams(vmem_limit_bytes=VMEM_LIMIT),
        cost_estimate=pl.CostEstimate(flops=2 * rows * dim * (heads + 2) * HEAD, bytes_accessed=20_000_000, transcendentals=0),
        name="qkv",
    )(x_steps, gain, shift, w_q, b_q, w_k, b_k, w_v, b_v, cos_t, sin_t)


def attn_kernel(first, count, group, slots, n_any, pos_ref, q_hbm, kn_hbm, vn_hbm, k_hbm, v_hbm, *rest):
    ko_hbm, vo_hbm, *outs = rest[n_any:n_any + 6]
    kbuf, vbuf, q_ref, kn_ref, vn_ref, o_all, in_sem, out_sem, small_sem = rest[n_any + 6:]
    me = lax.axis_index("sq").astype(jnp.int32)
    per = CHUNK // NB
    n = count * per
    local = kbuf.shape[2]
    rows = 4 * group
    first_slot = me * local
    exp_scale = math.log2(math.e) * HEAD ** -0.5
    step_col = lax.broadcasted_iota(jnp.int32, (rows, 1), 0) // group
    lane = lax.broadcasted_iota(jnp.int32, (1, local), 1) + first_slot
    new_lane = lax.broadcasted_iota(jnp.int32, (1, 8), 1)
    diag = lax.broadcasted_iota(jnp.int32, (rows, HEAD), 0) == lax.broadcasted_iota(jnp.int32, (rows, HEAD), 1)
    row16 = lax.broadcasted_iota(jnp.int32, (16, HEAD), 0)

    def place(i):
        rel = 3 - i % per // 2
        return jnp.bitwise_xor(me, rel) * 2 + i % 2

    def seqs(i):
        return pl.ds((first + i // per) * CHUNK + place(i) * NB, NB)

    def loads(i):
        return (pltpu.make_async_copy(k_hbm.at[seqs(i)], kbuf.at[i], in_sem.at[0, i]),
                pltpu.make_async_copy(v_hbm.at[seqs(i)], vbuf.at[i], in_sem.at[1, i]))

    def stores(i):
        return (pltpu.make_async_copy(kbuf.at[i], ko_hbm.at[seqs(i)], out_sem.at[0, i]),
                pltpu.make_async_copy(vbuf.at[i], vo_hbm.at[seqs(i)], out_sem.at[1, i]))

    small = [pltpu.make_async_copy(src.at[pl.ds(first, count)], dst, small_sem.at[4 + t]) for t, (src, dst) in enumerate(((q_hbm, q_ref), (kn_hbm, kn_ref), (vn_hbm, vn_ref)))]
    for copy in small:
        copy.start()
    for i in range(AHEAD):
        for copy in loads(i):
            copy.start()
    for copy in small:
        copy.wait()

    def body(i, carry):
        @pl.when(i + AHEAD < n)
        def _():
            for copy in loads(i + AHEAD):
                copy.start()

        for copy in loads(i):
            copy.wait()

        @pl.when(i > 0)
        def _():
            for copy in stores(i - 1):
                copy.start()

        grp = place(i)
        chunk = first + i // per
        here = i // per
        out_at = o_all.at[3 - i % per // 2, here * 2 + i % 2]
        bls = [jnp.bitwise_and(jb + me, NB - 1) for jb in range(NB)]
        ids = [grp * NB + bl for bl in bls]
        queries = [q_ref[here, pl.ds(seq, rows, stride=CHUNK), :].astype(BF16) for seq in ids]
        new_keys = kn_ref[here, pl.ds(ids[0], 8, stride=CHUNK), :].astype(BF16)
        new_vals = vn_ref[here, pl.ds(ids[0], 8, stride=CHUNK), :].astype(BF16)
        scores = []
        for bl, seq, query in zip(bls, ids, queries):
            pos = pos_ref[chunk * CHUNK + seq]
            age = jnp.where(lane < pos, jnp.bitwise_and(lane - pos, slots - 1), 0)
            scores.append(jnp.where(age > step_col, dot_nt(query, kbuf[i, bl]), NEG_BIG))
        new_scores = jnp.where(new_lane <= step_col, dot_nt(queries[0], new_keys), NEG_BIG)
        tops = [jnp.max(sc, axis=1, keepdims=True) for sc in scores]
        tops[0] = jnp.maximum(tops[0], jnp.max(new_scores, axis=1, keepdims=True))
        results = []
        for jb, bl in enumerate(bls):
            weights = jnp.exp2((scores[jb] - tops[jb]) * exp_scale)
            part_sum = jnp.sum(weights, axis=1, keepdims=True)
            out = dot(weights.astype(BF16), vbuf[i, bl])
            if jb == 0:
                new_weights = jnp.exp2((new_scores - tops[0]) * exp_scale)
                part_sum = part_sum + jnp.sum(new_weights, axis=1, keepdims=True)
                out = out + dot(new_weights.astype(BF16), new_vals)
            results.append((bl, out, tops[jb], part_sum))
        for bl, out, top, part_sum in results:
            out_at[pl.ds(pl.multiple_of(bl * rows, 8), rows), :] = out
            out_at[pl.ds(NB * rows + bl, 1), :] = jnp.sum(jnp.where(diag, top, 0.0), axis=0, keepdims=True)
            out_at[pl.ds(NB * rows + NB + bl, 1), :] = jnp.sum(jnp.where(diag, part_sum, 0.0), axis=0, keepdims=True)

        for bl in range(NB):
            seq = grp * NB + bl
            begin = jnp.bitwise_and(pos_ref[chunk * CHUNK + seq], slots - 1) - first_slot
            near = jnp.bitwise_and(begin, slots - 1)

            @pl.when((near < local) | (near > slots - 4))
            def _(bl=bl, seq=seq, begin=begin):
                for t in range(4):
                    slot = jnp.bitwise_and(begin + t, slots - 1)

                    @pl.when(slot < local)
                    def _(t=t, slot=slot):
                        window = pl.ds(pl.multiple_of(slot // 16 * 16, 16), 16)
                        hit = row16 == slot % 16
                        for buf, new_ref in ((kbuf, kn_ref), (vbuf, vn_ref)):
                            new = new_ref[here, pl.ds(t * CHUNK + seq, 1), :]
                            buf[i, bl, window, :] = jnp.where(hit, new, buf[i, bl, window, :].astype(F32)).astype(BF16)

        return carry

    lax.fori_loop(0, n, body, 0)
    tails = [pltpu.make_async_copy(o_all.at[r], outs[r], small_sem.at[r]) for r in range(4)]
    for copy in tails + list(stores(n - 1)):
        copy.start()
    for i in range(n):
        for copy in stores(i):
            copy.wait()
    for copy in tails:
        copy.wait()


def attention(first, count, slots, positions, q, kn, vn, k_cache, v_cache, outs, after):
    batch, local, _ = k_cache.shape
    chunks = batch // CHUNK
    group = q.shape[2]
    rows = 4 * group
    n = count * CHUNK // NB
    width = NB * rows + 2 * NB
    n_alias = 0 if outs is None else 2
    n_any = n_alias + len(after)
    any_spec = pl.BlockSpec(memory_space=pl.ANY)
    part_shape = jax.ShapeDtypeStruct((2 * count, width, HEAD), F32)
    cache_shape = jax.ShapeDtypeStruct(k_cache.shape, BF16)
    return pl.pallas_call(
        functools.partial(attn_kernel, first, count, group, slots, n_any),
        in_specs=[pl.BlockSpec(memory_space=pltpu.SMEM)] + [any_spec] * (5 + n_any),
        out_specs=[any_spec] * 6,
        out_shape=[cache_shape, cache_shape] + [part_shape] * 4,
        scratch_shapes=[
            pltpu.VMEM((n, NB, local, HEAD), BF16), pltpu.VMEM((n, NB, local, HEAD), BF16),
            pltpu.VMEM((count, rows * CHUNK, HEAD), F32), pltpu.VMEM((count, 8 * CHUNK, HEAD), F32), pltpu.VMEM((count, 8 * CHUNK, HEAD), F32),
            pltpu.VMEM((4, 2 * count, width, HEAD), F32),
            pltpu.SemaphoreType.DMA((2, n)), pltpu.SemaphoreType.DMA((2, n)), pltpu.SemaphoreType.DMA((7,)),
        ],
        input_output_aliases={6: 0, 7: 1} if n_alias else {},
        compiler_params=pltpu.CompilerParams(vmem_limit_bytes=VMEM_LIMIT),
        cost_estimate=pl.CostEstimate(flops=10_000_000_000 * count, bytes_accessed=count * CHUNK * local * HEAD * 8, transcendentals=CHUNK * rows * local),
        name="attn",
    )(positions, q.reshape(chunks, rows * CHUNK, HEAD), kn.reshape(chunks, 8 * CHUNK, HEAD), vn.reshape(chunks, 8 * CHUNK, HEAD), k_cache, v_cache, *(outs or ()), *after)


def combine_rows(group, parts, at, a_scr, a32_scr):
    rows = 4 * group
    exp_scale = math.log2(math.e) * HEAD ** -0.5
    for g in range(2):
        stats = [parts[i, 2 * at + g, NB * rows:NB * rows + 2 * NB, :] for i in range(SQ)]
        top = functools.reduce(jnp.maximum, stats)
        scale = [jnp.exp2((st - top) * exp_scale) for st in stats]
        total = sum(sc * pltpu.roll(st, NB, 0) for sc, st in zip(scale, stats))
        scale = [(sc / total).T for sc in scale]
        sums = [sum(parts[i, 2 * at + g, b * rows:(b + 1) * rows, :] * sc[:rows, b:b + 1] for i, sc in enumerate(scale)) for b in range(NB)]
        for b, acc in enumerate(sums):
            a_scr[pl.ds((g * NB + b) * rows, rows), :] = acc
    for s in range(4):
        for h in range(group):
            a32_scr[(4 * at + s) * QB:(4 * at + s + 1) * QB, h * HEAD:(h + 1) * HEAD] = a_scr[pl.ds(s * group + h, QB, stride=rows), :]


def combine_kernel(group, p0_hbm, p1_hbm, p2_hbm, p3_hbm, wo_hbm, *rest):
    out_ref, parts, a_scr, a32_scr, wbuf, psem, wsem = rest[-7:]
    n, _, block = wbuf.shape
    gets = [pltpu.make_async_copy(p, parts.at[i], psem.at[i]) for i, p in enumerate((p0_hbm, p1_hbm, p2_hbm, p3_hbm))]
    weights = [pltpu.make_async_copy(wo_hbm.at[:, pl.ds(j * block, block)], wbuf.at[j], wsem.at[j]) for j in range(n)]
    for copy in gets + weights:
        copy.start()
    for copy in gets:
        copy.wait()
    for at in range(parts.shape[1] // 2):
        combine_rows(group, parts, at, a_scr, a32_scr)
    for j in range(n):
        weights[j].wait()
        out_ref[:, j * block:(j + 1) * block] = dot(a32_scr[...].astype(BF16), wbuf[j])


def combine(parts, w_o, after):
    depth, dim = w_o.shape
    group = depth // HEAD
    n, block = 6, dim // 6
    out_rows = parts[0].shape[0] * 2 * QB
    any_spec = pl.BlockSpec(memory_space=pl.ANY)
    return pl.pallas_call(
        functools.partial(combine_kernel, group),
        in_specs=[any_spec] * (5 + len(after)),
        out_specs=pl.BlockSpec(memory_space=pltpu.VMEM),
        out_shape=jax.ShapeDtypeStruct((out_rows, dim), F32),
        scratch_shapes=[
            pltpu.VMEM((SQ,) + parts[0].shape, F32), pltpu.VMEM((4 * group * QB, HEAD), F32), pltpu.VMEM((out_rows, depth), F32),
            pltpu.VMEM((n, depth, block), BF16), pltpu.SemaphoreType.DMA((SQ,)), pltpu.SemaphoreType.DMA((n,)),
        ],
        compiler_params=pltpu.CompilerParams(vmem_limit_bytes=VMEM_LIMIT),
        cost_estimate=pl.CostEstimate(flops=2_500_000_000, bytes_accessed=depth * dim * 2, transcendentals=0),
        name="combine_wo",
    )(*parts, w_o, *after)


MESH = pl.DeviceIdType.MESH
BLK = 512
TAIL_VMEM = 67_000_000


def tail_kernel(n_blk, group, x_ref, bo_ref, gain_ref, shift_ref, bproj_ref, bfc_ref, own_hbm, got_hbm, *refs):
    ready, fresh = refs[:SQ], refs[SQ:2 * SQ]
    (wo_ref, wfc_ref, wproj_ref, ys_hbm, ys_ref, own_a, got_a, xs, pbuf, a_scr, a32_scr, wo, own_buf, got_buf, x1, hsend, hrecv, hall, g, wbuf, bproj, bfc,
     part, recv1, sums, recv2, ybuf, recv3, recv4, recv5,
     ysem, xsem, psem, fs, fr, wosem, wsem, os, og, hs, hr, s1, r1, s2, r2, s3, r3, s4, r4, s5, r5) = refs[2 * SQ:]
    me = lax.axis_index("sq").astype(jnp.int32)
    core = lax.rem(me, 2)
    peers = [me, me + 1 - 2 * core, lax.rem(me + 2, SQ), lax.rem(me + 3 - 2 * core, SQ)]
    sib, across = {"sq": peers[1]}, {"sq": peers[2]}
    partner = {"tp": 1 - lax.axis_index("tp")}
    span = 4 * QB
    half = 2 * span
    n_wo = wo.shape[0]

    def remote(src, dst, send, recv, device):
        return pltpu.make_async_remote_copy(src_ref=src, dst_ref=dst, send_sem=send, recv_sem=recv, device_id=device, device_id_type=MESH)

    def cols(j):
        return pl.ds(pl.multiple_of(j * BLK, BLK), BLK)

    def weights(kind, j):
        if kind % 2 == 0:
            src = wfc_ref.at[:, cols(core * n_blk + j)]
        else:
            src = wproj_ref.at[pl.ds(pl.multiple_of(core * n_blk * BLK, BLK), n_blk * BLK), cols(j)]
        return pltpu.make_async_copy(src, wbuf.at[j], wsem.at[j])

    def get_wo(j):
        return pltpu.make_async_copy(wo_ref.at[:, cols(j)], wo.at[j], wosem.at[j])

    def send_part(r):
        return remote(fresh[r], pbuf.at[1, r], fs.at[r], fr.at[r], {"sq": peers[r]})

    local = [pltpu.make_async_copy(ready[r], pbuf.at[0, r], psem.at[r]) for r in range(SQ)]
    local.append(pltpu.make_async_copy(fresh[0], pbuf.at[1, 0], psem.at[SQ]))
    x_copy = pltpu.make_async_copy(x_ref.at[:, :, me], xs, xsem)
    tops = [pltpu.make_async_copy(own_hbm, own_a, psem.at[SQ + 1]), pltpu.make_async_copy(got_hbm, got_a, psem.at[SQ + 2])]

    barrier = pltpu.get_barrier_semaphore()
    for device in ({"sq": peers[1]}, {"sq": peers[2]}, {"sq": peers[3]}, partner):
        pl.semaphore_signal(barrier, inc=1, device_id=device, device_id_type=MESH)
    for copy in local:
        copy.start()
    x_copy.start()
    for copy in tops:
        copy.start()
    for j in range(2):
        get_wo(j).start()
    pl.semaphore_wait(barrier, 4)
    for r in (2, 3, 1):
        send_part(r).start()
    for j in range(2, n_wo):
        get_wo(j).start()

    bias, gain, shift = as_row(bo_ref), as_row(gain_ref), as_row(shift_ref)
    bproj[...] = as_row(bproj_ref)
    bfc[...] = as_row(bfc_ref)

    def swap_own(i, j):
        return remote(own_buf.at[i, j], got_buf.at[i, j], os.at[i, j], og.at[i, j], partner)

    def project(i):
        combine_rows(group, pbuf.at[i], 0, a_scr, a32_scr)

        def body(j, carry):
            if i == 0:
                get_wo(j).wait()
            own_buf[i, j] = dot(a32_scr[...].astype(BF16), wo[j])
            swap_own(i, j).start()
            if i == 0:
                weights(0, j).start()
            return carry

        lax.fori_loop(0, n_wo, body, 0)

    def send_h(c):
        return remote(hsend.at[c], hrecv.at[c], hs.at[c], hr.at[c], sib)

    def enter(hf):
        for i in range(2):
            if hf == 0:
                delta = own_a[i * span:(i + 1) * span, :] + got_a[i * span:(i + 1) * span, :]
            else:
                for j in range(n_wo):
                    swap_own(i, j).wait_recv()
                delta = jnp.concatenate([own_buf[i, j] + got_buf[i, j] for j in range(n_wo)], axis=1)
            for s in range(4):
                mid = xs[s, 2 * hf + i].astype(F32) + delta[s * QB:(s + 1) * QB, :] + bias
                x1[hf, i * span + s * QB:i * span + (s + 1) * QB, :] = mid.astype(BF16).astype(F32)
            h = layer_norm(x1[hf, i * span:(i + 1) * span, :], gain, shift).astype(BF16)
            hall[i * span:(i + 1) * span, :] = h
            hsend[2 * hf + i] = h.astype(F32)
            send_h(2 * hf + i).start()

    def gather_h(hf):
        for i in range(2):
            send_h(2 * hf + i).wait_recv()
            hall[half + i * span:half + (i + 1) * span, :] = hrecv[2 * hf + i].astype(BF16)

    def first(hf):
        def body(j, carry):
            weights(2 * hf, j).wait()
            acc = dot(hall[...], wbuf[j]) + bfc[:, cols(core * n_blk + j)]
            g[:, cols(j)] = jax.nn.gelu(acc, approximate=True).astype(BF16)
            weights(2 * hf + 1, j).start()
            return carry

        lax.fori_loop(0, n_blk, body, 0)

    def send1(hf, j):
        return remote(part.at[hf, j], recv1.at[hf, j], s1.at[hf, j], r1.at[hf, j], sib)

    def send2(hf, j):
        return remote(sums.at[hf, j], recv2.at[hf, j], s2.at[hf, j], r2.at[hf, j], partner)

    def send3(hf, j):
        return remote(ybuf.at[hf, j], recv3.at[hf, j], s3.at[hf, j], r3.at[hf, j], across)

    def send4(hf, j):
        return remote(ybuf.at[hf, j], recv4.at[hf, j], s4.at[hf, j], r4.at[hf, j], sib)

    def send5(hf, j):
        return remote(recv3.at[hf, j], recv5.at[hf, j], s5.at[hf, j], r5.at[hf, j], sib)

    def reduce_cores(hf, j):
        send1(hf, j).wait_recv()
        sums[hf, j] = sums[hf, j] + recv1[hf, j]
        send2(hf, j).start()

    def store_rows(hf, j, value, owner):
        for i in range(2):
            for s in range(4):
                ys_ref[s, 2 * hf + i, owner, :, cols(j)] = value[i * span + s * QB:i * span + (s + 1) * QB, :].astype(BF16)

    def finish(hf, j):
        send2(hf, j).wait_recv()
        ybuf[hf, j] = (x1[hf, :, cols(j)] + (sums[hf, j] + recv2[hf, j]) + bproj[:, cols(j)]).astype(BF16).astype(F32)
        send3(hf, j).start()
        send4(hf, j).start()
        store_rows(hf, j, ybuf[hf, j], me)

    def ys_copy(hf, j):
        at = (slice(None), pl.ds(2 * hf, 2), slice(None), slice(None), cols(j))
        return pltpu.make_async_copy(ys_ref.at[at], ys_hbm.at[at], ysem.at[hf, j])

    def late(hf, j):
        send3(hf, j).wait_recv()
        send5(hf, j).start()
        store_rows(hf, j, recv3[hf, j], peers[2])
        send4(hf, j).wait_recv()
        store_rows(hf, j, recv4[hf, j], peers[1])
        send5(hf, j).wait_recv()
        store_rows(hf, j, recv5[hf, j], peers[3])
        ys_copy(hf, j).start()

    def second(hf):
        def body(j, carry):
            weights(2 * hf + 1, j).wait()
            acc = dot(g[...], wbuf[j])
            part[hf, j] = acc[half:, :]
            send1(hf, j).start()
            sums[hf, j] = acc[:half, :]
            if hf == 0:
                weights(2, j).start()

            @pl.when(j > 0)
            def _():
                reduce_cores(hf, j - 1)

            if hf == 1:
                finish(0, j)
            return carry

        lax.fori_loop(0, n_blk, body, 0)
        reduce_cores(hf, n_blk - 1)

    for copy in local[:SQ]:
        copy.wait()
    project(0)
    x_copy.wait()
    for copy in tops:
        copy.wait()
    enter(0)
    local[SQ].wait()
    for r in (1, 2, 3):
        send_part(r).wait_recv()
    project(1)
    gather_h(0)
    first(0)
    second(0)
    enter(1)
    gather_h(1)
    first(1)
    second(1)

    def drain(j, carry):
        late(0, j)
        finish(1, j)

        @pl.when(j > 0)
        def _():
            late(1, j - 1)

        return carry

    lax.fori_loop(0, n_blk, drain, 0)
    late(1, n_blk - 1)

    for r in range(1, SQ):
        send_part(r).wait_send()
    for i in range(2):
        for j in range(n_wo):
            swap_own(i, j).wait_send()
    for c in range(4):
        send_h(c).wait_send()

    def sent(j, carry):
        for hf in range(2):
            ys_copy(hf, j).wait()
            for send in (send1, send2, send3, send4, send5):
                send(hf, j).wait_send()
        return carry

    lax.fori_loop(0, n_blk, sent, 0)


def tail(x_view, vectors, own, got, ready, fresh, w_o, w_fc, w_proj):
    steps, chunks, _, _, dim = x_view.shape
    depth = w_o.shape[0]
    width = w_fc.shape[1] // 2
    n_blk = width // BLK
    span = 4 * QB
    any_spec = pl.BlockSpec(memory_space=pl.ANY)
    vmem = pl.BlockSpec(memory_space=pltpu.VMEM)
    blocks = lambda: pltpu.VMEM((2, n_blk, 2 * span, BLK), F32)
    sem = lambda *n: pltpu.SemaphoreType.DMA(n)
    return pl.pallas_call(
        functools.partial(tail_kernel, n_blk, depth // HEAD),
        in_specs=[any_spec] + [vmem] * len(vectors) + [any_spec] * (2 * SQ + 5),
        out_specs=any_spec,
        out_shape=jax.ShapeDtypeStruct((steps, chunks, SQ, QB, dim), BF16),
        scratch_shapes=[
            pltpu.VMEM((steps, chunks, SQ, QB, dim), BF16), pltpu.VMEM((2 * span, dim), F32), pltpu.VMEM((2 * span, dim), F32),
            pltpu.VMEM((steps, chunks, QB, dim), BF16), pltpu.VMEM((2, SQ) + ready[0].shape, F32),
            pltpu.VMEM((span * depth // HEAD, HEAD), F32), pltpu.VMEM((span, depth), F32), pltpu.VMEM((dim // BLK, depth, BLK), BF16),
            pltpu.VMEM((2, dim // BLK, span, BLK), F32), pltpu.VMEM((2, dim // BLK, span, BLK), F32), pltpu.VMEM((2, 2 * span, dim), F32),
            pltpu.VMEM((chunks, span, dim), F32), pltpu.VMEM((chunks, span, dim), F32),
            pltpu.VMEM((4 * span, dim), BF16), pltpu.VMEM((4 * span, width), BF16), pltpu.VMEM((n_blk, dim, BLK), BF16),
            pltpu.VMEM((1, dim), F32), pltpu.VMEM((1, 2 * width), F32),
        ] + [blocks() for _ in range(8)]
        + [sem(2, n_blk), pltpu.SemaphoreType.DMA, sem(SQ + 3), sem(SQ), sem(SQ), sem(dim // BLK), sem(n_blk), sem(2, dim // BLK), sem(2, dim // BLK), sem(chunks), sem(chunks)]
        + [sem(2, n_blk) for _ in range(10)],
        compiler_params=pltpu.CompilerParams(vmem_limit_bytes=TAIL_VMEM, collective_id=0, has_side_effects=True),
        cost_estimate=pl.CostEstimate(flops=40_000_000_000, bytes_accessed=dim * width * 8, transcendentals=0),
        name="tail",
    )(x_view, *vectors, own, got, *ready, *fresh, w_o, w_fc, w_proj)


def solution(mesh):
    act_spec = P(None, "dp", None)
    cache_spec = P("dp", "sq", "tp", None)
    col_spec = P(None, "tp")
    row_spec = P("tp", None)
    vec_spec = P("tp")
    rep_spec = P(None)
    in_specs = (act_spec, P("dp"), cache_spec, cache_spec, col_spec, vec_spec, col_spec, vec_spec,
                col_spec, vec_spec, row_spec, rep_spec, rep_spec, rep_spec, rep_spec, rep_spec,
                col_spec, vec_spec, row_spec, rep_spec)
    out_specs = (act_spec, cache_spec, cache_spec)

    def swap_sq(value, mask):
        return lax.ppermute(value, "sq", [(i, i ^ mask) for i in range(SQ)])

    def swap_tp(value):
        return lax.ppermute(value, "tp", [(0, 1), (1, 0)])

    def per_device(x_steps, positions, key_buf, val_buf, w_q, b_q, w_k, b_k, w_v, b_v, w_o, b_o,
                   ln1_gain, ln1_bias, ln2_gain, ln2_bias, w_fc, b_fc, w_proj, b_proj):
        steps, batch, dim = x_steps.shape
        local = key_buf.shape[1]
        slots = local * SQ
        chunks = batch // CHUNK
        inv_freq = jnp.power(F32(ROPE_BASE), -2.0 * jnp.arange(HEAD // 2, dtype=F32) / HEAD)
        cur = positions[None, :] + jnp.arange(steps, dtype=jnp.int32)[:, None]
        angle = cur.reshape(-1).astype(F32)[:, None] * inv_freq
        q, kn, vn = qkv(x_steps, ln1_gain, ln1_bias, w_q, b_q, w_k, b_k, w_v, b_v, jnp.cos(angle), jnp.sin(angle))
        k_old, v_old = key_buf.reshape(batch, local, HEAD), val_buf.reshape(batch, local, HEAD)
        x_view = x_steps.reshape(steps, chunks, SQ, QB, dim)

        half = chunks // 2

        def moved(parts):
            return [parts[0]] + [swap_sq(parts[r], r) for r in range(1, SQ)]

        first = attention(0, half, slots, positions, q, kn, vn, k_old, v_old, None, [])
        early = moved(first[2:])
        third = attention(half, 1, slots, positions, q, kn, vn, k_old, v_old, first[:2], [])
        own = combine(early, w_o, third[2:3])
        got = swap_tp(own)
        waiting = moved(third[2:])
        res = attention(half + 1, 1, slots, positions, q, kn, vn, k_old, v_old, third[:2], [own])
        caches = res[:2]
        ys = tail(x_view, (b_o, ln2_gain, ln2_bias, b_proj, b_fc), own, got, waiting, res[2:], w_o, w_fc, w_proj).reshape(steps, batch, dim)
        return ys, caches[0].reshape(key_buf.shape), caches[1].reshape(val_buf.shape)

    return jax.shard_map(per_device, mesh=mesh, in_specs=in_specs, out_specs=out_specs, check_vma=False)
```

```python
import functools
import math

import jax
import jax.numpy as jnp
from jax import lax
from jax.experimental import pallas as pl
from jax.experimental.pallas import tpu as pltpu
from jax.sharding import PartitionSpec as P

ROPE_BASE = 1000000.0
LN_EPS = 1e-5
NEG_BIG = -1e30
F32 = jnp.float32
BF16 = jnp.bfloat16
SQ = 4
QB = 8
NB = 4
CHUNK = SQ * QB
AHEAD = 3
HEAD = 128
VMEM_LIMIT = 60 * 1024 * 1024


def dot(a, b):
    return lax.dot_general(a, b, (((1,), (0,)), ((), ())), preferred_element_type=F32)


def dot_nt(a, b):
    return lax.dot_general(a, b, (((1,), (1,)), ((), ())), preferred_element_type=F32)


def layer_norm(vectors, gain, shift):
    row_mean = jnp.mean(vectors, axis=-1, keepdims=True)
    centered = vectors - row_mean
    row_var = jnp.mean(centered * centered, axis=-1, keepdims=True)
    return centered * lax.rsqrt(row_var + LN_EPS) * gain + shift


def params(n_grid, **kw):
    return pltpu.CompilerParams(dimension_semantics=("arbitrary",) * n_grid, vmem_limit_bytes=VMEM_LIMIT, **kw)


def as_row(ref):
    return ref[...].astype(F32).reshape(1, -1)


def qkv_kernel(x_hbm, gain_ref, shift_ref, wq_hbm, bq_ref, wk_hbm, bk_ref, wv_hbm, bv_ref, cos_ref, sin_ref,
               q_hbm, k_ref, v_ref, x_ref, h_ref, wq, wkv, cos_t, sin_t, bias_q, q_buf, x_sem, w_sem, q_sem):
    steps, batch = x_ref.shape[0], x_ref.shape[1]
    chunks = batch // CHUNK
    n_q = wq.shape[0]
    x_copies = [pltpu.make_async_copy(x_hbm.at[s], x_ref.at[s], x_sem.at[s]) for s in range(steps)]
    w_copies = [pltpu.make_async_copy(wq_hbm.at[:, pl.ds(j * 2 * HEAD, 2 * HEAD)], wq.at[j], w_sem.at[j]) for j in range(n_q)]
    w_copies += [pltpu.make_async_copy(src, wkv.at[:, pl.ds(i * HEAD, HEAD)], w_sem.at[n_q + i]) for i, src in enumerate((wk_hbm, wv_hbm))]
    for copy in x_copies:
        copy.start()
    gain, shift = as_row(gain_ref), as_row(shift_ref)
    cos_t[...] = jnp.concatenate([cos_ref[...], cos_ref[...]], axis=1)
    sin_t[...] = jnp.concatenate([-sin_ref[...], sin_ref[...]], axis=1)
    bias_q[...] = as_row(bq_ref)
    bias_kv = jnp.concatenate([as_row(bk_ref), as_row(bv_ref)], axis=1)
    tile = 64
    per = batch // tile

    def normalize(i, carry):
        s = i // per

        @pl.when(i % per == 0)
        def _():
            pltpu.make_async_copy(x_hbm.at[s], x_ref.at[s], x_sem.at[s]).wait()

        @pl.when(i == 0)
        def _():
            for copy in w_copies[n_q:] + w_copies[:n_q]:
                copy.start()

        rows = x_ref[s, pl.ds(pl.multiple_of(i % per * tile, tile), tile), :].astype(F32)
        h_ref[pl.ds(pl.multiple_of(i * tile, tile), tile), :] = layer_norm(rows, gain, shift).astype(BF16)
        return carry

    lax.fori_loop(0, steps * per, normalize, 0)

    def rope(vec, rows):
        vec = vec.astype(BF16).astype(F32)
        out = vec * cos_t[rows, :] + pltpu.roll(vec, HEAD // 2, 1) * sin_t[rows, :]
        return out.astype(BF16).astype(F32)

    for copy in w_copies[n_q:]:
        copy.wait()
    acc = dot(h_ref[...], wkv[...]) + bias_kv
    for s in range(steps):
        for c in range(chunks):
            rows = slice(s * batch + c * CHUNK, s * batch + (c + 1) * CHUNK)
            k_ref[c, s] = rope(acc[rows, :HEAD], rows)
            v_ref[c, s] = acc[rows, HEAD:].astype(BF16).astype(F32)
    for s in range(steps, 8):
        for c in range(chunks):
            k_ref[c, s] = jnp.zeros((CHUNK, HEAD), F32)
            v_ref[c, s] = jnp.zeros((CHUNK, HEAD), F32)

    def q_copy(j):
        return pltpu.make_async_copy(q_buf.at[j], q_hbm.at[:, :, pl.ds(2 * j, 2)], q_sem.at[j])

    def project(j, carry):
        pltpu.make_async_copy(wq_hbm.at[:, pl.ds(pl.multiple_of(j * 2 * HEAD, 2 * HEAD), 2 * HEAD)], wq.at[j], w_sem.at[j]).wait()
        acc = dot(h_ref[...], wq[j]) + bias_q[:, pl.ds(pl.multiple_of(j * 2 * HEAD, 2 * HEAD), 2 * HEAD)]
        for s in range(steps):
            for c in range(chunks):
                rows = slice(s * batch + c * CHUNK, s * batch + (c + 1) * CHUNK)
                for h in range(2):
                    q_buf[j, c, s, h] = rope(acc[rows, h * HEAD:(h + 1) * HEAD], rows)

        @pl.when(j > 0)
        def _():
            q_copy(j - 1).start()

        return carry

    lax.fori_loop(0, n_q, project, 0)
    q_copy(n_q - 1).start()
    for j in range(n_q):
        q_copy(j).wait()


def qkv(x_steps, gain, shift, w_q, b_q, w_k, b_k, w_v, b_v, cos_t, sin_t):
    steps, batch, dim = x_steps.shape
    chunks = batch // CHUNK
    heads = w_q.shape[1] // HEAD
    n_q = heads // 2
    rows = steps * batch
    any_spec = pl.BlockSpec(memory_space=pl.ANY)
    vmem = pl.BlockSpec(memory_space=pltpu.VMEM)
    return pl.pallas_call(
        qkv_kernel,
        in_specs=[any_spec, vmem, vmem, any_spec, vmem, any_spec, vmem, any_spec, vmem, vmem, vmem],
        out_specs=[any_spec, vmem, vmem],
        out_shape=[
            jax.ShapeDtypeStruct((chunks, steps, heads, CHUNK, HEAD), F32),
            jax.ShapeDtypeStruct((chunks, 8, CHUNK, HEAD), F32),
            jax.ShapeDtypeStruct((chunks, 8, CHUNK, HEAD), F32),
        ],
        scratch_shapes=[
            pltpu.VMEM((steps, batch, dim), BF16), pltpu.VMEM((rows, dim), BF16), pltpu.VMEM((n_q, dim, 2 * HEAD), BF16), pltpu.VMEM((dim, 2 * HEAD), BF16),
            pltpu.VMEM((rows, HEAD), F32), pltpu.VMEM((rows, HEAD), F32), pltpu.VMEM((1, heads * HEAD), F32), pltpu.VMEM((n_q, chunks, steps, 2, CHUNK, HEAD), F32),
            pltpu.SemaphoreType.DMA((steps,)), pltpu.SemaphoreType.DMA((n_q + 2,)), pltpu.SemaphoreType.DMA((n_q,)),
        ],
        compiler_params=pltpu.CompilerParams(vmem_limit_bytes=VMEM_LIMIT),
        cost_estimate=pl.CostEstimate(flops=2 * rows * dim * (heads + 2) * HEAD, bytes_accessed=20_000_000, transcendentals=0),
        name="qkv",
    )(x_steps, gain, shift, w_q, b_q, w_k, b_k, w_v, b_v, cos_t, sin_t)


def attn_kernel(first, count, group, slots, n_any, pos_ref, q_hbm, kn_hbm, vn_hbm, k_hbm, v_hbm, *rest):
    ko_hbm, vo_hbm, *outs = rest[n_any:n_any + 6]
    kbuf, vbuf, q_ref, kn_ref, vn_ref, o_all, in_sem, out_sem, small_sem = rest[n_any + 6:]
    me = lax.axis_index("sq").astype(jnp.int32)
    per = CHUNK // NB
    n = count * per
    local = kbuf.shape[2]
    rows = 4 * group
    first_slot = me * local
    exp_scale = math.log2(math.e) * HEAD ** -0.5
    step_col = lax.broadcasted_iota(jnp.int32, (rows, 1), 0) // group
    lane = lax.broadcasted_iota(jnp.int32, (1, local), 1) + first_slot
    new_lane = lax.broadcasted_iota(jnp.int32, (1, 8), 1)
    diag = lax.broadcasted_iota(jnp.int32, (rows, HEAD), 0) == lax.broadcasted_iota(jnp.int32, (rows, HEAD), 1)
    row16 = lax.broadcasted_iota(jnp.int32, (16, HEAD), 0)

    def place(i):
        rel = 3 - i % per // 2
        return jnp.bitwise_xor(me, rel) * 2 + i % 2

    def seqs(i):
        return pl.ds((first + i // per) * CHUNK + place(i) * NB, NB)

    def loads(i):
        return (pltpu.make_async_copy(k_hbm.at[seqs(i)], kbuf.at[i], in_sem.at[0, i]),
                pltpu.make_async_copy(v_hbm.at[seqs(i)], vbuf.at[i], in_sem.at[1, i]))

    def stores(i):
        return (pltpu.make_async_copy(kbuf.at[i], ko_hbm.at[seqs(i)], out_sem.at[0, i]),
                pltpu.make_async_copy(vbuf.at[i], vo_hbm.at[seqs(i)], out_sem.at[1, i]))

    small = [pltpu.make_async_copy(src.at[pl.ds(first, count)], dst, small_sem.at[4 + t]) for t, (src, dst) in enumerate(((q_hbm, q_ref), (kn_hbm, kn_ref), (vn_hbm, vn_ref)))]
    for copy in small:
        copy.start()
    for i in range(AHEAD):
        for copy in loads(i):
            copy.start()
    for copy in small:
        copy.wait()

    def body(i, carry):
        @pl.when(i + AHEAD < n)
        def _():
            for copy in loads(i + AHEAD):
                copy.start()

        for copy in loads(i):
            copy.wait()

        @pl.when(i > 0)
        def _():
            for copy in stores(i - 1):
                copy.start()

        grp = place(i)
        chunk = first + i // per
        here = i // per
        out_at = o_all.at[3 - i % per // 2, here * 2 + i % 2]
        bls = [jnp.bitwise_and(jb + me, NB - 1) for jb in range(NB)]
        ids = [grp * NB + bl for bl in bls]
        queries = [q_ref[here, pl.ds(seq, rows, stride=CHUNK), :].astype(BF16) for seq in ids]
        new_keys = kn_ref[here, pl.ds(ids[0], 8, stride=CHUNK), :].astype(BF16)
        new_vals = vn_ref[here, pl.ds(ids[0], 8, stride=CHUNK), :].astype(BF16)
        scores = []
        for bl, seq, query in zip(bls, ids, queries):
            pos = pos_ref[chunk * CHUNK + seq]
            age = jnp.where(lane < pos, jnp.bitwise_and(lane - pos, slots - 1), 0)
            scores.append(jnp.where(age > step_col, dot_nt(query, kbuf[i, bl]), NEG_BIG))
        new_scores = jnp.where(new_lane <= step_col, dot_nt(queries[0], new_keys), NEG_BIG)
        tops = [jnp.max(sc, axis=1, keepdims=True) for sc in scores]
        tops[0] = jnp.maximum(tops[0], jnp.max(new_scores, axis=1, keepdims=True))
        results = []
        for jb, bl in enumerate(bls):
            weights = jnp.exp2((scores[jb] - tops[jb]) * exp_scale)
            part_sum = jnp.sum(weights, axis=1, keepdims=True)
            out = dot(weights.astype(BF16), vbuf[i, bl])
            if jb == 0:
                new_weights = jnp.exp2((new_scores - tops[0]) * exp_scale)
                part_sum = part_sum + jnp.sum(new_weights, axis=1, keepdims=True)
                out = out + dot(new_weights.astype(BF16), new_vals)
            results.append((bl, out, tops[jb], part_sum))
        for bl, out, top, part_sum in results:
            out_at[pl.ds(pl.multiple_of(bl * rows, 8), rows), :] = out
            out_at[pl.ds(NB * rows + bl, 1), :] = jnp.sum(jnp.where(diag, top, 0.0), axis=0, keepdims=True)
            out_at[pl.ds(NB * rows + NB + bl, 1), :] = jnp.sum(jnp.where(diag, part_sum, 0.0), axis=0, keepdims=True)

        for bl in range(NB):
            seq = grp * NB + bl
            begin = jnp.bitwise_and(pos_ref[chunk * CHUNK + seq], slots - 1) - first_slot
            near = jnp.bitwise_and(begin, slots - 1)

            @pl.when((near < local) | (near > slots - 4))
            def _(bl=bl, seq=seq, begin=begin):
                for t in range(4):
                    slot = jnp.bitwise_and(begin + t, slots - 1)

                    @pl.when(slot < local)
                    def _(t=t, slot=slot):
                        window = pl.ds(pl.multiple_of(slot // 16 * 16, 16), 16)
                        hit = row16 == slot % 16
                        for buf, new_ref in ((kbuf, kn_ref), (vbuf, vn_ref)):
                            new = new_ref[here, pl.ds(t * CHUNK + seq, 1), :]
                            buf[i, bl, window, :] = jnp.where(hit, new, buf[i, bl, window, :].astype(F32)).astype(BF16)

        return carry

    lax.fori_loop(0, n, body, 0)
    tails = [pltpu.make_async_copy(o_all.at[r], outs[r], small_sem.at[r]) for r in range(4)]
    for copy in tails + list(stores(n - 1)):
        copy.start()
    for i in range(n):
        for copy in stores(i):
            copy.wait()
    for copy in tails:
        copy.wait()


def attention(first, count, slots, positions, q, kn, vn, k_cache, v_cache, outs, after):
    batch, local, _ = k_cache.shape
    chunks = batch // CHUNK
    group = q.shape[2]
    rows = 4 * group
    n = count * CHUNK // NB
    width = NB * rows + 2 * NB
    n_alias = 0 if outs is None else 2
    n_any = n_alias + len(after)
    any_spec = pl.BlockSpec(memory_space=pl.ANY)
    part_shape = jax.ShapeDtypeStruct((2 * count, width, HEAD), F32)
    cache_shape = jax.ShapeDtypeStruct(k_cache.shape, BF16)
    return pl.pallas_call(
        functools.partial(attn_kernel, first, count, group, slots, n_any),
        in_specs=[pl.BlockSpec(memory_space=pltpu.SMEM)] + [any_spec] * (5 + n_any),
        out_specs=[any_spec] * 6,
        out_shape=[cache_shape, cache_shape] + [part_shape] * 4,
        scratch_shapes=[
            pltpu.VMEM((n, NB, local, HEAD), BF16), pltpu.VMEM((n, NB, local, HEAD), BF16),
            pltpu.VMEM((count, rows * CHUNK, HEAD), F32), pltpu.VMEM((count, 8 * CHUNK, HEAD), F32), pltpu.VMEM((count, 8 * CHUNK, HEAD), F32),
            pltpu.VMEM((4, 2 * count, width, HEAD), F32),
            pltpu.SemaphoreType.DMA((2, n)), pltpu.SemaphoreType.DMA((2, n)), pltpu.SemaphoreType.DMA((7,)),
        ],
        input_output_aliases={6: 0, 7: 1} if n_alias else {},
        compiler_params=pltpu.CompilerParams(vmem_limit_bytes=VMEM_LIMIT),
        cost_estimate=pl.CostEstimate(flops=10_000_000_000 * count, bytes_accessed=count * CHUNK * local * HEAD * 8, transcendentals=CHUNK * rows * local),
        name="attn",
    )(positions, q.reshape(chunks, rows * CHUNK, HEAD), kn.reshape(chunks, 8 * CHUNK, HEAD), vn.reshape(chunks, 8 * CHUNK, HEAD), k_cache, v_cache, *(outs or ()), *after)


def combine_rows(group, parts, at, a_scr, a32_scr):
    rows = 4 * group
    exp_scale = math.log2(math.e) * HEAD ** -0.5
    for g in range(2):
        stats = [parts[i, 2 * at + g, NB * rows:NB * rows + 2 * NB, :] for i in range(SQ)]
        top = functools.reduce(jnp.maximum, stats)
        scale = [jnp.exp2((st - top) * exp_scale) for st in stats]
        total = sum(sc * pltpu.roll(st, NB, 0) for sc, st in zip(scale, stats))
        scale = [(sc / total).T for sc in scale]
        sums = [sum(parts[i, 2 * at + g, b * rows:(b + 1) * rows, :] * sc[:rows, b:b + 1] for i, sc in enumerate(scale)) for b in range(NB)]
        for b, acc in enumerate(sums):
            a_scr[pl.ds((g * NB + b) * rows, rows), :] = acc
    for s in range(4):
        for h in range(group):
            a32_scr[(4 * at + s) * QB:(4 * at + s + 1) * QB, h * HEAD:(h + 1) * HEAD] = a_scr[pl.ds(s * group + h, QB, stride=rows), :]


def combine_kernel(group, p0_hbm, p1_hbm, p2_hbm, p3_hbm, wo_hbm, *rest):
    out_hbm, parts, a_scr, a32_scr, a_bf, out_buf, wbuf, psem, wsem, osem = rest[-10:]
    n, _, block = wbuf.shape
    gets = [pltpu.make_async_copy(p, parts.at[i], psem.at[i]) for i, p in enumerate((p0_hbm, p1_hbm, p2_hbm, p3_hbm))]
    weights = [pltpu.make_async_copy(wo_hbm.at[:, pl.ds(j * block, block)], wbuf.at[j], wsem.at[j]) for j in range(n)]
    for copy in gets + weights:
        copy.start()
    for copy in gets:
        copy.wait()
    for at in range(parts.shape[1] // 2):
        combine_rows(group, parts, at, a_scr, a32_scr)
    a_bf[...] = a32_scr[...].astype(BF16)

    def columns(j):
        return pl.ds(pl.multiple_of(j * block, block), block)

    def out_copy(j):
        return pltpu.make_async_copy(out_buf.at[j], out_hbm.at[:, columns(j)], osem.at[j])

    def body(j, carry):
        pltpu.make_async_copy(wo_hbm.at[:, columns(j)], wbuf.at[j], wsem.at[j]).wait()
        out_buf[j] = dot(a_bf[...], wbuf[j])

        @pl.when(j > 0)
        def _():
            out_copy(j - 1).start()

        return carry

    lax.fori_loop(0, n, body, 0)
    out_copy(n - 1).start()
    for j in range(n):
        out_copy(j).wait()


def combine(parts, w_o, after):
    depth, dim = w_o.shape
    group = depth // HEAD
    n, block = 6, dim // 6
    out_rows = parts[0].shape[0] * 2 * QB
    any_spec = pl.BlockSpec(memory_space=pl.ANY)
    return pl.pallas_call(
        functools.partial(combine_kernel, group),
        in_specs=[any_spec] * (5 + len(after)),
        out_specs=any_spec,
        out_shape=jax.ShapeDtypeStruct((out_rows, dim), F32),
        scratch_shapes=[
            pltpu.VMEM((SQ,) + parts[0].shape, F32), pltpu.VMEM((4 * group * QB, HEAD), F32), pltpu.VMEM((out_rows, depth), F32),
            pltpu.VMEM((out_rows, depth), BF16), pltpu.VMEM((n, out_rows, block), F32), pltpu.VMEM((n, depth, block), BF16),
            pltpu.SemaphoreType.DMA((SQ,)), pltpu.SemaphoreType.DMA((n,)), pltpu.SemaphoreType.DMA((n,)),
        ],
        compiler_params=pltpu.CompilerParams(vmem_limit_bytes=VMEM_LIMIT),
        cost_estimate=pl.CostEstimate(flops=2_500_000_000, bytes_accessed=depth * dim * 2, transcendentals=0),
        name="combine_wo",
    )(*parts, w_o, *after)


MESH = pl.DeviceIdType.MESH
BLK = 512
TAIL_VMEM = 63_500_000


def tail_kernel(n_blk, group, x_ref, bo_ref, gain_ref, shift_ref, bproj_ref, bfc_ref, own_hbm, got_hbm, *refs):
    ready, fresh = refs[:SQ], refs[SQ:2 * SQ]
    (wo_ref, wfc_ref, wproj_ref, ys_ref, own_a, got_a, xs, pbuf, a_scr, a32_scr, wo, own_buf, got_buf, x1, hsend, hrecv, hall, g, wbuf, bproj, bfc,
     part, recv1, sums, recv2, ybuf, recv3, recv4, recv5,
     xsem, psem, fs, fr, wosem, wsem, os, og, hs, hr, s1, r1, s2, r2, s3, r3, s4, r4, s5, r5) = refs[2 * SQ:]
    me = lax.axis_index("sq").astype(jnp.int32)
    core = lax.rem(me, 2)
    peers = [me, me + 1 - 2 * core, lax.rem(me + 2, SQ), lax.rem(me + 3 - 2 * core, SQ)]
    sib, across = {"sq": peers[1]}, {"sq": peers[2]}
    partner = {"tp": 1 - lax.axis_index("tp")}
    span = 4 * QB
    half = 2 * span
    n_wo = wo.shape[0]

    def remote(src, dst, send, recv, device):
        return pltpu.make_async_remote_copy(src_ref=src, dst_ref=dst, send_sem=send, recv_sem=recv, device_id=device, device_id_type=MESH)

    def cols(j):
        return pl.ds(pl.multiple_of(j * BLK, BLK), BLK)

    def weights(kind, j):
        if kind % 2 == 0:
            src = wfc_ref.at[:, cols(core * n_blk + j)]
        else:
            src = wproj_ref.at[pl.ds(pl.multiple_of(core * n_blk * BLK, BLK), n_blk * BLK), cols(j)]
        return pltpu.make_async_copy(src, wbuf.at[j], wsem.at[j])

    def get_wo(j):
        return pltpu.make_async_copy(wo_ref.at[:, cols(j)], wo.at[j], wosem.at[j])

    def send_part(r):
        return remote(fresh[r], pbuf.at[1, r], fs.at[r], fr.at[r], {"sq": peers[r]})

    local = [pltpu.make_async_copy(ready[r], pbuf.at[0, r], psem.at[r]) for r in range(SQ)]
    local.append(pltpu.make_async_copy(fresh[0], pbuf.at[1, 0], psem.at[SQ]))
    x_copy = pltpu.make_async_copy(x_ref.at[:, :, me], xs, xsem)
    tops = [pltpu.make_async_copy(own_hbm, own_a, psem.at[SQ + 1]), pltpu.make_async_copy(got_hbm, got_a, psem.at[SQ + 2])]

    barrier = pltpu.get_barrier_semaphore()
    for device in ({"sq": peers[1]}, {"sq": peers[2]}, {"sq": peers[3]}, partner):
        pl.semaphore_signal(barrier, inc=1, device_id=device, device_id_type=MESH)
    for copy in local:
        copy.start()
    x_copy.start()
    for copy in tops:
        copy.start()
    for j in range(2):
        get_wo(j).start()
    pl.semaphore_wait(barrier, 4)
    for r in (2, 3, 1):
        send_part(r).start()
    for j in range(2, n_wo):
        get_wo(j).start()

    bias, gain, shift = as_row(bo_ref), as_row(gain_ref), as_row(shift_ref)
    bproj[...] = as_row(bproj_ref)
    bfc[...] = as_row(bfc_ref)

    def swap_own(i, j):
        return remote(own_buf.at[i, j], got_buf.at[i, j], os.at[i, j], og.at[i, j], partner)

    def project(i):
        combine_rows(group, pbuf.at[i], 0, a_scr, a32_scr)

        def body(j, carry):
            if i == 0:
                get_wo(j).wait()
            own_buf[i, j] = dot(a32_scr[...].astype(BF16), wo[j])
            swap_own(i, j).start()
            if i == 0:
                weights(0, j).start()
            return carry

        lax.fori_loop(0, n_wo, body, 0)

    def send_h(c):
        return remote(hsend.at[c], hrecv.at[c], hs.at[c], hr.at[c], sib)

    def enter(hf):
        for i in range(2):
            if hf == 0:
                delta = own_a[i * span:(i + 1) * span, :] + got_a[i * span:(i + 1) * span, :]
            else:
                for j in range(n_wo):
                    swap_own(i, j).wait_recv()
                delta = jnp.concatenate([own_buf[i, j] + got_buf[i, j] for j in range(n_wo)], axis=1)
            for s in range(4):
                mid = xs[s, 2 * hf + i].astype(F32) + delta[s * QB:(s + 1) * QB, :] + bias
                x1[hf, i * span + s * QB:i * span + (s + 1) * QB, :] = mid.astype(BF16).astype(F32)
            h = layer_norm(x1[hf, i * span:(i + 1) * span, :], gain, shift).astype(BF16)
            hall[i * span:(i + 1) * span, :] = h
            hsend[2 * hf + i] = h.astype(F32)
            send_h(2 * hf + i).start()

    def gather_h(hf):
        for i in range(2):
            send_h(2 * hf + i).wait_recv()
            hall[half + i * span:half + (i + 1) * span, :] = hrecv[2 * hf + i].astype(BF16)

    def first(hf):
        def body(j, carry):
            weights(2 * hf, j).wait()
            acc = dot(hall[...], wbuf[j]) + bfc[:, cols(core * n_blk + j)]
            g[:, cols(j)] = jax.nn.gelu(acc, approximate=True).astype(BF16)
            weights(2 * hf + 1, j).start()
            return carry

        lax.fori_loop(0, n_blk, body, 0)

    def send1(hf, j):
        return remote(part.at[hf, j], recv1.at[hf, j], s1.at[hf, j], r1.at[hf, j], sib)

    def send2(hf, j):
        return remote(sums.at[hf, j], recv2.at[hf, j], s2.at[hf, j], r2.at[hf, j], partner)

    def send3(hf, j):
        return remote(ybuf.at[hf, j], recv3.at[hf, j], s3.at[hf, j], r3.at[hf, j], across)

    def send4(hf, j):
        return remote(ybuf.at[hf, j], recv4.at[hf, j], s4.at[hf, j], r4.at[hf, j], sib)

    def send5(hf, j):
        return remote(recv3.at[hf, j], recv5.at[hf, j], s5.at[hf, j], r5.at[hf, j], sib)

    def reduce_cores(hf, j):
        send1(hf, j).wait_recv()
        sums[hf, j] = sums[hf, j] + recv1[hf, j]
        send2(hf, j).start()

    def store_rows(hf, j, value, owner):
        for i in range(2):
            for s in range(4):
                ys_ref[s, 2 * hf + i, owner, :, cols(j)] = value[i * span + s * QB:i * span + (s + 1) * QB, :].astype(BF16)

    def finish(hf, j):
        send2(hf, j).wait_recv()
        ybuf[hf, j] = (x1[hf, :, cols(j)] + (sums[hf, j] + recv2[hf, j]) + bproj[:, cols(j)]).astype(BF16).astype(F32)
        send3(hf, j).start()
        send4(hf, j).start()
        store_rows(hf, j, ybuf[hf, j], me)

    def late(hf, j):
        send3(hf, j).wait_recv()
        send5(hf, j).start()
        store_rows(hf, j, recv3[hf, j], peers[2])
        send4(hf, j).wait_recv()
        store_rows(hf, j, recv4[hf, j], peers[1])
        send5(hf, j).wait_recv()
        store_rows(hf, j, recv5[hf, j], peers[3])

    def second(hf):
        def body(j, carry):
            weights(2 * hf + 1, j).wait()
            acc = dot(g[...], wbuf[j])
            part[hf, j] = acc[half:, :]
            send1(hf, j).start()
            sums[hf, j] = acc[:half, :]
            if hf == 0:
                weights(2, j).start()

            @pl.when(j > 0)
            def _():
                reduce_cores(hf, j - 1)

            if hf == 1:
                finish(0, j)
            return carry

        lax.fori_loop(0, n_blk, body, 0)
        reduce_cores(hf, n_blk - 1)

    for copy in local[:SQ]:
        copy.wait()
    project(0)
    x_copy.wait()
    for copy in tops:
        copy.wait()
    enter(0)
    gather_h(0)
    first(0)
    local[SQ].wait()
    for r in (1, 2, 3):
        send_part(r).wait_recv()
    project(1)
    second(0)
    enter(1)
    gather_h(1)
    first(1)
    second(1)

    def drain(j, carry):
        late(0, j)
        finish(1, j)

        @pl.when(j > 0)
        def _():
            late(1, j - 1)

        return carry

    lax.fori_loop(0, n_blk, drain, 0)
    late(1, n_blk - 1)

    for r in range(1, SQ):
        send_part(r).wait_send()
    for i in range(2):
        for j in range(n_wo):
            swap_own(i, j).wait_send()
    for c in range(4):
        send_h(c).wait_send()

    def sent(j, carry):
        for hf in range(2):
            for send in (send1, send2, send3, send4, send5):
                send(hf, j).wait_send()
        return carry

    lax.fori_loop(0, n_blk, sent, 0)


def tail(x_view, vectors, own, got, ready, fresh, w_o, w_fc, w_proj):
    steps, chunks, _, _, dim = x_view.shape
    depth = w_o.shape[0]
    width = w_fc.shape[1] // 2
    n_blk = width // BLK
    span = 4 * QB
    any_spec = pl.BlockSpec(memory_space=pl.ANY)
    vmem = pl.BlockSpec(memory_space=pltpu.VMEM)
    blocks = lambda: pltpu.VMEM((2, n_blk, 2 * span, BLK), F32)
    sem = lambda *n: pltpu.SemaphoreType.DMA(n)
    return pl.pallas_call(
        functools.partial(tail_kernel, n_blk, depth // HEAD),
        in_specs=[any_spec] + [vmem] * len(vectors) + [any_spec] * (2 * SQ + 5),
        out_specs=vmem,
        out_shape=pltpu.VMEM((steps, chunks, SQ, QB, dim), BF16),
        scratch_shapes=[
            pltpu.VMEM((2 * span, dim), F32), pltpu.VMEM((2 * span, dim), F32),
            pltpu.VMEM((steps, chunks, QB, dim), BF16), pltpu.VMEM((2, SQ) + ready[0].shape, F32),
            pltpu.VMEM((span * depth // HEAD, HEAD), F32), pltpu.VMEM((span, depth), F32), pltpu.VMEM((dim // BLK, depth, BLK), BF16),
            pltpu.VMEM((2, dim // BLK, span, BLK), F32), pltpu.VMEM((2, dim // BLK, span, BLK), F32), pltpu.VMEM((2, 2 * span, dim), F32),
            pltpu.VMEM((chunks, span, dim), F32), pltpu.VMEM((chunks, span, dim), F32),
            pltpu.VMEM((4 * span, dim), BF16), pltpu.VMEM((4 * span, width), BF16), pltpu.VMEM((n_blk, dim, BLK), BF16),
            pltpu.VMEM((1, dim), F32), pltpu.VMEM((1, 2 * width), F32),
        ] + [blocks() for _ in range(8)]
        + [pltpu.SemaphoreType.DMA, sem(SQ + 3), sem(SQ), sem(SQ), sem(dim // BLK), sem(n_blk), sem(2, dim // BLK), sem(2, dim // BLK), sem(chunks), sem(chunks)]
        + [sem(2, n_blk) for _ in range(10)],
        compiler_params=pltpu.CompilerParams(vmem_limit_bytes=TAIL_VMEM, collective_id=0, has_side_effects=True),
        cost_estimate=pl.CostEstimate(flops=40_000_000_000, bytes_accessed=dim * width * 8, transcendentals=0),
        name="tail",
    )(x_view, *vectors, own, got, *ready, *fresh, w_o, w_fc, w_proj)


def solution(mesh):
    act_spec = P(None, "dp", None)
    cache_spec = P("dp", "sq", "tp", None)
    col_spec = P(None, "tp")
    row_spec = P("tp", None)
    vec_spec = P("tp")
    rep_spec = P(None)
    in_specs = (act_spec, P("dp"), cache_spec, cache_spec, col_spec, vec_spec, col_spec, vec_spec,
                col_spec, vec_spec, row_spec, rep_spec, rep_spec, rep_spec, rep_spec, rep_spec,
                col_spec, vec_spec, row_spec, rep_spec)
    out_specs = (act_spec, cache_spec, cache_spec)

    def swap_sq(value, mask):
        return lax.ppermute(value, "sq", [(i, i ^ mask) for i in range(SQ)])

    def swap_tp(value):
        return lax.ppermute(value, "tp", [(0, 1), (1, 0)])

    def per_device(x_steps, positions, key_buf, val_buf, w_q, b_q, w_k, b_k, w_v, b_v, w_o, b_o,
                   ln1_gain, ln1_bias, ln2_gain, ln2_bias, w_fc, b_fc, w_proj, b_proj):
        steps, batch, dim = x_steps.shape
        local = key_buf.shape[1]
        slots = local * SQ
        chunks = batch // CHUNK
        inv_freq = jnp.power(F32(ROPE_BASE), -2.0 * jnp.arange(HEAD // 2, dtype=F32) / HEAD)
        cur = positions[None, :] + jnp.arange(steps, dtype=jnp.int32)[:, None]
        angle = cur.reshape(-1).astype(F32)[:, None] * inv_freq
        q, kn, vn = qkv(x_steps, ln1_gain, ln1_bias, w_q, b_q, w_k, b_k, w_v, b_v, jnp.cos(angle), jnp.sin(angle))
        k_old, v_old = key_buf.reshape(batch, local, HEAD), val_buf.reshape(batch, local, HEAD)
        x_view = x_steps.reshape(steps, chunks, SQ, QB, dim)

        half = chunks // 2

        def moved(parts):
            return [parts[0]] + [swap_sq(parts[r], r) for r in range(1, SQ)]

        first = attention(0, half, slots, positions, q, kn, vn, k_old, v_old, None, [])
        early = moved(first[2:])
        third = attention(half, 1, slots, positions, q, kn, vn, k_old, v_old, first[:2], [])
        own = combine(early, w_o, third[2:3])
        got = swap_tp(own)
        waiting = moved(third[2:])
        res = attention(half + 1, 1, slots, positions, q, kn, vn, k_old, v_old, third[:2], [own])
        caches = res[:2]
        ys = tail(x_view, (b_o, ln2_gain, ln2_bias, b_proj, b_fc), own, got, waiting, res[2:], w_o, w_fc, w_proj).reshape(steps, batch, dim)
        return ys, caches[0].reshape(key_buf.shape), caches[1].reshape(val_buf.shape)

    return jax.shard_map(per_device, mesh=mesh, in_specs=in_specs, out_specs=out_specs, check_vma=False)
```

```python
import functools
import math

import jax
import jax.numpy as jnp
from jax import lax
from jax.experimental import pallas as pl
from jax.experimental.pallas import tpu as pltpu
from jax.sharding import PartitionSpec as P

ROPE_BASE = 1000000.0
LN_EPS = 1e-5
NEG_BIG = -1e30
F32 = jnp.float32
BF16 = jnp.bfloat16
SQ = 4
QB = 8
NB = 4
CHUNK = SQ * QB
AHEAD = 5
HEAD = 128
VMEM_LIMIT = 60 * 1024 * 1024


def dot(a, b):
    return lax.dot_general(a, b, (((1,), (0,)), ((), ())), preferred_element_type=F32)


def dot_nt(a, b):
    return lax.dot_general(a, b, (((1,), (1,)), ((), ())), preferred_element_type=F32)


def layer_norm(vectors, gain, shift):
    row_mean = jnp.mean(vectors, axis=-1, keepdims=True)
    centered = vectors - row_mean
    row_var = jnp.mean(centered * centered, axis=-1, keepdims=True)
    return centered * lax.rsqrt(row_var + LN_EPS) * gain + shift


def params(n_grid, **kw):
    return pltpu.CompilerParams(dimension_semantics=("arbitrary",) * n_grid, vmem_limit_bytes=VMEM_LIMIT, **kw)


def as_row(ref):
    return ref[...].astype(F32).reshape(1, -1)


def qkv_kernel(x_hbm, gain_ref, shift_ref, wq_hbm, bq_ref, wk_hbm, bk_ref, wv_hbm, bv_ref, cos_ref, sin_ref,
               q_hbm, k_ref, v_ref, x_ref, h_ref, wq, wkv, cos_t, sin_t, bias_q, q_buf, x_sem, w_sem, q_sem):
    steps, batch = x_ref.shape[0], x_ref.shape[1]
    chunks = batch // CHUNK
    n_q = wq.shape[0]
    x_copies = [pltpu.make_async_copy(x_hbm.at[s], x_ref.at[s], x_sem.at[s]) for s in range(steps)]
    w_copies = [pltpu.make_async_copy(wq_hbm.at[:, pl.ds(j * 2 * HEAD, 2 * HEAD)], wq.at[j], w_sem.at[j]) for j in range(n_q)]
    w_copies += [pltpu.make_async_copy(src, wkv.at[:, pl.ds(i * HEAD, HEAD)], w_sem.at[n_q + i]) for i, src in enumerate((wk_hbm, wv_hbm))]
    for copy in x_copies:
        copy.start()
    gain, shift = as_row(gain_ref), as_row(shift_ref)
    cos_t[...] = jnp.concatenate([cos_ref[...], cos_ref[...]], axis=1)
    sin_t[...] = jnp.concatenate([-sin_ref[...], sin_ref[...]], axis=1)
    bias_q[...] = as_row(bq_ref)
    bias_kv = jnp.concatenate([as_row(bk_ref), as_row(bv_ref)], axis=1)
    tile = 64
    per = batch // tile

    def normalize(i, carry):
        s = i // per

        @pl.when(i % per == 0)
        def _():
            pltpu.make_async_copy(x_hbm.at[s], x_ref.at[s], x_sem.at[s]).wait()

        @pl.when(i == 0)
        def _():
            for copy in w_copies[n_q:] + w_copies[:n_q]:
                copy.start()

        rows = x_ref[s, pl.ds(pl.multiple_of(i % per * tile, tile), tile), :].astype(F32)
        h_ref[pl.ds(pl.multiple_of(i * tile, tile), tile), :] = layer_norm(rows, gain, shift).astype(BF16)
        return carry

    lax.fori_loop(0, steps * per, normalize, 0)

    def rope(vec, rows):
        vec = vec.astype(BF16).astype(F32)
        out = vec * cos_t[rows, :] + pltpu.roll(vec, HEAD // 2, 1) * sin_t[rows, :]
        return out.astype(BF16).astype(F32)

    for copy in w_copies[n_q:]:
        copy.wait()
    acc = dot(h_ref[...], wkv[...]) + bias_kv
    for s in range(steps):
        for c in range(chunks):
            rows = slice(s * batch + c * CHUNK, s * batch + (c + 1) * CHUNK)
            k_ref[c, s] = rope(acc[rows, :HEAD], rows)
            v_ref[c, s] = acc[rows, HEAD:].astype(BF16).astype(F32)
    for s in range(steps, 8):
        for c in range(chunks):
            k_ref[c, s] = jnp.zeros((CHUNK, HEAD), F32)
            v_ref[c, s] = jnp.zeros((CHUNK, HEAD), F32)

    def q_copy(j):
        return pltpu.make_async_copy(q_buf.at[j], q_hbm.at[:, :, pl.ds(2 * j, 2)], q_sem.at[j])

    def project(j, carry):
        pltpu.make_async_copy(wq_hbm.at[:, pl.ds(pl.multiple_of(j * 2 * HEAD, 2 * HEAD), 2 * HEAD)], wq.at[j], w_sem.at[j]).wait()
        acc = dot(h_ref[...], wq[j]) + bias_q[:, pl.ds(pl.multiple_of(j * 2 * HEAD, 2 * HEAD), 2 * HEAD)]
        for s in range(steps):
            for c in range(chunks):
                rows = slice(s * batch + c * CHUNK, s * batch + (c + 1) * CHUNK)
                for h in range(2):
                    q_buf[j, c, s, h] = rope(acc[rows, h * HEAD:(h + 1) * HEAD], rows)

        @pl.when(j > 0)
        def _():
            q_copy(j - 1).start()

        return carry

    lax.fori_loop(0, n_q, project, 0)
    q_copy(n_q - 1).start()
    for j in range(n_q):
        q_copy(j).wait()


def qkv(x_steps, gain, shift, w_q, b_q, w_k, b_k, w_v, b_v, cos_t, sin_t):
    steps, batch, dim = x_steps.shape
    chunks = batch // CHUNK
    heads = w_q.shape[1] // HEAD
    n_q = heads // 2
    rows = steps * batch
    any_spec = pl.BlockSpec(memory_space=pl.ANY)
    vmem = pl.BlockSpec(memory_space=pltpu.VMEM)
    return pl.pallas_call(
        qkv_kernel,
        in_specs=[any_spec, vmem, vmem, any_spec, vmem, any_spec, vmem, any_spec, vmem, vmem, vmem],
        out_specs=[any_spec, vmem, vmem],
        out_shape=[
            jax.ShapeDtypeStruct((chunks, steps, heads, CHUNK, HEAD), F32),
            jax.ShapeDtypeStruct((chunks, 8, CHUNK, HEAD), F32),
            jax.ShapeDtypeStruct((chunks, 8, CHUNK, HEAD), F32),
        ],
        scratch_shapes=[
            pltpu.VMEM((steps, batch, dim), BF16), pltpu.VMEM((rows, dim), BF16), pltpu.VMEM((n_q, dim, 2 * HEAD), BF16), pltpu.VMEM((dim, 2 * HEAD), BF16),
            pltpu.VMEM((rows, HEAD), F32), pltpu.VMEM((rows, HEAD), F32), pltpu.VMEM((1, heads * HEAD), F32), pltpu.VMEM((n_q, chunks, steps, 2, CHUNK, HEAD), F32),
            pltpu.SemaphoreType.DMA((steps,)), pltpu.SemaphoreType.DMA((n_q + 2,)), pltpu.SemaphoreType.DMA((n_q,)),
        ],
        compiler_params=pltpu.CompilerParams(vmem_limit_bytes=VMEM_LIMIT),
        cost_estimate=pl.CostEstimate(flops=2 * rows * dim * (heads + 2) * HEAD, bytes_accessed=20_000_000, transcendentals=0),
        name="qkv",
    )(x_steps, gain, shift, w_q, b_q, w_k, b_k, w_v, b_v, cos_t, sin_t)


def attn_kernel(first, count, group, slots, n_any, pos_ref, q_hbm, kn_hbm, vn_hbm, k_hbm, v_hbm, *rest):
    ko_hbm, vo_hbm, *outs = rest[n_any:n_any + 6]
    kbuf, vbuf, q_ref, kn_ref, vn_ref, o_all, in_sem, out_sem, small_sem = rest[n_any + 6:]
    me = lax.axis_index("sq").astype(jnp.int32)
    per = CHUNK // NB
    n = count * per
    local = kbuf.shape[2]
    rows = 4 * group
    first_slot = me * local
    exp_scale = math.log2(math.e) * HEAD ** -0.5
    step_col = lax.broadcasted_iota(jnp.int32, (rows, 1), 0) // group
    lane = lax.broadcasted_iota(jnp.int32, (1, local), 1) + first_slot
    new_lane = lax.broadcasted_iota(jnp.int32, (1, 8), 1)
    diag = lax.broadcasted_iota(jnp.int32, (rows, HEAD), 0) == lax.broadcasted_iota(jnp.int32, (rows, HEAD), 1)
    row16 = lax.broadcasted_iota(jnp.int32, (16, HEAD), 0)

    def place(i):
        rel = 3 - i % per // 2
        return jnp.bitwise_xor(me, rel) * 2 + i % 2

    def seqs(i):
        return pl.ds((first + i // per) * CHUNK + place(i) * NB, NB)

    def loads(i):
        return (pltpu.make_async_copy(k_hbm.at[seqs(i)], kbuf.at[i], in_sem.at[0, i]),
                pltpu.make_async_copy(v_hbm.at[seqs(i)], vbuf.at[i], in_sem.at[1, i]))

    def stores(i):
        return (pltpu.make_async_copy(kbuf.at[i], ko_hbm.at[seqs(i)], out_sem.at[0, i]),
                pltpu.make_async_copy(vbuf.at[i], vo_hbm.at[seqs(i)], out_sem.at[1, i]))

    small = [pltpu.make_async_copy(src.at[pl.ds(first, count)], dst, small_sem.at[4 + t]) for t, (src, dst) in enumerate(((q_hbm, q_ref), (kn_hbm, kn_ref), (vn_hbm, vn_ref)))]
    for copy in small:
        copy.start()
    for i in range(2):
        for copy in loads(i):
            copy.start()
    for copy in small:
        copy.wait()

    def body(i, carry):
        for copy in loads(i):
            copy.wait()

        @pl.when(i < AHEAD - 2)
        def _():
            for copy in loads(2 * i + 2) + loads(2 * i + 3):
                copy.start()

        @pl.when((i >= AHEAD - 2) & (i + AHEAD < n))
        def _():
            for copy in loads(i + AHEAD):
                copy.start()

        @pl.when(i > 0)
        def _():
            for copy in stores(i - 1):
                copy.start()

        grp = place(i)
        chunk = first + i // per
        here = i // per
        out_at = o_all.at[3 - i % per // 2, here * 2 + i % 2]
        bls = [jnp.bitwise_and(jb + me, NB - 1) for jb in range(NB)]
        ids = [grp * NB + bl for bl in bls]
        queries = [q_ref[here, pl.ds(seq, rows, stride=CHUNK), :].astype(BF16) for seq in ids]
        new_keys = kn_ref[here, pl.ds(ids[0], 8, stride=CHUNK), :].astype(BF16)
        new_vals = vn_ref[here, pl.ds(ids[0], 8, stride=CHUNK), :].astype(BF16)
        scores = []
        for bl, seq, query in zip(bls, ids, queries):
            pos = pos_ref[chunk * CHUNK + seq]
            age = jnp.where(lane < pos, jnp.bitwise_and(lane - pos, slots - 1), 0)
            scores.append(jnp.where(age > step_col, dot_nt(query, kbuf[i, bl]), NEG_BIG))
        new_scores = jnp.where(new_lane <= step_col, dot_nt(queries[0], new_keys), NEG_BIG)
        tops = [jnp.max(sc, axis=1, keepdims=True) for sc in scores]
        tops[0] = jnp.maximum(tops[0], jnp.max(new_scores, axis=1, keepdims=True))
        results = []
        for jb, bl in enumerate(bls):
            weights = jnp.exp2((scores[jb] - tops[jb]) * exp_scale)
            part_sum = jnp.sum(weights, axis=1, keepdims=True)
            out = dot(weights.astype(BF16), vbuf[i, bl])
            if jb == 0:
                new_weights = jnp.exp2((new_scores - tops[0]) * exp_scale)
                part_sum = part_sum + jnp.sum(new_weights, axis=1, keepdims=True)
                out = out + dot(new_weights.astype(BF16), new_vals)
            results.append((bl, out, tops[jb], part_sum))
        for bl, out, top, part_sum in results:
            out_at[pl.ds(pl.multiple_of(bl * rows, 8), rows), :] = out
            out_at[pl.ds(NB * rows + bl, 1), :] = jnp.sum(jnp.where(diag, top, 0.0), axis=0, keepdims=True)
            out_at[pl.ds(NB * rows + NB + bl, 1), :] = jnp.sum(jnp.where(diag, part_sum, 0.0), axis=0, keepdims=True)

        for bl in range(NB):
            seq = grp * NB + bl
            begin = jnp.bitwise_and(pos_ref[chunk * CHUNK + seq], slots - 1) - first_slot
            near = jnp.bitwise_and(begin, slots - 1)

            @pl.when((near < local) | (near > slots - 4))
            def _(bl=bl, seq=seq, begin=begin):
                for t in range(4):
                    slot = jnp.bitwise_and(begin + t, slots - 1)

                    @pl.when(slot < local)
                    def _(t=t, slot=slot):
                        window = pl.ds(pl.multiple_of(slot // 16 * 16, 16), 16)
                        hit = row16 == slot % 16
                        for buf, new_ref in ((kbuf, kn_ref), (vbuf, vn_ref)):
                            new = new_ref[here, pl.ds(t * CHUNK + seq, 1), :]
                            buf[i, bl, window, :] = jnp.where(hit, new, buf[i, bl, window, :].astype(F32)).astype(BF16)

        return carry

    lax.fori_loop(0, n, body, 0)
    tails = [pltpu.make_async_copy(o_all.at[r], outs[r], small_sem.at[r]) for r in range(4)]
    for copy in tails + list(stores(n - 1)):
        copy.start()
    for i in range(n):
        for copy in stores(i):
            copy.wait()
    for copy in tails:
        copy.wait()


def attention(first, count, slots, positions, q, kn, vn, k_cache, v_cache, outs, after):
    batch, local, _ = k_cache.shape
    chunks = batch // CHUNK
    group = q.shape[2]
    rows = 4 * group
    n = count * CHUNK // NB
    width = NB * rows + 2 * NB
    n_alias = 0 if outs is None else 2
    n_any = n_alias + len(after)
    any_spec = pl.BlockSpec(memory_space=pl.ANY)
    part_shape = jax.ShapeDtypeStruct((2 * count, width, HEAD), F32)
    cache_shape = jax.ShapeDtypeStruct(k_cache.shape, BF16)
    return pl.pallas_call(
        functools.partial(attn_kernel, first, count, group, slots, n_any),
        in_specs=[pl.BlockSpec(memory_space=pltpu.SMEM)] + [any_spec] * (5 + n_any),
        out_specs=[any_spec] * 6,
        out_shape=[cache_shape, cache_shape] + [part_shape] * 4,
        scratch_shapes=[
            pltpu.VMEM((n, NB, local, HEAD), BF16), pltpu.VMEM((n, NB, local, HEAD), BF16),
            pltpu.VMEM((count, rows * CHUNK, HEAD), F32), pltpu.VMEM((count, 8 * CHUNK, HEAD), F32), pltpu.VMEM((count, 8 * CHUNK, HEAD), F32),
            pltpu.VMEM((4, 2 * count, width, HEAD), F32),
            pltpu.SemaphoreType.DMA((2, n)), pltpu.SemaphoreType.DMA((2, n)), pltpu.SemaphoreType.DMA((7,)),
        ],
        input_output_aliases={6: 0, 7: 1} if n_alias else {},
        compiler_params=pltpu.CompilerParams(vmem_limit_bytes=VMEM_LIMIT),
        cost_estimate=pl.CostEstimate(flops=10_000_000_000 * count, bytes_accessed=count * CHUNK * local * HEAD * 8, transcendentals=CHUNK * rows * local),
        name="attn",
    )(positions, q.reshape(chunks, rows * CHUNK, HEAD), kn.reshape(chunks, 8 * CHUNK, HEAD), vn.reshape(chunks, 8 * CHUNK, HEAD), k_cache, v_cache, *(outs or ()), *after)


def combine_rows(group, parts, at, a_scr, a32_scr):
    rows = 4 * group
    exp_scale = math.log2(math.e) * HEAD ** -0.5
    for g in range(2):
        stats = [parts[i, 2 * at + g, NB * rows:NB * rows + 2 * NB, :] for i in range(SQ)]
        top = functools.reduce(jnp.maximum, stats)
        scale = [jnp.exp2((st - top) * exp_scale) for st in stats]
        total = sum(sc * pltpu.roll(st, NB, 0) for sc, st in zip(scale, stats))
        scale = [(sc / total).T for sc in scale]
        sums = [sum(parts[i, 2 * at + g, b * rows:(b + 1) * rows, :] * sc[:rows, b:b + 1] for i, sc in enumerate(scale)) for b in range(NB)]
        for b, acc in enumerate(sums):
            a_scr[pl.ds((g * NB + b) * rows, rows), :] = acc
    for s in range(4):
        for h in range(group):
            a32_scr[(4 * at + s) * QB:(4 * at + s + 1) * QB, h * HEAD:(h + 1) * HEAD] = a_scr[pl.ds(s * group + h, QB, stride=rows), :]


def combine_kernel(group, p0_hbm, p1_hbm, p2_hbm, p3_hbm, wo_hbm, *rest):
    out_hbm, parts, a_scr, a32_scr, a_bf, out_buf, wbuf, psem, wsem, osem = rest[-10:]
    n, _, block = wbuf.shape
    gets = [pltpu.make_async_copy(p, parts.at[i], psem.at[i]) for i, p in enumerate((p0_hbm, p1_hbm, p2_hbm, p3_hbm))]
    weights = [pltpu.make_async_copy(wo_hbm.at[:, pl.ds(j * block, block)], wbuf.at[j], wsem.at[j]) for j in range(n)]
    for copy in gets + weights:
        copy.start()
    for copy in gets:
        copy.wait()
    for at in range(parts.shape[1] // 2):
        combine_rows(group, parts, at, a_scr, a32_scr)
    a_bf[...] = a32_scr[...].astype(BF16)

    def columns(j):
        return pl.ds(pl.multiple_of(j * block, block), block)

    def out_copy(j):
        return pltpu.make_async_copy(out_buf.at[j], out_hbm.at[:, columns(j)], osem.at[j])

    def body(j, carry):
        pltpu.make_async_copy(wo_hbm.at[:, columns(j)], wbuf.at[j], wsem.at[j]).wait()
        out_buf[j] = dot(a_bf[...], wbuf[j])

        @pl.when(j > 0)
        def _():
            out_copy(j - 1).start()

        return carry

    lax.fori_loop(0, n, body, 0)
    out_copy(n - 1).start()
    for j in range(n):
        out_copy(j).wait()


def combine(parts, w_o, after):
    depth, dim = w_o.shape
    group = depth // HEAD
    n, block = 6, dim // 6
    out_rows = parts[0].shape[0] * 2 * QB
    any_spec = pl.BlockSpec(memory_space=pl.ANY)
    return pl.pallas_call(
        functools.partial(combine_kernel, group),
        in_specs=[any_spec] * (5 + len(after)),
        out_specs=any_spec,
        out_shape=jax.ShapeDtypeStruct((out_rows, dim), F32),
        scratch_shapes=[
            pltpu.VMEM((SQ,) + parts[0].shape, F32), pltpu.VMEM((4 * group * QB, HEAD), F32), pltpu.VMEM((out_rows, depth), F32),
            pltpu.VMEM((out_rows, depth), BF16), pltpu.VMEM((n, out_rows, block), F32), pltpu.VMEM((n, depth, block), BF16),
            pltpu.SemaphoreType.DMA((SQ,)), pltpu.SemaphoreType.DMA((n,)), pltpu.SemaphoreType.DMA((n,)),
        ],
        compiler_params=pltpu.CompilerParams(vmem_limit_bytes=VMEM_LIMIT),
        cost_estimate=pl.CostEstimate(flops=2_500_000_000, bytes_accessed=depth * dim * 2, transcendentals=0),
        name="combine_wo",
    )(*parts, w_o, *after)


MESH = pl.DeviceIdType.MESH
BLK = 256
TAIL_VMEM = 63_500_000


def tail_kernel(n_blk, group, x_ref, bo_ref, gain_ref, shift_ref, bproj_ref, bfc_ref, own_hbm, got_hbm, *refs):
    ready, fresh = refs[:SQ], refs[SQ:2 * SQ]
    (wo_ref, wfc_ref, wproj_ref, ys_ref, own_a, got_a, xs, pbuf, a_scr, a32_scr, wo, own_buf, got_buf, x1, hsend, hrecv, hall, g, wbuf, bproj, bfc,
     part, recv1, sums, recv2, ybuf, recv3, recv4, recv5,
     xsem, psem, fs, fr, wosem, wsem, os, og, hs, hr, s1, r1, s2, r2, s3, r3, s4, r4, s5, r5) = refs[2 * SQ:]
    me = lax.axis_index("sq").astype(jnp.int32)
    core = lax.rem(me, 2)
    peers = [me, me + 1 - 2 * core, lax.rem(me + 2, SQ), lax.rem(me + 3 - 2 * core, SQ)]
    sib, across = {"sq": peers[1]}, {"sq": peers[2]}
    partner = {"tp": 1 - lax.axis_index("tp")}
    span = 4 * QB
    half = 2 * span
    n_wo = wo.shape[0]

    def remote(src, dst, send, recv, device):
        return pltpu.make_async_remote_copy(src_ref=src, dst_ref=dst, send_sem=send, recv_sem=recv, device_id=device, device_id_type=MESH)

    def cols(j):
        return pl.ds(pl.multiple_of(j * BLK, BLK), BLK)

    def weights(kind, j):
        if kind % 2 == 0:
            src = wfc_ref.at[:, cols(core * n_blk + j)]
        else:
            src = wproj_ref.at[pl.ds(pl.multiple_of(core * n_blk * BLK, BLK), n_blk * BLK), cols(j)]
        return pltpu.make_async_copy(src, wbuf.at[j], wsem.at[j])

    def get_wo(j):
        return pltpu.make_async_copy(wo_ref.at[:, cols(j)], wo.at[j], wosem.at[j])

    def send_part(r):
        return remote(fresh[r], pbuf.at[1, r], fs.at[r], fr.at[r], {"sq": peers[r]})

    local = [pltpu.make_async_copy(ready[r], pbuf.at[0, r], psem.at[r]) for r in range(SQ)]
    local.append(pltpu.make_async_copy(fresh[0], pbuf.at[1, 0], psem.at[SQ]))
    x_copy = pltpu.make_async_copy(x_ref.at[:, :, me], xs, xsem)
    tops = [pltpu.make_async_copy(own_hbm, own_a, psem.at[SQ + 1]), pltpu.make_async_copy(got_hbm, got_a, psem.at[SQ + 2])]

    barrier = pltpu.get_barrier_semaphore()
    for device in ({"sq": peers[1]}, {"sq": peers[2]}, {"sq": peers[3]}, partner):
        pl.semaphore_signal(barrier, inc=1, device_id=device, device_id_type=MESH)
    for copy in local:
        copy.start()
    x_copy.start()
    for copy in tops:
        copy.start()
    for j in range(2):
        get_wo(j).start()
    pl.semaphore_wait(barrier, 4)
    for r in (2, 3, 1):
        send_part(r).start()
    for j in range(2, n_wo):
        get_wo(j).start()

    bias, gain, shift = as_row(bo_ref), as_row(gain_ref), as_row(shift_ref)
    bproj[...] = as_row(bproj_ref)
    bfc[...] = as_row(bfc_ref)

    def swap_own(i, j):
        return remote(own_buf.at[i, j], got_buf.at[i, j], os.at[i, j], og.at[i, j], partner)

    def project(i):
        combine_rows(group, pbuf.at[i], 0, a_scr, a32_scr)

        def body(j, carry):
            if i == 0:
                get_wo(j).wait()
            own_buf[i, j] = dot(a32_scr[...].astype(BF16), wo[j])
            swap_own(i, j).start()
            if i == 0:
                weights(0, j).start()
            return carry

        lax.fori_loop(0, n_wo, body, 0)

    def send_h(c):
        return remote(hsend.at[c], hrecv.at[c], hs.at[c], hr.at[c], sib)

    def enter(hf):
        for i in range(2):
            if hf == 0:
                delta = own_a[i * span:(i + 1) * span, :] + got_a[i * span:(i + 1) * span, :]
            else:
                for j in range(n_wo):
                    swap_own(i, j).wait_recv()
                delta = jnp.concatenate([own_buf[i, j] + got_buf[i, j] for j in range(n_wo)], axis=1)
            for s in range(4):
                mid = xs[s, 2 * hf + i].astype(F32) + delta[s * QB:(s + 1) * QB, :] + bias
                x1[hf, i * span + s * QB:i * span + (s + 1) * QB, :] = mid.astype(BF16).astype(F32)
            h = layer_norm(x1[hf, i * span:(i + 1) * span, :], gain, shift).astype(BF16)
            hall[i * span:(i + 1) * span, :] = h
            hsend[2 * hf + i] = h.astype(F32)
            send_h(2 * hf + i).start()

    def gather_h(hf):
        for i in range(2):
            send_h(2 * hf + i).wait_recv()
            hall[half + i * span:half + (i + 1) * span, :] = hrecv[2 * hf + i].astype(BF16)

    def first(hf):
        def body(j, carry):
            weights(2 * hf, j).wait()
            acc = dot(hall[...], wbuf[j]) + bfc[:, cols(core * n_blk + j)]
            g[:, cols(j)] = jax.nn.gelu(acc, approximate=True).astype(BF16)
            weights(2 * hf + 1, j).start()
            return carry

        lax.fori_loop(0, n_blk, body, 0)

    def send1(hf, j):
        return remote(part.at[hf, j], recv1.at[hf, j], s1.at[hf, j], r1.at[hf, j], sib)

    def send2(hf, j):
        return remote(sums.at[hf, j], recv2.at[hf, j], s2.at[hf, j], r2.at[hf, j], partner)

    def send3(hf, j):
        return remote(ybuf.at[hf, j], recv3.at[hf, j], s3.at[hf, j], r3.at[hf, j], across)

    def send4(hf, j):
        return remote(ybuf.at[hf, j], recv4.at[hf, j], s4.at[hf, j], r4.at[hf, j], sib)

    def send5(hf, j):
        return remote(recv3.at[hf, j], recv5.at[hf, j], s5.at[hf, j], r5.at[hf, j], sib)

    def reduce_cores(hf, j):
        send1(hf, j).wait_recv()
        sums[hf, j] = sums[hf, j] + recv1[hf, j]
        send2(hf, j).start()

    def store_rows(hf, j, value, owner):
        for i in range(2):
            for s in range(4):
                ys_ref[s, 2 * hf + i, owner, :, cols(j)] = value[i * span + s * QB:i * span + (s + 1) * QB, :].astype(BF16)

    def finish(hf, j):
        send2(hf, j).wait_recv()
        ybuf[hf, j] = (x1[hf, :, cols(j)] + (sums[hf, j] + recv2[hf, j]) + bproj[:, cols(j)]).astype(BF16).astype(F32)
        send3(hf, j).start()
        send4(hf, j).start()
        store_rows(hf, j, ybuf[hf, j], me)

    def late(hf, j):
        send3(hf, j).wait_recv()
        send5(hf, j).start()
        store_rows(hf, j, recv3[hf, j], peers[2])
        send4(hf, j).wait_recv()
        store_rows(hf, j, recv4[hf, j], peers[1])
        send5(hf, j).wait_recv()
        store_rows(hf, j, recv5[hf, j], peers[3])

    def second(hf):
        def body(j, carry):
            weights(2 * hf + 1, j).wait()
            acc = dot(g[...], wbuf[j])
            part[hf, j] = acc[half:, :]
            send1(hf, j).start()
            sums[hf, j] = acc[:half, :]
            if hf == 0:
                weights(2, j).start()

            @pl.when(j > 1)
            def _():
                reduce_cores(hf, j - 2)

            if hf == 1:
                finish(0, j)
            return carry

        lax.fori_loop(0, n_blk, body, 0)
        reduce_cores(hf, n_blk - 2)
        reduce_cores(hf, n_blk - 1)

    for copy in local[:SQ]:
        copy.wait()
    project(0)
    x_copy.wait()
    for copy in tops:
        copy.wait()
    enter(0)
    gather_h(0)
    first(0)
    local[SQ].wait()
    for r in (1, 2, 3):
        send_part(r).wait_recv()
    project(1)
    second(0)
    enter(1)
    gather_h(1)
    first(1)
    second(1)

    def drain(j, carry):
        late(0, j)
        finish(1, j)

        @pl.when(j > 0)
        def _():
            late(1, j - 1)

        return carry

    lax.fori_loop(0, n_blk, drain, 0)
    late(1, n_blk - 1)

    for r in range(1, SQ):
        send_part(r).wait_send()
    for i in range(2):
        for j in range(n_wo):
            swap_own(i, j).wait_send()
    for c in range(4):
        send_h(c).wait_send()

    def sent(j, carry):
        for hf in range(2):
            for send in (send1, send2, send3, send4, send5):
                send(hf, j).wait_send()
        return carry

    lax.fori_loop(0, n_blk, sent, 0)


def tail(x_view, vectors, own, got, ready, fresh, w_o, w_fc, w_proj):
    steps, chunks, _, _, dim = x_view.shape
    depth = w_o.shape[0]
    width = w_fc.shape[1] // 2
    n_blk = width // BLK
    span = 4 * QB
    any_spec = pl.BlockSpec(memory_space=pl.ANY)
    vmem = pl.BlockSpec(memory_space=pltpu.VMEM)
    blocks = lambda: pltpu.VMEM((2, n_blk, 2 * span, BLK), F32)
    sem = lambda *n: pltpu.SemaphoreType.DMA(n)
    return pl.pallas_call(
        functools.partial(tail_kernel, n_blk, depth // HEAD),
        in_specs=[any_spec] + [vmem] * len(vectors) + [any_spec] * (2 * SQ + 5),
        out_specs=vmem,
        out_shape=pltpu.VMEM((steps, chunks, SQ, QB, dim), BF16),
        scratch_shapes=[
            pltpu.VMEM((2 * span, dim), F32), pltpu.VMEM((2 * span, dim), F32),
            pltpu.VMEM((steps, chunks, QB, dim), BF16), pltpu.VMEM((2, SQ) + ready[0].shape, F32),
            pltpu.VMEM((span * depth // HEAD, HEAD), F32), pltpu.VMEM((span, depth), F32), pltpu.VMEM((dim // BLK, depth, BLK), BF16),
            pltpu.VMEM((2, dim // BLK, span, BLK), F32), pltpu.VMEM((2, dim // BLK, span, BLK), F32), pltpu.VMEM((2, 2 * span, dim), F32),
            pltpu.VMEM((chunks, span, dim), F32), pltpu.VMEM((chunks, span, dim), F32),
            pltpu.VMEM((4 * span, dim), BF16), pltpu.VMEM((4 * span, width), BF16), pltpu.VMEM((n_blk, dim, BLK), BF16),
            pltpu.VMEM((1, dim), F32), pltpu.VMEM((1, 2 * width), F32),
        ] + [blocks() for _ in range(8)]
        + [pltpu.SemaphoreType.DMA, sem(SQ + 3), sem(SQ), sem(SQ), sem(dim // BLK), sem(n_blk), sem(2, dim // BLK), sem(2, dim // BLK), sem(chunks), sem(chunks)]
        + [sem(2, n_blk) for _ in range(10)],
        compiler_params=pltpu.CompilerParams(vmem_limit_bytes=TAIL_VMEM, collective_id=0, has_side_effects=True),
        cost_estimate=pl.CostEstimate(flops=40_000_000_000, bytes_accessed=dim * width * 8, transcendentals=0),
        name="tail",
    )(x_view, *vectors, own, got, *ready, *fresh, w_o, w_fc, w_proj)


def solution(mesh):
    act_spec = P(None, "dp", None)
    cache_spec = P("dp", "sq", "tp", None)
    col_spec = P(None, "tp")
    row_spec = P("tp", None)
    vec_spec = P("tp")
    rep_spec = P(None)
    in_specs = (act_spec, P("dp"), cache_spec, cache_spec, col_spec, vec_spec, col_spec, vec_spec,
                col_spec, vec_spec, row_spec, rep_spec, rep_spec, rep_spec, rep_spec, rep_spec,
                col_spec, vec_spec, row_spec, rep_spec)
    out_specs = (act_spec, cache_spec, cache_spec)

    def swap_sq(value, mask):
        return lax.ppermute(value, "sq", [(i, i ^ mask) for i in range(SQ)])

    def swap_tp(value):
        return lax.ppermute(value, "tp", [(0, 1), (1, 0)])

    def per_device(x_steps, positions, key_buf, val_buf, w_q, b_q, w_k, b_k, w_v, b_v, w_o, b_o,
                   ln1_gain, ln1_bias, ln2_gain, ln2_bias, w_fc, b_fc, w_proj, b_proj):
        steps, batch, dim = x_steps.shape
        local = key_buf.shape[1]
        slots = local * SQ
        chunks = batch // CHUNK
        inv_freq = jnp.power(F32(ROPE_BASE), -2.0 * jnp.arange(HEAD // 2, dtype=F32) / HEAD)
        cur = positions[None, :] + jnp.arange(steps, dtype=jnp.int32)[:, None]
        angle = cur.reshape(-1).astype(F32)[:, None] * inv_freq
        q, kn, vn = qkv(x_steps, ln1_gain, ln1_bias, w_q, b_q, w_k, b_k, w_v, b_v, jnp.cos(angle), jnp.sin(angle))
        k_old, v_old = key_buf.reshape(batch, local, HEAD), val_buf.reshape(batch, local, HEAD)
        x_view = x_steps.reshape(steps, chunks, SQ, QB, dim)

        half = chunks // 2

        def moved(parts):
            return [parts[0]] + [swap_sq(parts[r], r) for r in range(1, SQ)]

        first = attention(0, half, slots, positions, q, kn, vn, k_old, v_old, None, [])
        early = moved(first[2:])
        third = attention(half, 1, slots, positions, q, kn, vn, k_old, v_old, first[:2], [])
        own = combine(early, w_o, third[2:3])
        got = swap_tp(own)
        waiting = moved(third[2:])
        res = attention(half + 1, 1, slots, positions, q, kn, vn, k_old, v_old, third[:2], [own])
        caches = res[:2]
        ys = tail(x_view, (b_o, ln2_gain, ln2_bias, b_proj, b_fc), own, got, waiting, res[2:], w_o, w_fc, w_proj).reshape(steps, batch, dim)
        return ys, caches[0].reshape(key_buf.shape), caches[1].reshape(val_buf.shape)

    return jax.shard_map(per_device, mesh=mesh, in_specs=in_specs, out_specs=out_specs, check_vma=False)
```

```python
import functools
import math

import jax
import jax.numpy as jnp
from jax import lax
from jax.experimental import pallas as pl
from jax.experimental.pallas import tpu as pltpu
from jax.sharding import PartitionSpec as P

ROPE_BASE = 1000000.0
LN_EPS = 1e-5
NEG_BIG = -1e30
F32 = jnp.float32
BF16 = jnp.bfloat16
SQ = 4
QB = 8
NB = 4
CHUNK = SQ * QB
AHEAD = 5
HEAD = 128
VMEM_LIMIT = 60 * 1024 * 1024


def dot(a, b):
    return lax.dot_general(a, b, (((1,), (0,)), ((), ())), preferred_element_type=F32)


def dot_nt(a, b):
    return lax.dot_general(a, b, (((1,), (1,)), ((), ())), preferred_element_type=F32)


def layer_norm(vectors, gain, shift):
    row_mean = jnp.mean(vectors, axis=-1, keepdims=True)
    centered = vectors - row_mean
    row_var = jnp.mean(centered * centered, axis=-1, keepdims=True)
    return centered * lax.rsqrt(row_var + LN_EPS) * gain + shift


def params(n_grid, **kw):
    return pltpu.CompilerParams(dimension_semantics=("arbitrary",) * n_grid, vmem_limit_bytes=VMEM_LIMIT, **kw)


def as_row(ref):
    return ref[...].astype(F32).reshape(1, -1)


def qkv_kernel(x_hbm, gain_ref, shift_ref, wq_hbm, bq_ref, wk_hbm, bk_ref, wv_hbm, bv_ref, cos_ref, sin_ref,
               q_hbm, k_ref, v_ref, x_ref, h_ref, wq, wkv, cos_t, sin_t, bias_q, q_buf, x_sem, w_sem, q_sem):
    steps, batch = x_ref.shape[0], x_ref.shape[1]
    chunks = batch // CHUNK
    n_q = wq.shape[0]
    x_copies = [pltpu.make_async_copy(x_hbm.at[s], x_ref.at[s], x_sem.at[s]) for s in range(steps)]
    w_copies = [pltpu.make_async_copy(wq_hbm.at[:, pl.ds(j * 2 * HEAD, 2 * HEAD)], wq.at[j], w_sem.at[j]) for j in range(n_q)]
    w_copies += [pltpu.make_async_copy(src, wkv.at[:, pl.ds(i * HEAD, HEAD)], w_sem.at[n_q + i]) for i, src in enumerate((wk_hbm, wv_hbm))]
    for copy in x_copies:
        copy.start()
    gain, shift = as_row(gain_ref), as_row(shift_ref)
    cos_t[...] = jnp.concatenate([cos_ref[...], cos_ref[...]], axis=1)
    sin_t[...] = jnp.concatenate([-sin_ref[...], sin_ref[...]], axis=1)
    bias_q[...] = as_row(bq_ref)
    bias_kv = jnp.concatenate([as_row(bk_ref), as_row(bv_ref)], axis=1)
    tile = 64
    per = batch // tile

    def normalize(i, carry):
        s = i // per

        @pl.when(i % per == 0)
        def _():
            pltpu.make_async_copy(x_hbm.at[s], x_ref.at[s], x_sem.at[s]).wait()

        @pl.when(i == 0)
        def _():
            for copy in w_copies[n_q:] + w_copies[:n_q]:
                copy.start()

        rows = x_ref[s, pl.ds(pl.multiple_of(i % per * tile, tile), tile), :].astype(F32)
        h_ref[pl.ds(pl.multiple_of(i * tile, tile), tile), :] = layer_norm(rows, gain, shift).astype(BF16)
        return carry

    lax.fori_loop(0, steps * per, normalize, 0)

    def rope(vec, rows):
        vec = vec.astype(BF16).astype(F32)
        out = vec * cos_t[rows, :] + pltpu.roll(vec, HEAD // 2, 1) * sin_t[rows, :]
        return out.astype(BF16).astype(F32)

    for copy in w_copies[n_q:]:
        copy.wait()
    acc = dot(h_ref[...], wkv[...]) + bias_kv
    for s in range(steps):
        for c in range(chunks):
            rows = slice(s * batch + c * CHUNK, s * batch + (c + 1) * CHUNK)
            k_ref[c, s] = rope(acc[rows, :HEAD], rows)
            v_ref[c, s] = acc[rows, HEAD:].astype(BF16).astype(F32)
    for s in range(steps, 8):
        for c in range(chunks):
            k_ref[c, s] = jnp.zeros((CHUNK, HEAD), F32)
            v_ref[c, s] = jnp.zeros((CHUNK, HEAD), F32)

    def q_copy(j):
        return pltpu.make_async_copy(q_buf.at[j], q_hbm.at[:, :, pl.ds(2 * j, 2)], q_sem.at[j])

    def project(j, carry):
        pltpu.make_async_copy(wq_hbm.at[:, pl.ds(pl.multiple_of(j * 2 * HEAD, 2 * HEAD), 2 * HEAD)], wq.at[j], w_sem.at[j]).wait()
        acc = dot(h_ref[...], wq[j]) + bias_q[:, pl.ds(pl.multiple_of(j * 2 * HEAD, 2 * HEAD), 2 * HEAD)]
        for s in range(steps):
            for c in range(chunks):
                rows = slice(s * batch + c * CHUNK, s * batch + (c + 1) * CHUNK)
                for h in range(2):
                    q_buf[j, c, s, h] = rope(acc[rows, h * HEAD:(h + 1) * HEAD], rows)

        @pl.when(j > 0)
        def _():
            q_copy(j - 1).start()

        return carry

    lax.fori_loop(0, n_q, project, 0)
    q_copy(n_q - 1).start()
    for j in range(n_q):
        q_copy(j).wait()


def qkv(x_steps, gain, shift, w_q, b_q, w_k, b_k, w_v, b_v, cos_t, sin_t):
    steps, batch, dim = x_steps.shape
    chunks = batch // CHUNK
    heads = w_q.shape[1] // HEAD
    n_q = heads // 2
    rows = steps * batch
    any_spec = pl.BlockSpec(memory_space=pl.ANY)
    vmem = pl.BlockSpec(memory_space=pltpu.VMEM)
    return pl.pallas_call(
        qkv_kernel,
        in_specs=[any_spec, vmem, vmem, any_spec, vmem, any_spec, vmem, any_spec, vmem, vmem, vmem],
        out_specs=[any_spec, vmem, vmem],
        out_shape=[
            jax.ShapeDtypeStruct((chunks, steps, heads, CHUNK, HEAD), F32),
            jax.ShapeDtypeStruct((chunks, 8, CHUNK, HEAD), F32),
            jax.ShapeDtypeStruct((chunks, 8, CHUNK, HEAD), F32),
        ],
        scratch_shapes=[
            pltpu.VMEM((steps, batch, dim), BF16), pltpu.VMEM((rows, dim), BF16), pltpu.VMEM((n_q, dim, 2 * HEAD), BF16), pltpu.VMEM((dim, 2 * HEAD), BF16),
            pltpu.VMEM((rows, HEAD), F32), pltpu.VMEM((rows, HEAD), F32), pltpu.VMEM((1, heads * HEAD), F32), pltpu.VMEM((n_q, chunks, steps, 2, CHUNK, HEAD), F32),
            pltpu.SemaphoreType.DMA((steps,)), pltpu.SemaphoreType.DMA((n_q + 2,)), pltpu.SemaphoreType.DMA((n_q,)),
        ],
        compiler_params=pltpu.CompilerParams(vmem_limit_bytes=VMEM_LIMIT),
        cost_estimate=pl.CostEstimate(flops=2 * rows * dim * (heads + 2) * HEAD, bytes_accessed=20_000_000, transcendentals=0),
        name="qkv",
    )(x_steps, gain, shift, w_q, b_q, w_k, b_k, w_v, b_v, cos_t, sin_t)


def attn_kernel(first, count, group, slots, n_any, pos_ref, q_hbm, kn_hbm, vn_hbm, k_hbm, v_hbm, *rest):
    ko_hbm, vo_hbm, *outs = rest[n_any:n_any + 6]
    kbuf, vbuf, q_ref, kn_ref, vn_ref, o_all, in_sem, out_sem, small_sem = rest[n_any + 6:]
    me = lax.axis_index("sq").astype(jnp.int32)
    per = CHUNK // NB
    n = count * per
    local = kbuf.shape[2]
    rows = 4 * group
    first_slot = me * local
    exp_scale = math.log2(math.e) * HEAD ** -0.5
    step_col = lax.broadcasted_iota(jnp.int32, (rows, 1), 0) // group
    lane = lax.broadcasted_iota(jnp.int32, (1, local), 1) + first_slot
    new_lane = lax.broadcasted_iota(jnp.int32, (1, 8), 1)
    diag = lax.broadcasted_iota(jnp.int32, (rows, HEAD), 0) == lax.broadcasted_iota(jnp.int32, (rows, HEAD), 1)
    row16 = lax.broadcasted_iota(jnp.int32, (16, HEAD), 0)

    def place(i):
        rel = 3 - i % per // 2
        return jnp.bitwise_xor(me, rel) * 2 + i % 2

    def seqs(i):
        return pl.ds((first + i // per) * CHUNK + place(i) * NB, NB)

    def loads(i):
        return (pltpu.make_async_copy(k_hbm.at[seqs(i)], kbuf.at[i], in_sem.at[0, i]),
                pltpu.make_async_copy(v_hbm.at[seqs(i)], vbuf.at[i], in_sem.at[1, i]))

    def stores(i):
        return (pltpu.make_async_copy(kbuf.at[i], ko_hbm.at[seqs(i)], out_sem.at[0, i]),
                pltpu.make_async_copy(vbuf.at[i], vo_hbm.at[seqs(i)], out_sem.at[1, i]))

    small = [pltpu.make_async_copy(src.at[pl.ds(first, count)], dst, small_sem.at[4 + t]) for t, (src, dst) in enumerate(((q_hbm, q_ref), (kn_hbm, kn_ref), (vn_hbm, vn_ref)))]
    for copy in small:
        copy.start()
    for i in range(2):
        for copy in loads(i):
            copy.start()
    for copy in small:
        copy.wait()

    def body(i, carry):
        for copy in loads(i):
            copy.wait()

        @pl.when(i < AHEAD - 2)
        def _():
            for copy in loads(2 * i + 2) + loads(2 * i + 3):
                copy.start()

        @pl.when((i >= AHEAD - 2) & (i + AHEAD < n))
        def _():
            for copy in loads(i + AHEAD):
                copy.start()

        @pl.when(i > 0)
        def _():
            for copy in stores(i - 1):
                copy.start()

        grp = place(i)
        chunk = first + i // per
        here = i // per
        out_at = o_all.at[3 - i % per // 2, here * 2 + i % 2]
        bls = [jnp.bitwise_and(jb + me, NB - 1) for jb in range(NB)]
        ids = [grp * NB + bl for bl in bls]
        queries = [q_ref[here, pl.ds(seq, rows, stride=CHUNK), :].astype(BF16) for seq in ids]
        new_keys = kn_ref[here, pl.ds(ids[0], 8, stride=CHUNK), :].astype(BF16)
        new_vals = vn_ref[here, pl.ds(ids[0], 8, stride=CHUNK), :].astype(BF16)
        scores = []
        for bl, seq, query in zip(bls, ids, queries):
            pos = pos_ref[chunk * CHUNK + seq]
            age = jnp.where(lane < pos, jnp.bitwise_and(lane - pos, slots - 1), 0)
            scores.append(jnp.where(age > step_col, dot_nt(query, kbuf[i, bl]), NEG_BIG))
        new_scores = jnp.where(new_lane <= step_col, dot_nt(queries[0], new_keys), NEG_BIG)
        tops = [jnp.max(sc, axis=1, keepdims=True) for sc in scores]
        tops[0] = jnp.maximum(tops[0], jnp.max(new_scores, axis=1, keepdims=True))
        results = []
        for jb, bl in enumerate(bls):
            weights = jnp.exp2((scores[jb] - tops[jb]) * exp_scale)
            part_sum = jnp.sum(weights, axis=1, keepdims=True)
            out = dot(weights.astype(BF16), vbuf[i, bl])
            if jb == 0:
                new_weights = jnp.exp2((new_scores - tops[0]) * exp_scale)
                part_sum = part_sum + jnp.sum(new_weights, axis=1, keepdims=True)
                out = out + dot(new_weights.astype(BF16), new_vals)
            results.append((bl, out, tops[jb], part_sum))
        for bl, out, top, part_sum in results:
            out_at[pl.ds(pl.multiple_of(bl * rows, 8), rows), :] = out
            out_at[pl.ds(NB * rows + bl, 1), :] = jnp.sum(jnp.where(diag, top, 0.0), axis=0, keepdims=True)
            out_at[pl.ds(NB * rows + NB + bl, 1), :] = jnp.sum(jnp.where(diag, part_sum, 0.0), axis=0, keepdims=True)

        for bl in range(NB):
            seq = grp * NB + bl
            begin = jnp.bitwise_and(pos_ref[chunk * CHUNK + seq], slots - 1) - first_slot
            near = jnp.bitwise_and(begin, slots - 1)

            @pl.when((near < local) | (near > slots - 4))
            def _(bl=bl, seq=seq, begin=begin):
                for t in range(4):
                    slot = jnp.bitwise_and(begin + t, slots - 1)

                    @pl.when(slot < local)
                    def _(t=t, slot=slot):
                        window = pl.ds(pl.multiple_of(slot // 16 * 16, 16), 16)
                        hit = row16 == slot % 16
                        for buf, new_ref in ((kbuf, kn_ref), (vbuf, vn_ref)):
                            new = new_ref[here, pl.ds(t * CHUNK + seq, 1), :]
                            buf[i, bl, window, :] = jnp.where(hit, new, buf[i, bl, window, :].astype(F32)).astype(BF16)

        return carry

    lax.fori_loop(0, n, body, 0)
    tails = [pltpu.make_async_copy(o_all.at[r], outs[r], small_sem.at[r]) for r in range(4)]
    for copy in tails + list(stores(n - 1)):
        copy.start()
    for i in range(n):
        for copy in stores(i):
            copy.wait()
    for copy in tails:
        copy.wait()


def attention(first, count, slots, positions, q, kn, vn, k_cache, v_cache, outs, after):
    batch, local, _ = k_cache.shape
    chunks = batch // CHUNK
    group = q.shape[2]
    rows = 4 * group
    n = count * CHUNK // NB
    width = NB * rows + 2 * NB
    n_alias = 0 if outs is None else 2
    n_any = n_alias + len(after)
    any_spec = pl.BlockSpec(memory_space=pl.ANY)
    part_shape = jax.ShapeDtypeStruct((2 * count, width, HEAD), F32)
    cache_shape = jax.ShapeDtypeStruct(k_cache.shape, BF16)
    return pl.pallas_call(
        functools.partial(attn_kernel, first, count, group, slots, n_any),
        in_specs=[pl.BlockSpec(memory_space=pltpu.SMEM)] + [any_spec] * (5 + n_any),
        out_specs=[any_spec] * 6,
        out_shape=[cache_shape, cache_shape] + [part_shape] * 4,
        scratch_shapes=[
            pltpu.VMEM((n, NB, local, HEAD), BF16), pltpu.VMEM((n, NB, local, HEAD), BF16),
            pltpu.VMEM((count, rows * CHUNK, HEAD), F32), pltpu.VMEM((count, 8 * CHUNK, HEAD), F32), pltpu.VMEM((count, 8 * CHUNK, HEAD), F32),
            pltpu.VMEM((4, 2 * count, width, HEAD), F32),
            pltpu.SemaphoreType.DMA((2, n)), pltpu.SemaphoreType.DMA((2, n)), pltpu.SemaphoreType.DMA((7,)),
        ],
        input_output_aliases={6: 0, 7: 1} if n_alias else {},
        compiler_params=pltpu.CompilerParams(vmem_limit_bytes=VMEM_LIMIT),
        cost_estimate=pl.CostEstimate(flops=10_000_000_000 * count, bytes_accessed=count * CHUNK * local * HEAD * 8, transcendentals=CHUNK * rows * local),
        name="attn",
    )(positions, q.reshape(chunks, rows * CHUNK, HEAD), kn.reshape(chunks, 8 * CHUNK, HEAD), vn.reshape(chunks, 8 * CHUNK, HEAD), k_cache, v_cache, *(outs or ()), *after)


def combine_rows(group, parts, at, a_scr, a32_scr):
    rows = 4 * group
    exp_scale = math.log2(math.e) * HEAD ** -0.5
    for g in range(2):
        stats = [parts[i, 2 * at + g, NB * rows:NB * rows + 2 * NB, :] for i in range(SQ)]
        top = functools.reduce(jnp.maximum, stats)
        scale = [jnp.exp2((st - top) * exp_scale) for st in stats]
        total = sum(sc * pltpu.roll(st, NB, 0) for sc, st in zip(scale, stats))
        scale = [(sc / total).T for sc in scale]
        sums = [sum(parts[i, 2 * at + g, b * rows:(b + 1) * rows, :] * sc[:rows, b:b + 1] for i, sc in enumerate(scale)) for b in range(NB)]
        for b, acc in enumerate(sums):
            a_scr[pl.ds((g * NB + b) * rows, rows), :] = acc
    for s in range(4):
        for h in range(group):
            a32_scr[(4 * at + s) * QB:(4 * at + s + 1) * QB, h * HEAD:(h + 1) * HEAD] = a_scr[pl.ds(s * group + h, QB, stride=rows), :]


def combine_kernel(group, p0_hbm, p1_hbm, p2_hbm, p3_hbm, wo_hbm, *rest):
    out_hbm, parts, a_scr, a32_scr, a_bf, out_buf, wbuf, psem, wsem, osem = rest[-10:]
    n, _, block = wbuf.shape
    gets = [pltpu.make_async_copy(p, parts.at[i], psem.at[i]) for i, p in enumerate((p0_hbm, p1_hbm, p2_hbm, p3_hbm))]
    weights = [pltpu.make_async_copy(wo_hbm.at[:, pl.ds(j * block, block)], wbuf.at[j], wsem.at[j]) for j in range(n)]
    for copy in gets + weights:
        copy.start()
    for copy in gets:
        copy.wait()
    for at in range(parts.shape[1] // 2):
        combine_rows(group, parts, at, a_scr, a32_scr)
    a_bf[...] = a32_scr[...].astype(BF16)

    def columns(j):
        return pl.ds(pl.multiple_of(j * block, block), block)

    def out_copy(j):
        return pltpu.make_async_copy(out_buf.at[j], out_hbm.at[:, columns(j)], osem.at[j])

    def body(j, carry):
        pltpu.make_async_copy(wo_hbm.at[:, columns(j)], wbuf.at[j], wsem.at[j]).wait()
        out_buf[j] = dot(a_bf[...], wbuf[j])

        @pl.when(j > 0)
        def _():
            out_copy(j - 1).start()

        return carry

    lax.fori_loop(0, n, body, 0)
    out_copy(n - 1).start()
    for j in range(n):
        out_copy(j).wait()


def combine(parts, w_o, after):
    depth, dim = w_o.shape
    group = depth // HEAD
    n, block = 6, dim // 6
    out_rows = parts[0].shape[0] * 2 * QB
    any_spec = pl.BlockSpec(memory_space=pl.ANY)
    return pl.pallas_call(
        functools.partial(combine_kernel, group),
        in_specs=[any_spec] * (5 + len(after)),
        out_specs=any_spec,
        out_shape=jax.ShapeDtypeStruct((out_rows, dim), F32),
        scratch_shapes=[
            pltpu.VMEM((SQ,) + parts[0].shape, F32), pltpu.VMEM((4 * group * QB, HEAD), F32), pltpu.VMEM((out_rows, depth), F32),
            pltpu.VMEM((out_rows, depth), BF16), pltpu.VMEM((n, out_rows, block), F32), pltpu.VMEM((n, depth, block), BF16),
            pltpu.SemaphoreType.DMA((SQ,)), pltpu.SemaphoreType.DMA((n,)), pltpu.SemaphoreType.DMA((n,)),
        ],
        compiler_params=pltpu.CompilerParams(vmem_limit_bytes=VMEM_LIMIT),
        cost_estimate=pl.CostEstimate(flops=2_500_000_000, bytes_accessed=depth * dim * 2, transcendentals=0),
        name="combine_wo",
    )(*parts, w_o, *after)


MESH = pl.DeviceIdType.MESH
BLK = 512
TAIL_VMEM = 63_500_000


def tail_kernel(n_blk, group, x_ref, bo_ref, gain_ref, shift_ref, bproj_ref, bfc_ref, own_hbm, got_hbm, *refs):
    ready, fresh = refs[:SQ], refs[SQ:2 * SQ]
    (wo_ref, wfc_ref, wproj_ref, ys_ref, own_a, got_a, xs, pbuf, a_scr, a32_scr, wo, own_buf, got_buf, x1, hsend, hrecv, hall, g, wbuf, bproj, bfc,
     part, recv1, sums, recv2, ybuf, recv3, recv4, recv5,
     xsem, psem, fs, fr, wosem, wsem, os, og, hs, hr, s1, r1, s2, r2, s3, r3, s4, r4, s5, r5) = refs[2 * SQ:]
    me = lax.axis_index("sq").astype(jnp.int32)
    core = lax.rem(me, 2)
    peers = [me, me + 1 - 2 * core, lax.rem(me + 2, SQ), lax.rem(me + 3 - 2 * core, SQ)]
    sib, across = {"sq": peers[1]}, {"sq": peers[2]}
    partner = {"tp": 1 - lax.axis_index("tp")}
    span = 4 * QB
    half = 2 * span
    n_wo = wo.shape[0]

    def remote(src, dst, send, recv, device):
        return pltpu.make_async_remote_copy(src_ref=src, dst_ref=dst, send_sem=send, recv_sem=recv, device_id=device, device_id_type=MESH)

    def cols(j):
        return pl.ds(pl.multiple_of(j * BLK, BLK), BLK)

    def weights(kind, j):
        if kind % 2 == 0:
            src = wfc_ref.at[:, cols(core * n_blk + j)]
        else:
            src = wproj_ref.at[pl.ds(pl.multiple_of(core * n_blk * BLK, BLK), n_blk * BLK), cols(j)]
        return pltpu.make_async_copy(src, wbuf.at[j], wsem.at[j])

    def get_wo(j):
        return pltpu.make_async_copy(wo_ref.at[:, cols(j)], wo.at[j], wosem.at[j])

    def send_part(r):
        return remote(fresh[r], pbuf.at[1, r], fs.at[r], fr.at[r], {"sq": peers[r]})

    local = [pltpu.make_async_copy(ready[r], pbuf.at[0, r], psem.at[r]) for r in range(SQ)]
    local.append(pltpu.make_async_copy(fresh[0], pbuf.at[1, 0], psem.at[SQ]))
    x_copy = pltpu.make_async_copy(x_ref.at[:, :, me], xs, xsem)
    tops = [pltpu.make_async_copy(own_hbm, own_a, psem.at[SQ + 1]), pltpu.make_async_copy(got_hbm, got_a, psem.at[SQ + 2])]

    barrier = pltpu.get_barrier_semaphore()
    for device in ({"sq": peers[1]}, {"sq": peers[2]}, {"sq": peers[3]}, partner):
        pl.semaphore_signal(barrier, inc=1, device_id=device, device_id_type=MESH)
    for copy in local:
        copy.start()
    x_copy.start()
    for copy in tops:
        copy.start()
    for j in range(2):
        get_wo(j).start()
    pl.semaphore_wait(barrier, 4)
    for r in (2, 3, 1):
        send_part(r).start()
    for j in range(2, n_wo):
        get_wo(j).start()

    bias, gain, shift = as_row(bo_ref), as_row(gain_ref), as_row(shift_ref)
    bproj[...] = as_row(bproj_ref)
    bfc[...] = as_row(bfc_ref)

    def swap_own(i, j):
        return remote(own_buf.at[i, j], got_buf.at[i, j], os.at[i, j], og.at[i, j], partner)

    def project(i):
        combine_rows(group, pbuf.at[i], 0, a_scr, a32_scr)

        def body(j, carry):
            if i == 0:
                get_wo(j).wait()
            own_buf[i, j] = dot(a32_scr[...].astype(BF16), wo[j])
            swap_own(i, j).start()
            if i == 0:
                weights(0, j).start()
            return carry

        lax.fori_loop(0, n_wo, body, 0)

    def send_h(c):
        return remote(hsend.at[c], hrecv.at[c], hs.at[c], hr.at[c], sib)

    def enter(hf):
        for i in range(2):
            if hf == 0:
                delta = own_a[i * span:(i + 1) * span, :] + got_a[i * span:(i + 1) * span, :]
            else:
                for j in range(n_wo):
                    swap_own(i, j).wait_recv()
                delta = jnp.concatenate([own_buf[i, j] + got_buf[i, j] for j in range(n_wo)], axis=1)
            for s in range(4):
                mid = xs[s, 2 * hf + i].astype(F32) + delta[s * QB:(s + 1) * QB, :] + bias
                x1[hf, i * span + s * QB:i * span + (s + 1) * QB, :] = mid.astype(BF16).astype(F32)
            h = layer_norm(x1[hf, i * span:(i + 1) * span, :], gain, shift).astype(BF16)
            hall[i * span:(i + 1) * span, :] = h
            hsend[2 * hf + i] = h.astype(F32)
            send_h(2 * hf + i).start()

    def gather_h(hf):
        for i in range(2):
            send_h(2 * hf + i).wait_recv()
            hall[half + i * span:half + (i + 1) * span, :] = hrecv[2 * hf + i].astype(BF16)

    def first(hf):
        def body(j, carry):
            weights(2 * hf, j).wait()
            acc = dot(hall[...], wbuf[j]) + bfc[:, cols(core * n_blk + j)]
            g[:, cols(j)] = jax.nn.gelu(acc, approximate=True).astype(BF16)
            weights(2 * hf + 1, j).start()
            return carry

        lax.fori_loop(0, n_blk, body, 0)

    def send1(hf, j):
        return remote(part.at[hf, j], recv1.at[hf, j], s1.at[hf, j], r1.at[hf, j], sib)

    def send2(hf, j):
        return remote(sums.at[hf, j], recv2.at[hf, j], s2.at[hf, j], r2.at[hf, j], partner)

    def send3(hf, j):
        return remote(ybuf.at[hf, j], recv3.at[hf, j], s3.at[hf, j], r3.at[hf, j], across)

    def send4(hf, j):
        return remote(ybuf.at[hf, j], recv4.at[hf, j], s4.at[hf, j], r4.at[hf, j], sib)

    def send5(hf, j):
        return remote(recv3.at[hf, j], recv5.at[hf, j], s5.at[hf, j], r5.at[hf, j], sib)

    def reduce_cores(hf, j):
        send1(hf, j).wait_recv()
        sums[hf, j] = sums[hf, j] + recv1[hf, j]
        send2(hf, j).start()

    def store_rows(hf, j, value, owner):
        for i in range(2):
            for s in range(4):
                ys_ref[s, 2 * hf + i, owner, :, cols(j)] = value[i * span + s * QB:i * span + (s + 1) * QB, :].astype(BF16)

    def finish(hf, j):
        send2(hf, j).wait_recv()
        ybuf[hf, j] = (x1[hf, :, cols(j)] + (sums[hf, j] + recv2[hf, j]) + bproj[:, cols(j)]).astype(BF16).astype(F32)
        send3(hf, j).start()
        send4(hf, j).start()
        store_rows(hf, j, ybuf[hf, j], me)

    def late(hf, j):
        send3(hf, j).wait_recv()
        send5(hf, j).start()
        store_rows(hf, j, recv3[hf, j], peers[2])
        send4(hf, j).wait_recv()
        store_rows(hf, j, recv4[hf, j], peers[1])
        send5(hf, j).wait_recv()
        store_rows(hf, j, recv5[hf, j], peers[3])

    def second(hf):
        def body(j, carry):
            weights(2 * hf + 1, j).wait()
            acc = dot(g[...], wbuf[j])
            part[hf, j] = acc[half:, :]
            send1(hf, j).start()
            sums[hf, j] = acc[:half, :]
            if hf == 0:
                weights(2, j).start()

            @pl.when(j > 1)
            def _():
                reduce_cores(hf, j - 2)

            if hf == 1:
                finish(0, j)
            return carry

        lax.fori_loop(0, n_blk, body, 0)
        reduce_cores(hf, n_blk - 2)
        reduce_cores(hf, n_blk - 1)

    for copy in local[:SQ]:
        copy.wait()
    project(0)
    x_copy.wait()
    for copy in tops:
        copy.wait()
    enter(0)
    gather_h(0)
    first(0)
    local[SQ].wait()
    for r in (1, 2, 3):
        send_part(r).wait_recv()
    project(1)
    second(0)
    enter(1)
    gather_h(1)
    first(1)
    second(1)

    def drain(j, carry):
        late(0, j)
        finish(1, j)

        @pl.when(j > 0)
        def _():
            late(1, j - 1)

        return carry

    lax.fori_loop(0, n_blk, drain, 0)
    late(1, n_blk - 1)

    for r in range(1, SQ):
        send_part(r).wait_send()
    for i in range(2):
        for j in range(n_wo):
            swap_own(i, j).wait_send()
    for c in range(4):
        send_h(c).wait_send()

    def sent(j, carry):
        for hf in range(2):
            for send in (send1, send2, send3, send4, send5):
                send(hf, j).wait_send()
        return carry

    lax.fori_loop(0, n_blk, sent, 0)


def tail(x_view, vectors, own, got, ready, fresh, w_o, w_fc, w_proj):
    steps, chunks, _, _, dim = x_view.shape
    depth = w_o.shape[0]
    width = w_fc.shape[1] // 2
    n_blk = width // BLK
    span = 4 * QB
    any_spec = pl.BlockSpec(memory_space=pl.ANY)
    vmem = pl.BlockSpec(memory_space=pltpu.VMEM)
    blocks = lambda: pltpu.VMEM((2, n_blk, 2 * span, BLK), F32)
    sem = lambda *n: pltpu.SemaphoreType.DMA(n)
    return pl.pallas_call(
        functools.partial(tail_kernel, n_blk, depth // HEAD),
        in_specs=[any_spec] + [vmem] * len(vectors) + [any_spec] * (2 * SQ + 5),
        out_specs=vmem,
        out_shape=pltpu.VMEM((steps, chunks, SQ, QB, dim), BF16),
        scratch_shapes=[
            pltpu.VMEM((2 * span, dim), F32), pltpu.VMEM((2 * span, dim), F32),
            pltpu.VMEM((steps, chunks, QB, dim), BF16), pltpu.VMEM((2, SQ) + ready[0].shape, F32),
            pltpu.VMEM((span * depth // HEAD, HEAD), F32), pltpu.VMEM((span, depth), F32), pltpu.VMEM((dim // BLK, depth, BLK), BF16),
            pltpu.VMEM((2, dim // BLK, span, BLK), F32), pltpu.VMEM((2, dim // BLK, span, BLK), F32), pltpu.VMEM((2, 2 * span, dim), F32),
            pltpu.VMEM((chunks, span, dim), F32), pltpu.VMEM((chunks, span, dim), F32),
            pltpu.VMEM((4 * span, dim), BF16), pltpu.VMEM((4 * span, width), BF16), pltpu.VMEM((n_blk, dim, BLK), BF16),
            pltpu.VMEM((1, dim), F32), pltpu.VMEM((1, 2 * width), F32),
        ] + [blocks() for _ in range(8)]
        + [pltpu.SemaphoreType.DMA, sem(SQ + 3), sem(SQ), sem(SQ), sem(dim // BLK), sem(n_blk), sem(2, dim // BLK), sem(2, dim // BLK), sem(chunks), sem(chunks)]
        + [sem(2, n_blk) for _ in range(10)],
        compiler_params=pltpu.CompilerParams(vmem_limit_bytes=TAIL_VMEM, collective_id=0, has_side_effects=True),
        cost_estimate=pl.CostEstimate(flops=40_000_000_000, bytes_accessed=dim * width * 8, transcendentals=0),
        name="tail",
    )(x_view, *vectors, own, got, *ready, *fresh, w_o, w_fc, w_proj)


def solution(mesh):
    act_spec = P(None, "dp", None)
    cache_spec = P("dp", "sq", "tp", None)
    col_spec = P(None, "tp")
    row_spec = P("tp", None)
    vec_spec = P("tp")
    rep_spec = P(None)
    in_specs = (act_spec, P("dp"), cache_spec, cache_spec, col_spec, vec_spec, col_spec, vec_spec,
                col_spec, vec_spec, row_spec, rep_spec, rep_spec, rep_spec, rep_spec, rep_spec,
                col_spec, vec_spec, row_spec, rep_spec)
    out_specs = (act_spec, cache_spec, cache_spec)

    def swap_sq(value, mask):
        return lax.ppermute(value, "sq", [(i, i ^ mask) for i in range(SQ)])

    def swap_tp(value):
        return lax.ppermute(value, "tp", [(0, 1), (1, 0)])

    def per_device(x_steps, positions, key_buf, val_buf, w_q, b_q, w_k, b_k, w_v, b_v, w_o, b_o,
                   ln1_gain, ln1_bias, ln2_gain, ln2_bias, w_fc, b_fc, w_proj, b_proj):
        steps, batch, dim = x_steps.shape
        local = key_buf.shape[1]
        slots = local * SQ
        chunks = batch // CHUNK
        inv_freq = jnp.power(F32(ROPE_BASE), -2.0 * jnp.arange(HEAD // 2, dtype=F32) / HEAD)
        cur = positions[None, :] + jnp.arange(steps, dtype=jnp.int32)[:, None]
        angle = cur.reshape(-1).astype(F32)[:, None] * inv_freq
        q, kn, vn = qkv(x_steps, ln1_gain, ln1_bias, w_q, b_q, w_k, b_k, w_v, b_v, jnp.cos(angle), jnp.sin(angle))
        k_old, v_old = key_buf.reshape(batch, local, HEAD), val_buf.reshape(batch, local, HEAD)
        x_view = x_steps.reshape(steps, chunks, SQ, QB, dim)

        half = chunks // 2

        def moved(parts):
            return [parts[0]] + [swap_sq(parts[r], r) for r in range(1, SQ)]

        first = attention(0, half, slots, positions, q, kn, vn, k_old, v_old, None, [])
        early = moved(first[2:])
        third = attention(half, 1, slots, positions, q, kn, vn, k_old, v_old, first[:2], [])
        own = combine(early, w_o, third[2:3])
        got = swap_tp(own)
        waiting = moved(third[2:])
        res = attention(half + 1, 1, slots, positions, q, kn, vn, k_old, v_old, third[:2], [own])
        caches = res[:2]
        ys = tail(x_view, (b_o, ln2_gain, ln2_bias, b_proj, b_fc), own, got, waiting, res[2:], w_o, w_fc, w_proj).reshape(steps, batch, dim)
        return ys, caches[0].reshape(key_buf.shape), caches[1].reshape(val_buf.shape)

    return jax.shard_map(per_device, mesh=mesh, in_specs=in_specs, out_specs=out_specs, check_vma=False)
```
